1024 devices in a mesh: gx: 8 (over z_hi, x), gy: 8 (over y, core), gz: 16 (over z_lo).
Axes of the slice: x: 4, y: 4, z: 32 (z_hi: 2, z_lo: 16; z = z_hi * 16 + z_lo), core: 2. Of those that a mesh axis runs over, the one named last changes fastest.
Arguments:
- vorticity: float32 [3, 64, 128, 2048], P(None, 'gx', 'gy', 'gz'), may hold values from -6 to 6
- velocity: float32 [3, 64, 128, 2048], P(None, 'gx', 'gy', 'gz'), may hold values from -1 to 1
Outputs:
- vorticity_out: float32 [3, 64, 128, 2048], P(None, 'gx', 'gy', 'gz')
The draws below stay inside these ranges and needn't reach their ends.
All inputs are finite; a program needn't handle non-finite values.
Results may differ from the reference program's by a relative error of at most 0.0003.
Values sent between devices are 32-bit elements; how exact they have to be, the bound alone decides.
No kernel may reach another device: no remote copies, remote signals or barrier semaphores. Data moves between devices by JAX's collectives and lax.ppermute only.
A program may use at most 32 MiB of HBM per device.

```python
import jax
import jax.numpy as jnp

SUBSTEPS = 2
NX = 64
NY = 128
NZ = 2048


def level_of(key, shape, shards, least, largest):
    def one(position, blocks):
        heights = jax.random.uniform(jax.random.fold_in(jax.random.fold_in(key, 6), position), (blocks,), jnp.float32, least / len(shards), largest / len(shards))
        return jnp.repeat(jnp.exp(heights), shape[position] // blocks).reshape((-1,) + (1,) * (len(shape) - position - 1))

    gain = one(*shards[0])
    for cut in shards[1:]:
        gain = gain * one(*cut)
    return gain


def bell_draw(stream_key, extent, deviation, bound, split=(), held_as=jnp.bfloat16):
    factor_of = level_of(stream_key, extent, split, -0.22, 0.18) if split else 1.0
    array = jax.random.normal(stream_key, extent, jnp.float32) * deviation * factor_of
    return jnp.minimum(jnp.maximum(array, -bound), bound).astype(held_as)


def setup_inputs(seed: int = 0) -> dict:
    splits = jax.random.split(jax.random.key(seed), 3)
    vorticity = bell_draw(splits[0], (3, NX, NY, NZ), 1.0, 6.0, ((1, 8), (2, 8), (3, 16)), jnp.float32)
    velocity = jnp.clip(jax.random.uniform(splits[1], (3, NX, NY, NZ), jnp.float32, -1.0, 1.0) * level_of(splits[1], (3, NX, NY, NZ), ((1, 8), (2, 8), (3, 16)), -0.4, 0.0), -1.0, 1.0)
    return dict(vorticity=vorticity, velocity=velocity)


time_step = 0.5


def kernel(distance):
    magnitude = jnp.abs(distance)
    near = 1.0 - 2.5 * magnitude * magnitude + 1.5 * magnitude * magnitude * magnitude
    far = 0.5 * (2.0 - magnitude) * (2.0 - magnitude) * (1.0 - magnitude)
    return jnp.where(magnitude < 1.0, near, jnp.where(magnitude < 2.0, far, 0.0))


def remesh(current, displace, along):
    total = jnp.zeros_like(current)
    for offset in range(-2, 3):
        total = total + jnp.roll(kernel(offset - displace) * current, offset, axis=along)
    return total


def derive(values, along):
    near_diff = jnp.roll(values, -1, axis=along) - jnp.roll(values, 1, axis=along)
    far_diff = jnp.roll(values, -2, axis=along) - jnp.roll(values, 2, axis=along)
    return (8.0 * near_diff - far_diff) / 12.0


def reference(vorticity, velocity):
    slopes = [derive(velocity, along) for along in (1, 2, 3)]
    current = vorticity
    for substep in range(SUBSTEPS):
        for along in (1, 2, 3):
            current = remesh(current, time_step * velocity[along - 1], along)
        stretch = current[0] * slopes[0] + current[1] * slopes[1] + current[2] * slopes[2]
        current = current + time_step * stretch
    return current
```

```python
import jax
import jax.numpy as jnp
from jax import lax
from jax.experimental import pallas as pl
from jax.experimental.pallas import tpu as pltpu
from jax.sharding import PartitionSpec as P

AXES = ("gx", "gy", "gz")
HALF = 0.5


def flat_pairs(mesh, move):
    nx, ny, nz = (mesh.shape[a] for a in AXES)
    pairs = []
    for x in range(nx):
        for y in range(ny):
            for z in range(nz):
                to = move(x, y, z)
                if to is not None:
                    tx, ty, tz = to[0] % nx, to[1] % ny, to[2] % nz
                    pairs.append(((x * ny + y) * nz + z, (tx * ny + ty) * nz + tz))
    return pairs


def lanes_of(shape):
    return lax.broadcasted_iota(jnp.int32, shape, len(shape) - 1)


def rows_of(shape):
    return lax.broadcasted_iota(jnp.int32, shape, len(shape) - 2)


def roll(x, shift, axis):
    shift = shift % x.shape[axis]
    return x if shift == 0 else pltpu.roll(x, shift, axis)


def between(index, first, last):
    return (index >= first) & (index < last)


def pack_x(odd_ref, c_ref, v_ref, a_ref, b_ref):
    high = 4 * odd_ref[0]
    low = 4 - high
    for i in range(3):
        a_ref[i] = c_ref[i, pl.ds(high, 4)]
        a_ref[3 + i] = v_ref[i, pl.ds(high, 4)]
        b_ref[i] = c_ref[i, pl.ds(low, 4)]
        b_ref[3 + i] = v_ref[i, pl.ds(low, 4)]


def x_layer(slot, odd, c_ref, v_ref, lo_ref, hi_ref, field):
    if slot < 4:
        return lo_ref[field, slot]
    if slot < 12:
        return c_ref[field, slot - 4] if field < 3 else v_ref[field - 3, slot - 4]
    return hi_ref[field, slot - 12]


def pack_z(odd_ref, c_ref, v_ref, a_ref, b_ref, lo_ref, hi_ref, left_ref, right_ref):
    odd = odd_ref[0]

    @pl.when(odd == 1)
    def _():
        hi_ref[...] = a_ref[...]
        lo_ref[...] = b_ref[...]

    @pl.when(odd == 0)
    def _():
        hi_ref[...] = b_ref[...]
        lo_ref[...] = a_ref[...]

    lane = lanes_of((16, 128))
    for q in range(4):
        left = jnp.zeros((16, 128), jnp.float32)
        right = left
        for g in range(4):
            for field in range(6):
                at = 32 * g + 4 * field
                x = x_layer(4 * g + q, odd, c_ref, v_ref, lo_ref, hi_ref, field)
                here = between(lane, at, at + 4)
                left = jnp.where(here, roll(x, at, 1), left)
                right = jnp.where(here, roll(x, at + 4, 1), right)
        left_ref[q] = left
        right_ref[q] = right


def pack_y(c_ref, v_ref, lo_ref, hi_ref, zl_ref, zr_ref, down_ref, up_ref):
    upper = rows_of((8, 128)) < 4

    def join(first, second):
        down = jnp.where(upper, first[0:8], roll(second[0:8], 4, 0))
        up = jnp.where(upper, roll(first[8:16], 4, 0), second[8:16])
        return down, up

    for field in range(6):
        for s in range(8):
            pair = [x_layer(t, None, c_ref, v_ref, lo_ref, hi_ref, field) for t in (s, s + 8)]
            down_ref[8 * field + s], up_ref[8 * field + s] = join(*pair)
    for q in range(4):
        down_ref[48 + q], up_ref[48 + q] = join(zl_ref[q], zr_ref[q])


def weights(v):
    t = HALF * jnp.abs(v)
    ahead = v > 0.0
    u = 1.0 - t
    tt = t * t
    centre = 1.0 + tt * (1.5 * t - 2.5)
    near = t * (0.5 + t * (2.0 - 1.5 * t))
    tu = -0.5 * t * u
    behind = tu * u
    far = tu * t
    return (
        jnp.where(ahead, 0.0, far),
        jnp.where(ahead, behind, near),
        centre,
        jnp.where(ahead, near, behind),
        jnp.where(ahead, far, 0.0),
    )


def spread(c, w, axis):
    forth = roll(w[3] * c + roll(w[4] * c, 1, axis), 1, axis)
    back = roll(w[1] * c + roll(w[0] * c, -1, axis), -1, axis)
    return w[2] * c + forth + back


def slope_of(two_back, back, forth, two_forth):
    return (8.0 * (forth - back) - (two_forth - two_back)) * (1.0 / 12.0)


def slope_roll(v, axis):
    return slope_of(roll(v, 2, axis), roll(v, 1, axis), roll(v, -1, axis), roll(v, -2, axis))


def replicate(e):
    lane = lanes_of(e.shape)
    up1, up2 = roll(e, 32, 1), roll(e, 64, 1)
    dn1, dn2 = roll(e, -32, 1), roll(e, -64, 1)
    first, second = lane < 32, lane < 64
    return (
        jnp.where(first, e, jnp.where(second, up1, up2)),
        jnp.where(first, dn1, jnp.where(second, e, up1)),
        jnp.where(first, dn2, jnp.where(second, dn1, e)),
    )


def compute(
    c_ref, v_ref, lo_ref, hi_ref, zl_ref, zr_ref, above_ref, below_ref, out_ref,
    m_ref, ec_ref, ev_ref, ed_ref, x_ref, ex_ref, s_ref, es_ref, y_ref, ey_ref,
):
    upper = rows_of((8, 128)) < 4

    def halo(entry, second):
        above, below = above_ref[entry], below_ref[entry]
        if second:
            return jnp.where(upper, roll(above, 4, 0), below)
        return jnp.where(upper, above, roll(below, 4, 0))

    for field in range(6):
        for s in range(16):
            m_ref[field, s, 0:16] = x_layer(s, None, c_ref, v_ref, lo_ref, hi_ref, field)
            m_ref[field, s, 16:24] = halo(8 * field + s % 8, s >= 8)
    lane = lanes_of((24, 128))
    for s in range(16):
        g, q = s // 4, s % 4
        zl = jnp.concatenate([zl_ref[q], halo(48 + q, False)], axis=0)
        zr = jnp.concatenate([zr_ref[q], halo(48 + q, True)], axis=0)
        for kind, e_ref in ((0, ec_ref), (1, ev_ref)):
            e = jnp.zeros((24, 128), jnp.float32)
            for i in range(3):
                field = 3 * kind + i
                at = 32 * i
                held = 32 * g + 4 * field
                x = m_ref[field, s]
                e = jnp.where(between(lane, at, at + 4), roll(zl, at - held, 1), e)
                e = jnp.where(between(lane, at + 4, at + 16), roll(x, at + 4, 1), e)
                e = jnp.where(between(lane, at + 16, at + 28), roll(x, at + 28, 1), e)
                e = jnp.where(between(lane, at + 28, at + 32), roll(zr, at + 28 - held, 1), e)
            e_ref[s] = e
        for k, d in enumerate(replicate(ev_ref[s])):
            ed_ref[k, s] = d

    for s in range(2, 14):
        for i in range(3):
            around = [m_ref[3 + i, s + k] for k in (-2, -1, 1, 2)]
            s_ref[0, i, s] = slope_of(*around)
            v = m_ref[3 + i, s]
            s_ref[1, i, s] = slope_roll(v, 0)
            s_ref[2, i, s] = slope_roll(v, 1)
        around = [ev_ref[s + k] for k in (-2, -1, 1, 2)]
        es_ref[0, s] = slope_of(*around)
        v = ev_ref[s]
        es_ref[1, s] = slope_roll(v, 0)
        es_ref[2, s] = slope_roll(v, 1)

    def along_x(sources, v_of, stores, first, last):
        for tile in range(3):
            rows = slice(8 * tile, 8 * tile + 8)
            open_sums = {}
            for p in range(first - 2, last + 2):
                w = weights(v_of(p, rows))
                cs = [source(p, rows) for source in sources]
                for a in range(-2, 3):
                    to = p + a
                    if first <= to < last:
                        terms = [w[a + 2] * c for c in cs]
                        had = open_sums.get(to)
                        open_sums[to] = terms if had is None else [h + t for h, t in zip(had, terms)]
                done = open_sums.pop(p - 2, None)
                if done is not None:
                    for store, value in zip(stores, done):
                        store(p - 2, rows, value)

    def put(ref, *lead):
        def store(p, rows, value):
            ref[(*lead, p, rows)] = value
        return store

    def get(ref, *lead):
        return lambda p, rows: ref[(*lead, p, rows)]

    for substep in range(2):
        first, last = (2, 14) if substep == 0 else (4, 12)
        from_main = m_ref if substep == 0 else y_ref
        from_edge = ec_ref if substep == 0 else ey_ref
        along_x(
            [get(from_main, i) for i in range(3)], get(m_ref, 3),
            [put(x_ref, i) for i in range(3)], first, last,
        )
        along_x([get(from_edge)], get(ed_ref, 0), [put(ex_ref)], first, last)
        for s in range(first, last):
            w = weights(m_ref[4, s])
            cs = [spread(x_ref[i, s], w, 0) for i in range(3)]
            rows = 24 if substep == 0 else 16
            cs = [c[0:rows] for c in cs]
            w = weights(m_ref[5, s, 0:rows])
            cs = [spread(c, w, 1) for c in cs]
            new = []
            for i in range(3):
                stretch = sum(cs[j] * s_ref[j, i, s, 0:rows] for j in range(3))
                new.append(cs[i] + HALF * stretch)
            e = spread(ex_ref[s], weights(ed_ref[1, s]), 0)[0:rows]
            e = spread(e, weights(ed_ref[2, s, 0:rows]), 1)
            parts = replicate(e)
            e = e + HALF * sum(parts[j] * es_ref[j, s, 0:rows] for j in range(3))
            if substep == 0:
                for i in range(3):
                    y_ref[i, s] = new[i]
                ey_ref[s] = e
            else:
                lane16 = lanes_of((16, 128))
                for i in range(3):
                    value = jnp.where(lane16 < 4, roll(e, -(32 * i + 4), 1), new[i])
                    value = jnp.where(lane16 >= 124, roll(e, 100 - 32 * i, 1), value)
                    out_ref[i, s - 4] = value


def call(kernel, outs, scratch=(), scalars=0, operands=0):
    smem = pl.BlockSpec(memory_space=pltpu.SMEM)
    vmem = pl.BlockSpec(memory_space=pltpu.VMEM)
    shapes = [jax.ShapeDtypeStruct(o, jnp.float32) for o in outs]
    return pl.pallas_call(
        kernel,
        out_shape=shapes,
        in_specs=[smem] * scalars + [vmem] * operands,
        out_specs=[vmem] * len(outs),
        scratch_shapes=[pltpu.VMEM(s, jnp.float32) for s in scratch],
        name=kernel.__name__,
    )


def solution(mesh):
    step = 1
    across = flat_pairs(mesh, lambda x, y, z: (x + 1 if x % 2 else x - 1, y, z))
    other = flat_pairs(mesh, lambda x, y, z: (x - 1 if x % 2 else x + 1, y, z))
    y_up = flat_pairs(mesh, lambda x, y, z: (x, y + step, z))
    y_down = flat_pairs(mesh, lambda x, y, z: (x, y - step, z))
    z_up = flat_pairs(mesh, lambda x, y, z: (x, y, z + step))
    z_down = flat_pairs(mesh, lambda x, y, z: (x, y, z - step))

    def send(value, pairs):
        return lax.ppermute(value, AXES, pairs)

    def local(c, v):
        odd = (lax.axis_index("gx") % 2).astype(jnp.int32).reshape(1)
        layers = (6, 4, 16, 128)
        a, b = call(pack_x, [layers, layers], (), 1, 2)(odd, c, v)
        b = send(b, other)
        a = send(a, across)
        edge = (4, 16, 128)
        lo, hi, left, right = call(pack_z, [layers, layers, edge, edge], (), 1, 4)(odd, c, v, a, b)
        zl = send(right, z_up)
        zr = send(left, z_down)
        down, up = call(pack_y, [(52, 8, 128)] * 2, (), 0, 6)(c, v, lo, hi, zl, zr)
        above = send(down, y_down)
        below = send(up, y_up)
        block = (16, 24, 128)
        scratch = [
            (6, *block), block, block, (3, *block), (3, *block), block,
            (3, 3, *block), (3, *block), (3, *block), block,
        ]
        (out,) = call(compute, [(3, 8, 16, 128)], scratch, 0, 8)(c, v, lo, hi, zl, zr, above, below)
        return out

    placed = P(None, *AXES)
    return jax.shard_map(local, mesh=mesh, in_specs=(placed, placed), out_specs=placed, check_vma=False)
```

```python
import jax
import jax.numpy as jnp
from jax import lax
from jax.experimental import pallas as pl
from jax.experimental.pallas import tpu as pltpu
from jax.sharding import PartitionSpec as P

AXES = ("gx", "gy", "gz")
HALF = 0.5


def flat_pairs(mesh, move):
    nx, ny, nz = (mesh.shape[a] for a in AXES)
    pairs = []
    for x in range(nx):
        for y in range(ny):
            for z in range(nz):
                to = move(x, y, z)
                if to is not None:
                    tx, ty, tz = to[0] % nx, to[1] % ny, to[2] % nz
                    pairs.append(((x * ny + y) * nz + z, (tx * ny + ty) * nz + tz))
    return pairs


def lanes_of(shape):
    return lax.broadcasted_iota(jnp.int32, shape, len(shape) - 1)


def rows_of(shape):
    return lax.broadcasted_iota(jnp.int32, shape, len(shape) - 2)


def roll(x, shift, axis):
    shift = shift % x.shape[axis]
    return x if shift == 0 else pltpu.roll(x, shift, axis)


def between(index, first, last):
    return (index >= first) & (index < last)


def loop(first, last, body, unroll=1):
    def step(i, carry):
        body(i)
        return carry

    lax.fori_loop(first, last, step, 0, unroll=unroll)


def field_of(c_ref, v_ref, field):
    return (c_ref, field) if field < 3 else (v_ref, field - 3)


def pack_x(place_ref, c_ref, v_ref, a_ref, b_ref, edge_ref):
    high = 4 * place_ref[0]
    low = 4 - high
    shift = 4 * place_ref[1]

    def copy(q):
        for field in range(6):
            ref, i = field_of(c_ref, v_ref, field)
            a_ref[field, q] = ref[i, high + q]
            b_ref[field, q] = ref[i, low + q]
        lane = lanes_of((16, 128))
        edge = jnp.zeros((16, 128), jnp.float32)
        for g in (1, 2):
            for field in range(6):
                ref, i = field_of(c_ref, v_ref, field)
                at = 32 * g + 4 * field
                x = pltpu.roll(ref[i, 4 * (g - 1) + q], shift + at, 1)
                edge = jnp.where(between(lane, at, at + 4), x, edge)
        edge_ref[q] = edge

    loop(0, 4, copy)


def lower_upper(odd, a_ref, b_ref, field, q):
    a, b = a_ref[field, q], b_ref[field, q]
    return jnp.where(odd, b, a), jnp.where(odd, a, b)


def pack_z(place_ref, c_ref, v_ref, a_ref, b_ref, left_ref, right_ref):
    odd = place_ref[0] == 1

    def pack(q):
        lane = lanes_of((16, 128))
        left = jnp.zeros((16, 128), jnp.float32)
        right = left
        for field in range(6):
            ref, i = field_of(c_ref, v_ref, field)
            lo, hi = lower_upper(odd, a_ref, b_ref, field, q)
            for g, x in enumerate((lo, ref[i, q], ref[i, 4 + q], hi)):
                at = 32 * g + 4 * field
                here = between(lane, at, at + 4)
                left = jnp.where(here, roll(x, at, 1), left)
                right = jnp.where(here, roll(x, at + 4, 1), right)
        left_ref[q] = left
        right_ref[q] = right

    loop(0, 4, pack)


def pack_y(
    place_ref, c_ref, v_ref, a_ref, b_ref, zl_ref, zr_ref, wrap_ref, wrap_a_ref, wrap_b_ref,
    down_ref, up_ref, zl_out_ref, zr_out_ref,
):
    odd = place_ref[0] == 1
    first_end = place_ref[2] == 1
    last_end = place_ref[3] == 1
    upper = rows_of((8, 128)) < 4

    def join(entry, first, second):
        down_ref[entry] = jnp.where(upper, first[0:8], roll(second[0:8], 4, 0))
        up_ref[entry] = jnp.where(upper, roll(first[8:16], 4, 0), second[8:16])

    def pack(q):
        for field in range(6):
            ref, i = field_of(c_ref, v_ref, field)
            lo, hi = lower_upper(odd, a_ref, b_ref, field, q)
            near, far = ref[i, q], ref[i, 4 + q]
            join(8 * field + q, lo, far)
            join(8 * field + 4 + q, near, hi)
        lane = lanes_of((16, 128))
        wrap_a, wrap_b = roll(wrap_a_ref[q], 64, 1), roll(wrap_b_ref[q], 64, 1)
        lo, hi = jnp.where(odd, wrap_b, wrap_a), jnp.where(odd, wrap_a, wrap_b)
        wrap = jnp.where(lane < 32, lo, jnp.where(lane < 96, wrap_ref[q], hi))
        zl = jnp.where(first_end, wrap, zl_ref[q])
        zr = jnp.where(last_end, wrap, zr_ref[q])
        zl_out_ref[q] = zl
        zr_out_ref[q] = zr
        join(48 + q, zl, zr)

    loop(0, 4, pack)


def weights(v):
    t = HALF * jnp.abs(v)
    ahead = v > 0.0
    u = 1.0 - t
    tt = t * t
    centre = 1.0 + tt * (1.5 * t - 2.5)
    near = t * (0.5 + t * (2.0 - 1.5 * t))
    tu = -0.5 * t * u
    behind = tu * u
    far = tu * t
    return (
        jnp.where(ahead, 0.0, far),
        jnp.where(ahead, behind, near),
        centre,
        jnp.where(ahead, near, behind),
        jnp.where(ahead, far, 0.0),
    )


def spread(c, w, axis):
    near = roll(w[3] * c, 1, axis) + roll(w[1] * c, -1, axis)
    far = roll(w[4] * c, 2, axis) + roll(w[0] * c, -2, axis)
    return w[2] * c + near + far


def slope_of(two_back, back, forth, two_forth):
    return (8.0 * (forth - back) - (two_forth - two_back)) * (1.0 / 12.0)


def slope_roll(v, axis):
    return slope_of(roll(v, 2, axis), roll(v, 1, axis), roll(v, -1, axis), roll(v, -2, axis))


def replicate(e):
    lane = lanes_of(e.shape)
    up1, up2 = roll(e, 32, 1), roll(e, 64, 1)
    dn1, dn2 = roll(e, -32, 1), roll(e, -64, 1)
    first, second = lane < 32, lane < 64
    return (
        jnp.where(first, e, jnp.where(second, up1, up2)),
        jnp.where(first, dn1, jnp.where(second, e, up1)),
        jnp.where(first, dn2, jnp.where(second, dn1, e)),
    )


def compute(
    place_ref, c_ref, v_ref, a_ref, b_ref, zl_ref, zr_ref, above_ref, below_ref, out_ref,
    m_ref, ec_ref, ev_ref, ed_ref, x_ref, ex_ref, s_ref, es_ref,
):
    odd = place_ref[0] == 1
    upper = rows_of((8, 128)) < 4

    def halo(entry):
        above, below = above_ref[entry], below_ref[entry]
        first = jnp.where(upper, above, roll(below, 4, 0))
        return first, jnp.where(upper, roll(above, 4, 0), below)

    def widen(q):
        for field in range(6):
            ref, i = field_of(c_ref, v_ref, field)
            lo, hi = lower_upper(odd, a_ref, b_ref, field, q)
            m_ref[field, q, 0:16] = lo
            m_ref[field, 4 + q, 0:16] = ref[i, q]
            m_ref[field, 8 + q, 0:16] = ref[i, 4 + q]
            m_ref[field, 12 + q, 0:16] = hi
            m_ref[field, q, 16:24], m_ref[field, 8 + q, 16:24] = halo(8 * field + q)
            m_ref[field, 4 + q, 16:24], m_ref[field, 12 + q, 16:24] = halo(8 * field + 4 + q)

    loop(0, 4, widen)

    def edges(s):
        lane = lanes_of((24, 128))
        g, q = lax.shift_right_logical(s, 2), lax.bitwise_and(s, 3)
        zl_halo, zr_halo = halo(48 + q)
        zl = jnp.concatenate([zl_ref[q], zl_halo], axis=0)
        zr = jnp.concatenate([zr_ref[q], zr_halo], axis=0)
        back = 128 - 32 * g
        zl, zr = pltpu.roll(zl, back, 1), pltpu.roll(zr, back, 1)
        for kind, e_ref in ((0, ec_ref), (1, ev_ref)):
            e = jnp.zeros((24, 128), jnp.float32)
            for i in range(3):
                field = 3 * kind + i
                at = 32 * i
                x = m_ref[field, s]
                e = jnp.where(between(lane, at, at + 4), roll(zl, at - 4 * field, 1), e)
                e = jnp.where(between(lane, at + 4, at + 16), roll(x, at + 4, 1), e)
                e = jnp.where(between(lane, at + 16, at + 28), roll(x, at + 28, 1), e)
                e = jnp.where(between(lane, at + 28, at + 32), roll(zr, at + 28 - 4 * field, 1), e)
            e_ref[s] = e
        for k, d in enumerate(replicate(e)):
            ed_ref[k, s] = d

    loop(0, 16, edges, 2)

    def slopes(s):
        for i in range(3):
            v = m_ref[3 + i, s]
            s_ref[0, i, s] = slope_of(*[m_ref[3 + i, s + k] for k in (-2, -1, 1, 2)])
            s_ref[1, i, s] = slope_roll(v, 0)
            s_ref[2, i, s] = slope_roll(v, 1)
        v = ev_ref[s]
        es_ref[0, s] = slope_of(*[ev_ref[s + k] for k in (-2, -1, 1, 2)])
        es_ref[1, s] = slope_roll(v, 0)
        es_ref[2, s] = slope_roll(v, 1)

    loop(2, 14, slopes, 2)

    def along_x(sources, v_of, stores, rows):
        open_sums = {}
        for p in range(16):
            w = weights(v_of(p, rows))
            cs = [source(p, rows) for source in sources]
            for a in range(-2, 3):
                to = p + a
                if 2 <= to < 14:
                    terms = [w[a + 2] * c for c in cs]
                    had = open_sums.get(to)
                    open_sums[to] = terms if had is None else [h + t for h, t in zip(had, terms)]
            done = open_sums.pop(p - 2, None)
            if done is not None:
                for store, value in zip(stores, done):
                    store(p - 2, rows, value)

    def put(ref, *lead):
        def store(p, rows, value):
            ref[(*lead, p, rows)] = value
        return store

    def get(ref, *lead):
        return lambda p, rows: ref[(*lead, p, rows)]

    def tile_along_x(tile):
        rows = pl.ds(pl.multiple_of(8 * tile, 8), 8)
        along_x(
            [get(m_ref, i) for i in range(3)], get(m_ref, 3), [put(x_ref, i) for i in range(3)], rows
        )
        along_x([get(ec_ref)], get(ed_ref, 0), [put(ex_ref)], rows)

    def along_yz(s):
        w = weights(m_ref[4, s])
        cs = [spread(x_ref[i, s], w, 0) for i in range(3)]
        w = weights(m_ref[5, s])
        cs = [spread(c, w, 1) for c in cs]
        e = spread(ex_ref[s], weights(ed_ref[1, s]), 0)
        e = spread(e, weights(ed_ref[2, s]), 1)
        for i in range(3):
            stretch = sum(cs[j] * s_ref[j, i, s] for j in range(3))
            m_ref[i, s] = cs[i] + HALF * stretch
        parts = replicate(e)
        ec_ref[s] = e + HALF * sum(parts[j] * es_ref[j, s] for j in range(3))

    def substep(n):
        loop(0, 3, tile_along_x)
        loop(2, 14, along_yz, 2)

    loop(0, 2, substep)

    def finish(s):
        lane = lanes_of((16, 128))
        e = ec_ref[s + 4, 0:16]
        for i in range(3):
            value = jnp.where(lane < 4, roll(e, -(32 * i + 4), 1), m_ref[i, s + 4, 0:16])
            out_ref[i, s] = jnp.where(lane >= 124, roll(e, 100 - 32 * i, 1), value)

    loop(0, 8, finish, 2)


def call(kernel, outs, scratch=(), operands=0):
    smem = pl.BlockSpec(memory_space=pltpu.SMEM)
    vmem = pl.BlockSpec(memory_space=pltpu.VMEM)
    shapes = [jax.ShapeDtypeStruct(o, jnp.float32) for o in outs]
    return pl.pallas_call(
        kernel,
        out_shape=shapes,
        in_specs=[smem] + [vmem] * operands,
        out_specs=[vmem] * len(outs),
        scratch_shapes=[pltpu.VMEM(s, jnp.float32) for s in scratch],
        compiler_params=pltpu.CompilerParams(vmem_limit_bytes=16 * 1024 * 1024),
        name=kernel.__name__,
    )


def is_far(x):
    return x % 4 in (0, 3)


def solution(mesh):
    end = mesh.shape["gz"] - 1

    def across_of(x):
        return x + 1 if x % 2 else x - 1

    across = flat_pairs(mesh, lambda x, y, z: (across_of(x), y, z))
    other = flat_pairs(mesh, lambda x, y, z: (x - 1 if x % 2 else x + 1, y, z))
    y_up = flat_pairs(mesh, lambda x, y, z: (x, y + 1, z))
    y_down = flat_pairs(mesh, lambda x, y, z: (x, y - 1, z))
    z_up = flat_pairs(mesh, lambda x, y, z: (x, y, z + 1) if z < end else None)
    z_down = flat_pairs(mesh, lambda x, y, z: (x, y, z - 1) if z > 0 else None)
    ends = flat_pairs(mesh, lambda x, y, z: (x, y, end - z) if z in (0, end) else None)
    ends_other = flat_pairs(
        mesh, lambda x, y, z: (x - 1 if x % 2 else x + 1, y, z) if z in (0, end) else None
    )
    ends_across = flat_pairs(
        mesh,
        lambda x, y, z: (across_of(x), y, end - z if is_far(x) else z) if z in (0, end) else None,
    )

    def send(value, pairs):
        return lax.ppermute(value, AXES, pairs)

    def local(c, v):
        x, z = lax.axis_index("gx"), lax.axis_index("gz")
        place = jnp.stack([x % 2, (z > 0).astype(x.dtype), (z == 0).astype(x.dtype), (z == end).astype(x.dtype)])
        place = place.astype(jnp.int32)
        layers = (6, 4, 16, 128)
        edge = (4, 16, 128)
        a, b, own = call(pack_x, [layers, layers, edge], (), 2)(place, c, v)
        a = send(a, across)
        wrap = send(own, ends)
        b = send(b, other)
        wrap_b = send(wrap, ends_other)
        wrap_a = send(jnp.where((x % 4 == 0) | (x % 4 == 3), own, wrap), ends_across)
        left, right = call(pack_z, [edge, edge], (), 4)(place, c, v, a, b)
        zl = send(right, z_up)
        zr = send(left, z_down)
        down, up, zl, zr = call(pack_y, [(52, 8, 128)] * 2 + [edge] * 2, (), 9)(
            place, c, v, a, b, zl, zr, wrap, wrap_a, wrap_b
        )
        above = send(down, y_down)
        below = send(up, y_up)
        block = (16, 24, 128)
        scratch = [
            (6, *block), block, block, (3, *block), (3, *block), block, (3, 3, *block), (3, *block),
        ]
        (out,) = call(compute, [(3, 8, 16, 128)], scratch, 8)(place, c, v, a, b, zl, zr, above, below)
        return out

    placed = P(None, *AXES)
    return jax.shard_map(local, mesh=mesh, in_specs=(placed, placed), out_specs=placed, check_vma=False)
```

```python
import jax
import jax.numpy as jnp
from jax import lax
from jax.experimental import pallas as pl
from jax.experimental.pallas import tpu as pltpu
from jax.sharding import PartitionSpec as P


AXES = ("gx", "gy", "gz")
HALF = 0.5


def flat_pairs(mesh, move):
    nx, ny, nz = (mesh.shape[a] for a in AXES)
    pairs = []
    for x in range(nx):
        for y in range(ny):
            for z in range(nz):
                to = move(x, y, z)
                if to is not None:
                    tx, ty, tz = to[0] % nx, to[1] % ny, to[2] % nz
                    pairs.append(((x * ny + y) * nz + z, (tx * ny + ty) * nz + tz))
    return pairs


def lanes_of(shape):
    return lax.broadcasted_iota(jnp.int32, shape, len(shape) - 1)


def rows_of(shape):
    return lax.broadcasted_iota(jnp.int32, shape, len(shape) - 2)


def roll(x, shift, axis):
    shift = shift % x.shape[axis]
    return x if shift == 0 else pltpu.roll(x, shift, axis)


def between(index, first, last):
    return (index >= first) & (index < last)


def loop(first, last, body, unroll=1):
    def step(i, carry):
        body(i)
        return carry

    lax.fori_loop(first, last, step, 0, unroll=unroll)


def field_of(c_ref, v_ref, field):
    return (c_ref, field) if field < 3 else (v_ref, field - 3)


def pack_x(place_ref, c_ref, v_ref, ac_ref, av_ref, b_ref, edge_ref):
    high = 4 * place_ref[0]
    low = 4 - high
    shift = 4 * place_ref[1]

    def copy(q):
        for field in range(6):
            ref, i = field_of(c_ref, v_ref, field)
            to, j = field_of(ac_ref, av_ref, field)
            to[j, q] = ref[i, high + q]
            b_ref[field, q] = ref[i, low + q]
        lane = lanes_of((16, 128))
        edge = jnp.zeros((16, 128), jnp.float32)
        for g in (1, 2):
            for field in range(6):
                ref, i = field_of(c_ref, v_ref, field)
                at = 32 * g + 4 * field
                x = pltpu.roll(ref[i, 4 * (g - 1) + q], shift + at, 1)
                edge = jnp.where(between(lane, at, at + 4), x, edge)
        edge_ref[q] = edge

    loop(0, 4, copy)


def lower_upper(odd, ac_ref, av_ref, b_ref, field, q):
    ref, i = field_of(ac_ref, av_ref, field)
    a, b = ref[i, q], b_ref[field, q]
    return jnp.where(odd, b, a), jnp.where(odd, a, b)


def pack_z(place_ref, c_ref, v_ref, ac_ref, av_ref, b_ref, left_ref, right_ref):
    odd = place_ref[0] == 1

    def pack(q):
        lane = lanes_of((16, 128))
        left = jnp.zeros((16, 128), jnp.float32)
        right = left
        for field in range(6):
            ref, i = field_of(c_ref, v_ref, field)
            lo, hi = lower_upper(odd, ac_ref, av_ref, b_ref, field, q)
            for g, x in enumerate((lo, ref[i, q], ref[i, 4 + q], hi)):
                at = 32 * g + 4 * field
                here = between(lane, at, at + 4)
                left = jnp.where(here, roll(x, at, 1), left)
                right = jnp.where(here, roll(x, at + 4, 1), right)
        left_ref[q] = left
        right_ref[q] = right

    loop(0, 4, pack)


def pack_y(
    place_ref, c_ref, v_ref, ac_ref, av_ref, b_ref, zl_ref, zr_ref, wrap_ref, wrap_a_ref, wrap_b_ref,
    down_ref, up_ref, zl_out_ref, zr_out_ref,
):
    odd = place_ref[0] == 1
    first_end = place_ref[2] == 1
    last_end = place_ref[3] == 1
    upper = rows_of((8, 128)) < 4

    def join(entry, first, second):
        down_ref[entry] = jnp.where(upper, first[0:8], roll(second[0:8], 4, 0))
        up_ref[entry] = jnp.where(upper, roll(first[8:16], 4, 0), second[8:16])

    def pack(q):
        for field in range(6):
            ref, i = field_of(c_ref, v_ref, field)
            lo, hi = lower_upper(odd, ac_ref, av_ref, b_ref, field, q)
            near, far = ref[i, q], ref[i, 4 + q]
            join(8 * field + q, lo, far)
            join(8 * field + 4 + q, near, hi)
        lane = lanes_of((16, 128))
        wrap_a, wrap_b = roll(wrap_a_ref[q], 64, 1), roll(wrap_b_ref[q], 64, 1)
        lo, hi = jnp.where(odd, wrap_b, wrap_a), jnp.where(odd, wrap_a, wrap_b)
        wrap = jnp.where(lane < 32, lo, jnp.where(lane < 96, wrap_ref[q], hi))
        zl = jnp.where(first_end, wrap, zl_ref[q])
        zr = jnp.where(last_end, wrap, zr_ref[q])
        zl_out_ref[q] = zl
        zr_out_ref[q] = zr
        join(48 + q, zl, zr)

    loop(0, 4, pack)


def weights(v):
    t = HALF * jnp.abs(v)
    ahead = v > 0.0
    u = 1.0 - t
    tt = t * t
    centre = 1.0 + tt * (1.5 * t - 2.5)
    near = t * (0.5 + t * (2.0 - 1.5 * t))
    tu = -0.5 * t * u
    behind = tu * u
    far = tu * t
    return (
        jnp.where(ahead, 0.0, far),
        jnp.where(ahead, behind, near),
        centre,
        jnp.where(ahead, near, behind),
        jnp.where(ahead, far, 0.0),
    )


def spread(c, w, axis):
    near = roll(w[3] * c, 1, axis) + roll(w[1] * c, -1, axis)
    far = roll(w[4] * c, 2, axis) + roll(w[0] * c, -2, axis)
    return w[2] * c + near + far


def slope_of(two_back, back, forth, two_forth):
    return (8.0 * (forth - back) - (two_forth - two_back)) * (1.0 / 12.0)


def slope_roll(v, axis):
    return slope_of(roll(v, 2, axis), roll(v, 1, axis), roll(v, -1, axis), roll(v, -2, axis))


def replicate(e):
    lane = lanes_of(e.shape)
    up1, up2 = roll(e, 32, 1), roll(e, 64, 1)
    dn1, dn2 = roll(e, -32, 1), roll(e, -64, 1)
    first, second = lane < 32, lane < 64
    return (
        jnp.where(first, e, jnp.where(second, up1, up2)),
        jnp.where(first, dn1, jnp.where(second, e, up1)),
        jnp.where(first, dn2, jnp.where(second, dn1, e)),
    )


def compute(
    place_ref, c_ref, v_ref, ac_ref, av_ref, b_ref, zl_ref, zr_ref, above_ref, below_ref, out_ref,
    m_ref, ec_ref, ev_ref, ed_ref, x_ref, ex_ref, s_ref, es_ref,
):
    odd = place_ref[0] == 1
    upper = rows_of((8, 128)) < 4

    def halo(entry):
        above, below = above_ref[entry], below_ref[entry]
        first = jnp.where(upper, above, roll(below, 4, 0))
        return first, jnp.where(upper, roll(above, 4, 0), below)

    def widen(q):
        for field in range(6):
            ref, i = field_of(c_ref, v_ref, field)
            lo, hi = lower_upper(odd, ac_ref, av_ref, b_ref, field, q)
            m_ref[field, q, 0:16] = lo
            m_ref[field, 4 + q, 0:16] = ref[i, q]
            m_ref[field, 8 + q, 0:16] = ref[i, 4 + q]
            m_ref[field, 12 + q, 0:16] = hi
            m_ref[field, q, 16:24], m_ref[field, 8 + q, 16:24] = halo(8 * field + q)
            m_ref[field, 4 + q, 16:24], m_ref[field, 12 + q, 16:24] = halo(8 * field + 4 + q)

    loop(0, 4, widen)

    def edges(s):
        lane = lanes_of((24, 128))
        g, q = lax.shift_right_logical(s, 2), lax.bitwise_and(s, 3)
        zl_halo, zr_halo = halo(48 + q)
        zl = jnp.concatenate([zl_ref[q], zl_halo], axis=0)
        zr = jnp.concatenate([zr_ref[q], zr_halo], axis=0)
        back = 128 - 32 * g
        zl, zr = pltpu.roll(zl, back, 1), pltpu.roll(zr, back, 1)
        for kind, e_ref in ((0, ec_ref), (1, ev_ref)):
            e = jnp.zeros((24, 128), jnp.float32)
            for i in range(3):
                field = 3 * kind + i
                at = 32 * i
                x = m_ref[field, s]
                e = jnp.where(between(lane, at, at + 4), roll(zl, at - 4 * field, 1), e)
                e = jnp.where(between(lane, at + 4, at + 16), roll(x, at + 4, 1), e)
                e = jnp.where(between(lane, at + 16, at + 28), roll(x, at + 28, 1), e)
                e = jnp.where(between(lane, at + 28, at + 32), roll(zr, at + 28 - 4 * field, 1), e)
            e_ref[s] = e
        for k, d in enumerate(replicate(e)):
            ed_ref[k, s] = d

    loop(0, 16, edges, 2)

    def slopes(s):
        for i in range(3):
            v = m_ref[3 + i, s]
            s_ref[0, i, s] = slope_of(*[m_ref[3 + i, s + k] for k in (-2, -1, 1, 2)])
            s_ref[1, i, s] = slope_roll(v, 0)
            s_ref[2, i, s] = slope_roll(v, 1)
        v = ev_ref[s]
        es_ref[0, s] = slope_of(*[ev_ref[s + k] for k in (-2, -1, 1, 2)])
        es_ref[1, s] = slope_roll(v, 0)
        es_ref[2, s] = slope_roll(v, 1)

    loop(2, 14, slopes, 2)

    def along_x(sources, v_of, stores, rows):
        open_sums = {}
        for p in range(16):
            w = weights(v_of(p, rows))
            cs = [source(p, rows) for source in sources]
            for a in range(-2, 3):
                to = p + a
                if 2 <= to < 14:
                    terms = [w[a + 2] * c for c in cs]
                    had = open_sums.get(to)
                    open_sums[to] = terms if had is None else [h + t for h, t in zip(had, terms)]
            done = open_sums.pop(p - 2, None)
            if done is not None:
                for store, value in zip(stores, done):
                    store(p - 2, rows, value)

    def put(ref, *lead):
        def store(p, rows, value):
            ref[(*lead, p, rows)] = value

        return store

    def get(ref, *lead):
        return lambda p, rows: ref[(*lead, p, rows)]

    def tile_along_x(tile):
        rows = pl.ds(pl.multiple_of(8 * tile, 8), 8)
        along_x(
            [get(m_ref, i) for i in range(3)], get(m_ref, 3), [put(x_ref, i) for i in range(3)], rows
        )
        along_x([get(ec_ref)], get(ed_ref, 0), [put(ex_ref)], rows)

    def along_yz(s):
        w = weights(m_ref[4, s])
        cs = [spread(x_ref[i, s], w, 0) for i in range(3)]
        w = weights(m_ref[5, s])
        cs = [spread(c, w, 1) for c in cs]
        e = spread(ex_ref[s], weights(ed_ref[1, s]), 0)
        e = spread(e, weights(ed_ref[2, s]), 1)
        for i in range(3):
            stretch = sum(cs[j] * s_ref[j, i, s] for j in range(3))
            m_ref[i, s] = cs[i] + HALF * stretch
        parts = replicate(e)
        ec_ref[s] = e + HALF * sum(parts[j] * es_ref[j, s] for j in range(3))

    def substep(n):
        loop(0, 3, tile_along_x)
        loop(2, 14, along_yz, 2)

    loop(0, 2, substep)

    def finish(s):
        lane = lanes_of((16, 128))
        e = ec_ref[s + 4, 0:16]
        for i in range(3):
            value = jnp.where(lane < 4, roll(e, -(32 * i + 4), 1), m_ref[i, s + 4, 0:16])
            out_ref[i, s] = jnp.where(lane >= 124, roll(e, 100 - 32 * i, 1), value)

    loop(0, 8, finish, 2)


def call(kernel, outs, scratch=(), operands=0):
    smem = pl.BlockSpec(memory_space=pltpu.SMEM)
    vmem = pl.BlockSpec(memory_space=pltpu.VMEM)
    shapes = [jax.ShapeDtypeStruct(o, jnp.float32) for o in outs]
    return pl.pallas_call(
        kernel,
        out_shape=shapes,
        in_specs=[smem] + [vmem] * operands,
        out_specs=[vmem] * len(outs),
        scratch_shapes=[pltpu.VMEM(s, jnp.float32) for s in scratch],
        compiler_params=pltpu.CompilerParams(vmem_limit_bytes=16 * 1024 * 1024),
    )


def is_far(x):
    return x % 4 in (0, 3)


def solution(mesh):
    end = mesh.shape["gz"] - 1

    def across_of(x):
        return x + 1 if x % 2 else x - 1

    def other_of(x):
        return x - 1 if x % 2 else x + 1

    across = flat_pairs(mesh, lambda x, y, z: (across_of(x), y, z))
    other = flat_pairs(mesh, lambda x, y, z: (other_of(x), y, z))
    aside = flat_pairs(mesh, lambda x, y, z: (other_of(x), y, z) if is_far(x) else None)
    relay = flat_pairs(
        mesh, lambda x, y, z: None if is_far(x) else (other_of(across_of(other_of(x))), y, z)
    )
    forward = flat_pairs(mesh, lambda x, y, z: None if is_far(x) else (other_of(x), y, z))
    beside = flat_pairs(mesh, lambda x, y, z: None if is_far(x) else (across_of(x), y, z))
    y_up = flat_pairs(mesh, lambda x, y, z: (x, y + 1, z))
    y_down = flat_pairs(mesh, lambda x, y, z: (x, y - 1, z))
    z_up = flat_pairs(mesh, lambda x, y, z: (x, y, z + 1) if z < end else None)
    z_down = flat_pairs(mesh, lambda x, y, z: (x, y, z - 1) if z > 0 else None)
    ends = flat_pairs(mesh, lambda x, y, z: (x, y, end - z) if z in (0, end) else None)
    ends_other = flat_pairs(
        mesh, lambda x, y, z: (other_of(x), y, z) if z in (0, end) else None
    )
    ends_across = flat_pairs(
        mesh,
        lambda x, y, z: (across_of(x), y, end - z if is_far(x) else z) if z in (0, end) else None,
    )

    def send(value, pairs):
        return lax.ppermute(value, AXES, pairs)

    def local(c, v):
        x, z = lax.axis_index("gx"), lax.axis_index("gz")
        place = jnp.stack([x % 2, (z > 0).astype(x.dtype), (z == 0).astype(x.dtype), (z == end).astype(x.dtype)])
        place = place.astype(jnp.int32)
        far = (x % 4 == 0) | (x % 4 == 3)
        layers = (6, 4, 16, 128)
        half = (3, 4, 16, 128)
        edge = (4, 16, 128)
        ac, av, b, own = call(pack_x, [half, half, layers, edge], (), 2)(place, c, v)
        passed = send(av, aside)
        ac = send(ac, across)
        passed = send(passed, relay)
        near_av = send(av, beside)
        av = jnp.where(far, send(passed, forward), near_av)
        wrap = send(own, ends)
        b = send(b, other)
        wrap_b = send(wrap, ends_other)
        wrap_a = send(jnp.where(far, own, wrap), ends_across)
        left, right = call(pack_z, [edge, edge], (), 5)(place, c, v, ac, av, b)
        zl = send(right, z_up)
        zr = send(left, z_down)
        down, up, zl, zr = call(pack_y, [(52, 8, 128)] * 2 + [edge] * 2, (), 10)(
            place, c, v, ac, av, b, zl, zr, wrap, wrap_a, wrap_b
        )
        above = send(down, y_down)
        below = send(up, y_up)
        block = (16, 24, 128)
        scratch = [
            (6, *block), block, block, (3, *block), (3, *block), block, (3, 3, *block), (3, *block),
        ]
        (out,) = call(compute, [(3, 8, 16, 128)], scratch, 9)(place, c, v, ac, av, b, zl, zr, above, below)
        return out

    placed = P(None, *AXES)
    return jax.shard_map(local, mesh=mesh, in_specs=(placed, placed), out_specs=placed, check_vma=False)
```

```python
import jax
import jax.numpy as jnp
from jax import lax
from jax.experimental import pallas as pl
from jax.experimental.pallas import tpu as pltpu
from jax.sharding import PartitionSpec as P


AXES = ("gx", "gy", "gz")
HALF = 0.5


def flat_pairs(mesh, move):
    nx, ny, nz = (mesh.shape[a] for a in AXES)
    pairs = []
    for x in range(nx):
        for y in range(ny):
            for z in range(nz):
                to = move(x, y, z)
                if to is not None:
                    tx, ty, tz = to[0] % nx, to[1] % ny, to[2] % nz
                    pairs.append(((x * ny + y) * nz + z, (tx * ny + ty) * nz + tz))
    return pairs


def lanes_of(shape):
    return lax.broadcasted_iota(jnp.int32, shape, len(shape) - 1)


def rows_of(shape):
    return lax.broadcasted_iota(jnp.int32, shape, len(shape) - 2)


def roll(x, shift, axis):
    shift = shift % x.shape[axis]
    return x if shift == 0 else pltpu.roll(x, shift, axis)


def between(index, first, last):
    return (index >= first) & (index < last)


def loop(first, last, body, unroll=1):
    def step(i, carry):
        body(i)
        return carry

    lax.fori_loop(first, last, step, 0, unroll=unroll)


def field_of(c_ref, v_ref, field):
    return (c_ref, field) if field < 3 else (v_ref, field - 3)


def pack_x(place_ref, c_in, v_in, c_ref, v_ref, ac_ref, av_ref, b_ref, edge_ref, sems):
    fetches = [
        pltpu.make_async_copy(c_in, c_ref, sems.at[0]), pltpu.make_async_copy(v_in, v_ref, sems.at[1])
    ]
    for fetch in fetches:
        fetch.start()
    for fetch in fetches:
        fetch.wait()
    high = 4 * place_ref[0]
    low = 4 - high
    shift = 4 * place_ref[1]

    def copy(q):
        for field in range(6):
            ref, i = field_of(c_ref, v_ref, field)
            to, j = field_of(ac_ref, av_ref, field)
            to[j, q] = ref[i, high + q]
            b_ref[field, q] = ref[i, low + q]
        lane = lanes_of((16, 128))
        edge = jnp.zeros((16, 128), jnp.float32)
        for g in (1, 2):
            for field in range(6):
                ref, i = field_of(c_ref, v_ref, field)
                at = 32 * g + 4 * field
                x = pltpu.roll(ref[i, 4 * (g - 1) + q], shift + at, 1)
                edge = jnp.where(between(lane, at, at + 4), x, edge)
        edge_ref[q] = edge

    loop(0, 4, copy)


def lower_upper(odd, ac_ref, av_ref, b_ref, field, q):
    ref, i = field_of(ac_ref, av_ref, field)
    a, b = ref[i, q], b_ref[field, q]
    return jnp.where(odd, b, a), jnp.where(odd, a, b)


def pack_z(place_ref, c_ref, v_ref, ac_ref, av_ref, b_ref, left_ref, right_ref):
    odd = place_ref[0] == 1

    def pack(q):
        lane = lanes_of((16, 128))
        left = jnp.zeros((16, 128), jnp.float32)
        right = left
        for field in range(6):
            ref, i = field_of(c_ref, v_ref, field)
            lo, hi = lower_upper(odd, ac_ref, av_ref, b_ref, field, q)
            for g, x in enumerate((lo, ref[i, q], ref[i, 4 + q], hi)):
                at = 32 * g + 4 * field
                here = between(lane, at, at + 4)
                left = jnp.where(here, roll(x, at, 1), left)
                right = jnp.where(here, roll(x, at + 4, 1), right)
        left_ref[q] = left
        right_ref[q] = right

    loop(0, 4, pack)


def pack_y(
    place_ref, c_ref, v_ref, ac_ref, av_ref, b_ref, zl_ref, zr_ref, wrap_ref, wrap_a_ref, wrap_b_ref,
    down_ref, up_ref, zl_out_ref, zr_out_ref,
):
    odd = place_ref[0] == 1
    first_end = place_ref[2] == 1
    last_end = place_ref[3] == 1
    upper = rows_of((8, 128)) < 4

    def join(entry, first, second):
        down_ref[entry] = jnp.where(upper, first[0:8], roll(second[0:8], 4, 0))
        up_ref[entry] = jnp.where(upper, roll(first[8:16], 4, 0), second[8:16])

    def pack(q):
        for field in range(6):
            ref, i = field_of(c_ref, v_ref, field)
            lo, hi = lower_upper(odd, ac_ref, av_ref, b_ref, field, q)
            near, far = ref[i, q], ref[i, 4 + q]
            join(8 * field + q, lo, far)
            join(8 * field + 4 + q, near, hi)
        lane = lanes_of((16, 128))
        wrap_a, wrap_b = roll(wrap_a_ref[q], 64, 1), roll(wrap_b_ref[q], 64, 1)
        lo, hi = jnp.where(odd, wrap_b, wrap_a), jnp.where(odd, wrap_a, wrap_b)
        wrap = jnp.where(lane < 32, lo, jnp.where(lane < 96, wrap_ref[q], hi))
        zl = jnp.where(first_end, wrap, zl_ref[q])
        zr = jnp.where(last_end, wrap, zr_ref[q])
        zl_out_ref[q] = zl
        zr_out_ref[q] = zr
        join(48 + q, zl, zr)

    loop(0, 4, pack)


def weights(v):
    t = HALF * jnp.abs(v)
    ahead = v > 0.0
    u = 1.0 - t
    tt = t * t
    centre = 1.0 + tt * (1.5 * t - 2.5)
    near = t * (0.5 + t * (2.0 - 1.5 * t))
    tu = -0.5 * t * u
    behind = tu * u
    far = tu * t
    return (
        jnp.where(ahead, 0.0, far),
        jnp.where(ahead, behind, near),
        centre,
        jnp.where(ahead, near, behind),
        jnp.where(ahead, far, 0.0),
    )


def spread(c, w, axis):
    near = roll(w[3] * c, 1, axis) + roll(w[1] * c, -1, axis)
    far = roll(w[4] * c, 2, axis) + roll(w[0] * c, -2, axis)
    return w[2] * c + near + far


def slope_of(two_back, back, forth, two_forth):
    return (8.0 * (forth - back) - (two_forth - two_back)) * (1.0 / 12.0)


def slope_roll(v, axis):
    return slope_of(roll(v, 2, axis), roll(v, 1, axis), roll(v, -1, axis), roll(v, -2, axis))


def replicate(e):
    lane = lanes_of(e.shape)
    up1, up2 = roll(e, 32, 1), roll(e, 64, 1)
    dn1, dn2 = roll(e, -32, 1), roll(e, -64, 1)
    first, second = lane < 32, lane < 64
    return (
        jnp.where(first, e, jnp.where(second, up1, up2)),
        jnp.where(first, dn1, jnp.where(second, e, up1)),
        jnp.where(first, dn2, jnp.where(second, dn1, e)),
    )


def compute(
    place_ref, c_ref, v_ref, ac_ref, av_ref, b_ref, zl_ref, zr_ref, above_ref, below_ref, out_ref,
    m_ref, ec_ref, ev_ref, ed_ref, x_ref, ex_ref, s_ref, es_ref,
):
    odd = place_ref[0] == 1
    upper = rows_of((8, 128)) < 4

    def halo(entry):
        above, below = above_ref[entry], below_ref[entry]
        first = jnp.where(upper, above, roll(below, 4, 0))
        return first, jnp.where(upper, roll(above, 4, 0), below)

    def widen(q):
        for field in range(6):
            ref, i = field_of(c_ref, v_ref, field)
            lo, hi = lower_upper(odd, ac_ref, av_ref, b_ref, field, q)
            m_ref[field, q, 0:16] = lo
            m_ref[field, 4 + q, 0:16] = ref[i, q]
            m_ref[field, 8 + q, 0:16] = ref[i, 4 + q]
            m_ref[field, 12 + q, 0:16] = hi
            m_ref[field, q, 16:24], m_ref[field, 8 + q, 16:24] = halo(8 * field + q)
            m_ref[field, 4 + q, 16:24], m_ref[field, 12 + q, 16:24] = halo(8 * field + 4 + q)

    loop(0, 4, widen)

    def edges(s):
        lane = lanes_of((24, 128))
        g, q = lax.shift_right_logical(s, 2), lax.bitwise_and(s, 3)
        zl_halo, zr_halo = halo(48 + q)
        zl = jnp.concatenate([zl_ref[q], zl_halo], axis=0)
        zr = jnp.concatenate([zr_ref[q], zr_halo], axis=0)
        back = 128 - 32 * g
        zl, zr = pltpu.roll(zl, back, 1), pltpu.roll(zr, back, 1)
        for kind, e_ref in ((0, ec_ref), (1, ev_ref)):
            e = jnp.zeros((24, 128), jnp.float32)
            for i in range(3):
                field = 3 * kind + i
                at = 32 * i
                x = m_ref[field, s]
                e = jnp.where(between(lane, at, at + 4), roll(zl, at - 4 * field, 1), e)
                e = jnp.where(between(lane, at + 4, at + 16), roll(x, at + 4, 1), e)
                e = jnp.where(between(lane, at + 16, at + 28), roll(x, at + 28, 1), e)
                e = jnp.where(between(lane, at + 28, at + 32), roll(zr, at + 28 - 4 * field, 1), e)
            e_ref[s] = e
        for k, d in enumerate(replicate(e)):
            ed_ref[k, s] = d

    loop(0, 16, edges, 2)

    def slopes(s):
        for i in range(3):
            v = m_ref[3 + i, s]
            s_ref[0, i, s] = slope_of(*[m_ref[3 + i, s + k] for k in (-2, -1, 1, 2)])
            s_ref[1, i, s] = slope_roll(v, 0)
            s_ref[2, i, s] = slope_roll(v, 1)
        v = ev_ref[s]
        es_ref[0, s] = slope_of(*[ev_ref[s + k] for k in (-2, -1, 1, 2)])
        es_ref[1, s] = slope_roll(v, 0)
        es_ref[2, s] = slope_roll(v, 1)

    loop(2, 14, slopes, 2)

    def along_x(sources, v_of, stores, rows):
        open_sums = {}
        for p in range(16):
            w = weights(v_of(p, rows))
            cs = [source(p, rows) for source in sources]
            for a in range(-2, 3):
                to = p + a
                if 2 <= to < 14:
                    terms = [w[a + 2] * c for c in cs]
                    had = open_sums.get(to)
                    open_sums[to] = terms if had is None else [h + t for h, t in zip(had, terms)]
            done = open_sums.pop(p - 2, None)
            if done is not None:
                for store, value in zip(stores, done):
                    store(p - 2, rows, value)

    def put(ref, *lead):
        def store(p, rows, value):
            ref[(*lead, p, rows)] = value

        return store

    def get(ref, *lead):
        return lambda p, rows: ref[(*lead, p, rows)]

    def tile_along_x(tile):
        rows = pl.ds(pl.multiple_of(8 * tile, 8), 8)
        along_x(
            [get(m_ref, i) for i in range(3)], get(m_ref, 3), [put(x_ref, i) for i in range(3)], rows
        )
        along_x([get(ec_ref)], get(ed_ref, 0), [put(ex_ref)], rows)

    def along_yz(s):
        w = weights(m_ref[4, s])
        cs = [spread(x_ref[i, s], w, 0) for i in range(3)]
        w = weights(m_ref[5, s])
        cs = [spread(c, w, 1) for c in cs]
        e = spread(ex_ref[s], weights(ed_ref[1, s]), 0)
        e = spread(e, weights(ed_ref[2, s]), 1)
        for i in range(3):
            stretch = sum(cs[j] * s_ref[j, i, s] for j in range(3))
            m_ref[i, s] = cs[i] + HALF * stretch
        parts = replicate(e)
        ec_ref[s] = e + HALF * sum(parts[j] * es_ref[j, s] for j in range(3))

    def substep(n):
        loop(0, 3, tile_along_x)
        loop(2, 14, along_yz, 2)

    loop(0, 2, substep)

    def finish(s):
        lane = lanes_of((16, 128))
        e = ec_ref[s + 4, 0:16]
        for i in range(3):
            value = jnp.where(lane < 4, roll(e, -(32 * i + 4), 1), m_ref[i, s + 4, 0:16])
            out_ref[i, s] = jnp.where(lane >= 124, roll(e, 100 - 32 * i, 1), value)

    loop(0, 8, finish, 2)


def call(kernel, outs, scratch=(), operands=0, sems=0):
    smem = pl.BlockSpec(memory_space=pltpu.SMEM)
    vmem = pl.BlockSpec(memory_space=pltpu.VMEM)
    space = pl.BlockSpec(memory_space=pltpu.HBM) if sems else vmem
    shapes = [jax.ShapeDtypeStruct(o, jnp.float32) for o in outs]
    return pl.pallas_call(
        kernel,
        out_shape=shapes,
        in_specs=[smem] + [space] * operands,
        out_specs=[vmem] * len(outs),
        scratch_shapes=[pltpu.VMEM(s, jnp.float32) for s in scratch]
        + ([pltpu.SemaphoreType.DMA((sems,))] if sems else []),
        compiler_params=pltpu.CompilerParams(vmem_limit_bytes=16 * 1024 * 1024),
    )


def is_far(x):
    return x % 4 in (0, 3)


def solution(mesh):
    end = mesh.shape["gz"] - 1

    def across_of(x):
        return x + 1 if x % 2 else x - 1

    def other_of(x):
        return x - 1 if x % 2 else x + 1

    across = flat_pairs(mesh, lambda x, y, z: (across_of(x), y, z))
    other = flat_pairs(mesh, lambda x, y, z: (other_of(x), y, z))
    aside = flat_pairs(mesh, lambda x, y, z: (other_of(x), y, z) if is_far(x) else None)
    relay = flat_pairs(
        mesh, lambda x, y, z: None if is_far(x) else (other_of(across_of(other_of(x))), y, z)
    )
    forward = flat_pairs(mesh, lambda x, y, z: None if is_far(x) else (other_of(x), y, z))
    beside = flat_pairs(mesh, lambda x, y, z: None if is_far(x) else (across_of(x), y, z))
    y_up = flat_pairs(mesh, lambda x, y, z: (x, y + 1, z))
    y_down = flat_pairs(mesh, lambda x, y, z: (x, y - 1, z))
    z_up = flat_pairs(mesh, lambda x, y, z: (x, y, z + 1) if z < end else None)
    z_down = flat_pairs(mesh, lambda x, y, z: (x, y, z - 1) if z > 0 else None)
    ends = flat_pairs(mesh, lambda x, y, z: (x, y, end - z) if z in (0, end) else None)
    ends_other = flat_pairs(
        mesh, lambda x, y, z: (other_of(x), y, z) if z in (0, end) else None
    )
    ends_across = flat_pairs(
        mesh,
        lambda x, y, z: (across_of(x), y, end - z if is_far(x) else z) if z in (0, end) else None,
    )

    def send(value, pairs):
        return lax.ppermute(value, AXES, pairs)

    def local(c, v):
        x, z = lax.axis_index("gx"), lax.axis_index("gz")
        place = jnp.stack([x % 2, (z > 0).astype(x.dtype), (z == 0).astype(x.dtype), (z == end).astype(x.dtype)])
        place = place.astype(jnp.int32)
        far = (x % 4 == 0) | (x % 4 == 3)
        layers = (6, 4, 16, 128)
        half = (3, 4, 16, 128)
        edge = (4, 16, 128)
        own_block = (3, 8, 16, 128)
        c, v, ac, av, b, own = call(
            pack_x, [own_block, own_block, half, half, layers, edge], (), 2, 2
        )(place, c, v)
        passed = send(av, aside)
        ac = send(ac, across)
        passed = send(passed, relay)
        near_av = send(av, beside)
        av = jnp.where(far, send(passed, forward), near_av)
        wrap = send(own, ends)
        b = send(b, other)
        wrap_b = send(wrap, ends_other)
        picked = jnp.where(far, own, wrap)
        wrap_a = send(picked, ends_across)
        left, right = call(pack_z, [edge, edge], (), 5)(place, c, v, ac, av, b)
        zl = send(right, z_up)
        zr = send(left, z_down)
        down, up, zl, zr = call(pack_y, [(52, 8, 128)] * 2 + [edge] * 2, (), 10)(
            place, c, v, ac, av, b, zl, zr, wrap, wrap_a, wrap_b
        )
        above = send(down, y_down)
        below = send(up, y_up)
        block = (16, 24, 128)
        scratch = [
            (6, *block), block, block, (3, *block), (3, *block), block, (3, 3, *block), (3, *block),
        ]
        (out,) = call(compute, [(3, 8, 16, 128)], scratch, 9)(place, c, v, ac, av, b, zl, zr, above, below)
        return out

    placed = P(None, *AXES)
    return jax.shard_map(local, mesh=mesh, in_specs=(placed, placed), out_specs=placed, check_vma=False)
```

```python
import jax
import jax.numpy as jnp
from jax import lax
from jax.experimental import pallas as pl
from jax.experimental.pallas import tpu as pltpu
from jax.sharding import PartitionSpec as P


AXES = ("gx", "gy", "gz")
HALF = 0.5


def flat_pairs(mesh, move):
    nx, ny, nz = (mesh.shape[a] for a in AXES)
    pairs = []
    for x in range(nx):
        for y in range(ny):
            for z in range(nz):
                to = move(x, y, z)
                if to is not None:
                    tx, ty, tz = to[0] % nx, to[1] % ny, to[2] % nz
                    pairs.append(((x * ny + y) * nz + z, (tx * ny + ty) * nz + tz))
    return pairs


def lanes_of(shape):
    return lax.broadcasted_iota(jnp.int32, shape, len(shape) - 1)


def rows_of(shape):
    return lax.broadcasted_iota(jnp.int32, shape, len(shape) - 2)


def roll(x, shift, axis):
    shift = shift % x.shape[axis]
    return x if shift == 0 else pltpu.roll(x, shift, axis)


def between(index, first, last):
    return (index >= first) & (index < last)


def loop(first, last, body, unroll=1):
    def step(i, carry):
        body(i)
        return carry

    lax.fori_loop(first, last, step, 0, unroll=unroll)


def field_of(c_ref, v_ref, field):
    return (c_ref, field) if field < 3 else (v_ref, field - 3)


def pack_x(place_ref, c_ref, v_ref, ac_ref, av_ref, b_ref, edge_ref):
    high = 4 * place_ref[0]
    low = 4 - high
    shift = 4 * place_ref[1]

    def copy(q):
        for field in range(6):
            ref, i = field_of(c_ref, v_ref, field)
            to, j = field_of(ac_ref, av_ref, field)
            to[4 * j + q] = ref[i, high + q]
            b_ref[field, q] = ref[i, low + q]
        lane = lanes_of((16, 128))
        edge = jnp.zeros((16, 128), jnp.float32)
        for g in (1, 2):
            for field in range(6):
                ref, i = field_of(c_ref, v_ref, field)
                at = 32 * g + 4 * field
                x = pltpu.roll(ref[i, 4 * (g - 1) + q], shift + at, 1)
                edge = jnp.where(between(lane, at, at + 4), x, edge)
        edge_ref[q] = edge

    loop(0, 4, copy)
    for q in range(2):
        ac_ref[12 + q] = edge_ref[q] + roll(edge_ref[q + 2], 64, 1)


def lower_upper(odd, ac_ref, av_ref, b_ref, field, q):
    ref, i = field_of(ac_ref, av_ref, field)
    a, b = ref[4 * i + q], b_ref[field, q]
    return jnp.where(odd, b, a), jnp.where(odd, a, b)


def pack_z(
    place_ref, c_ref, v_ref, ac_ref, av_ref, b_ref, end_ref, end_a_ref, end_b_ref, left_ref, right_ref
):
    odd = place_ref[0] == 1
    first_end = place_ref[2] == 1
    last_end = place_ref[3] == 1

    def pack(q):
        lane = lanes_of((16, 128))
        left = jnp.zeros((16, 128), jnp.float32)
        right = left
        for field in range(6):
            ref, i = field_of(c_ref, v_ref, field)
            lo, hi = lower_upper(odd, ac_ref, av_ref, b_ref, field, q)
            for g, x in enumerate((lo, ref[i, q], ref[i, 4 + q], hi)):
                at = 32 * g + 4 * field
                here = between(lane, at, at + 4)
                left = jnp.where(here, roll(x, at, 1), left)
                right = jnp.where(here, roll(x, at + 4, 1), right)
        turn = 64 * lax.shift_right_logical(q, 1)
        base, a, b = (
            pltpu.roll(ref[lax.bitwise_and(q, 1)], turn, 1) for ref in (end_ref, end_a_ref, end_b_ref)
        )
        a, b = roll(a, 64, 1), roll(b, 64, 1)
        lo, hi = jnp.where(odd, a, b), jnp.where(odd, b, a)
        end = jnp.where(lane < 32, lo, jnp.where(lane < 96, base, hi))
        left_ref[q] = jnp.where(first_end, end, left)
        right_ref[q] = jnp.where(last_end, end, right)

    loop(0, 4, pack)


def pack_y(
    place_ref, c_ref, v_ref, ac_ref, av_ref, b_ref, zl_ref, zr_ref, down_ref, up_ref
):
    odd = place_ref[0] == 1
    upper = rows_of((8, 128)) < 4

    def join(entry, first, second):
        down_ref[entry] = jnp.where(upper, first[0:8], roll(second[0:8], 4, 0))
        up_ref[entry] = jnp.where(upper, roll(first[8:16], 4, 0), second[8:16])

    def pack(q):
        for field in range(6):
            ref, i = field_of(c_ref, v_ref, field)
            lo, hi = lower_upper(odd, ac_ref, av_ref, b_ref, field, q)
            near, far = ref[i, q], ref[i, 4 + q]
            join(8 * field + q, lo, far)
            join(8 * field + 4 + q, near, hi)
        join(48 + q, zl_ref[q], zr_ref[q])

    loop(0, 4, pack)


def weights(v):
    t = HALF * jnp.abs(v)
    ahead = v > 0.0
    u = 1.0 - t
    tt = t * t
    centre = 1.0 + tt * (1.5 * t - 2.5)
    near = t * (0.5 + t * (2.0 - 1.5 * t))
    tu = -0.5 * t * u
    behind = tu * u
    far = tu * t
    return (
        jnp.where(ahead, 0.0, far),
        jnp.where(ahead, behind, near),
        centre,
        jnp.where(ahead, near, behind),
        jnp.where(ahead, far, 0.0),
    )


def spread(c, w, axis):
    near = roll(w[3] * c, 1, axis) + roll(w[1] * c, -1, axis)
    far = roll(w[4] * c, 2, axis) + roll(w[0] * c, -2, axis)
    return w[2] * c + near + far


def slope_of(two_back, back, forth, two_forth):
    return (8.0 * (forth - back) - (two_forth - two_back)) * (1.0 / 12.0)


def slope_roll(v, axis):
    return slope_of(roll(v, 2, axis), roll(v, 1, axis), roll(v, -1, axis), roll(v, -2, axis))


def replicate(e):
    lane = lanes_of(e.shape)
    up1, up2 = roll(e, 32, 1), roll(e, 64, 1)
    dn1, dn2 = roll(e, -32, 1), roll(e, -64, 1)
    first, second = lane < 32, lane < 64
    return (
        jnp.where(first, e, jnp.where(second, up1, up2)),
        jnp.where(first, dn1, jnp.where(second, e, up1)),
        jnp.where(first, dn2, jnp.where(second, dn1, e)),
    )


def compute(
    place_ref, c_ref, v_ref, ac_ref, av_ref, b_ref, zl_ref, zr_ref, above_ref, below_ref, out_ref,
    m_ref, ec_ref, ev_ref, ed_ref, x_ref, ex_ref, s_ref, es_ref,
):
    odd = place_ref[0] == 1
    upper = rows_of((8, 128)) < 4

    def halo(entry):
        above, below = above_ref[entry], below_ref[entry]
        first = jnp.where(upper, above, roll(below, 4, 0))
        return first, jnp.where(upper, roll(above, 4, 0), below)

    def widen(q):
        for field in range(6):
            ref, i = field_of(c_ref, v_ref, field)
            lo, hi = lower_upper(odd, ac_ref, av_ref, b_ref, field, q)
            m_ref[field, q, 0:16] = lo
            m_ref[field, 4 + q, 0:16] = ref[i, q]
            m_ref[field, 8 + q, 0:16] = ref[i, 4 + q]
            m_ref[field, 12 + q, 0:16] = hi
            m_ref[field, q, 16:24], m_ref[field, 8 + q, 16:24] = halo(8 * field + q)
            m_ref[field, 4 + q, 16:24], m_ref[field, 12 + q, 16:24] = halo(8 * field + 4 + q)

    loop(0, 4, widen)

    def edges(s):
        lane = lanes_of((24, 128))
        g, q = lax.shift_right_logical(s, 2), lax.bitwise_and(s, 3)
        zl_halo, zr_halo = halo(48 + q)
        zl = jnp.concatenate([zl_ref[q], zl_halo], axis=0)
        zr = jnp.concatenate([zr_ref[q], zr_halo], axis=0)
        back = 128 - 32 * g
        zl, zr = pltpu.roll(zl, back, 1), pltpu.roll(zr, back, 1)
        for kind, e_ref in ((0, ec_ref), (1, ev_ref)):
            e = jnp.zeros((24, 128), jnp.float32)
            for i in range(3):
                field = 3 * kind + i
                at = 32 * i
                x = m_ref[field, s]
                e = jnp.where(between(lane, at, at + 4), roll(zl, at - 4 * field, 1), e)
                e = jnp.where(between(lane, at + 4, at + 16), roll(x, at + 4, 1), e)
                e = jnp.where(between(lane, at + 16, at + 28), roll(x, at + 28, 1), e)
                e = jnp.where(between(lane, at + 28, at + 32), roll(zr, at + 28 - 4 * field, 1), e)
            e_ref[s] = e
        for k, d in enumerate(replicate(e)):
            ed_ref[k, s] = d

    loop(0, 16, edges, 2)

    def slopes(s):
        for i in range(3):
            v = m_ref[3 + i, s]
            s_ref[0, i, s] = slope_of(*[m_ref[3 + i, s + k] for k in (-2, -1, 1, 2)])
            s_ref[1, i, s] = slope_roll(v, 0)
            s_ref[2, i, s] = slope_roll(v, 1)
        v = ev_ref[s]
        es_ref[0, s] = slope_of(*[ev_ref[s + k] for k in (-2, -1, 1, 2)])
        es_ref[1, s] = slope_roll(v, 0)
        es_ref[2, s] = slope_roll(v, 1)

    loop(2, 14, slopes, 2)

    def along_x(sources, v_of, stores, rows):
        open_sums = {}
        for p in range(16):
            w = weights(v_of(p, rows))
            cs = [source(p, rows) for source in sources]
            for a in range(-2, 3):
                to = p + a
                if 2 <= to < 14:
                    terms = [w[a + 2] * c for c in cs]
                    had = open_sums.get(to)
                    open_sums[to] = terms if had is None else [h + t for h, t in zip(had, terms)]
            done = open_sums.pop(p - 2, None)
            if done is not None:
                for store, value in zip(stores, done):
                    store(p - 2, rows, value)

    def put(ref, *lead):
        def store(p, rows, value):
            ref[(*lead, p, rows)] = value

        return store

    def get(ref, *lead):
        return lambda p, rows: ref[(*lead, p, rows)]

    def tile_along_x(tile):
        rows = pl.ds(pl.multiple_of(8 * tile, 8), 8)
        along_x(
            [get(m_ref, i) for i in range(3)], get(m_ref, 3), [put(x_ref, i) for i in range(3)], rows
        )
        along_x([get(ec_ref)], get(ed_ref, 0), [put(ex_ref)], rows)

    def along_yz(s):
        w = weights(m_ref[4, s])
        cs = [spread(x_ref[i, s], w, 0) for i in range(3)]
        w = weights(m_ref[5, s])
        cs = [spread(c, w, 1) for c in cs]
        e = spread(ex_ref[s], weights(ed_ref[1, s]), 0)
        e = spread(e, weights(ed_ref[2, s]), 1)
        for i in range(3):
            stretch = sum(cs[j] * s_ref[j, i, s] for j in range(3))
            m_ref[i, s] = cs[i] + HALF * stretch
        parts = replicate(e)
        ec_ref[s] = e + HALF * sum(parts[j] * es_ref[j, s] for j in range(3))

    def substep(n):
        loop(0, 3, tile_along_x)
        loop(2, 14, along_yz, 2)

    loop(0, 2, substep)

    def finish(s):
        lane = lanes_of((16, 128))
        e = ec_ref[s + 4, 0:16]
        for i in range(3):
            value = jnp.where(lane < 4, roll(e, -(32 * i + 4), 1), m_ref[i, s + 4, 0:16])
            out_ref[i, s] = jnp.where(lane >= 124, roll(e, 100 - 32 * i, 1), value)

    loop(0, 8, finish, 2)


def call(kernel, outs, scratch=(), operands=0):
    smem = pl.BlockSpec(memory_space=pltpu.SMEM)
    vmem = pl.BlockSpec(memory_space=pltpu.VMEM)
    shapes = [jax.ShapeDtypeStruct(o, jnp.float32) for o in outs]
    return pl.pallas_call(
        kernel,
        out_shape=shapes,
        in_specs=[smem] + [vmem] * operands,
        out_specs=[vmem] * len(outs),
        scratch_shapes=[pltpu.VMEM(s, jnp.float32) for s in scratch],
        compiler_params=pltpu.CompilerParams(vmem_limit_bytes=16 * 1024 * 1024),
    )


def is_far(x):
    return x % 4 in (0, 3)


def solution(mesh):
    end = mesh.shape["gz"] - 1

    def across_of(x):
        return x + 1 if x % 2 else x - 1

    def other_of(x):
        return x - 1 if x % 2 else x + 1

    across = flat_pairs(mesh, lambda x, y, z: (across_of(x), y, z))
    other = flat_pairs(mesh, lambda x, y, z: (other_of(x), y, z))
    aside = flat_pairs(mesh, lambda x, y, z: (other_of(x), y, z) if is_far(x) else None)
    relay = flat_pairs(
        mesh, lambda x, y, z: None if is_far(x) else (other_of(across_of(other_of(x))), y, z)
    )
    beside = flat_pairs(mesh, lambda x, y, z: None if is_far(x) else (across_of(x), y, z))
    y_up = flat_pairs(mesh, lambda x, y, z: (x, y + 1, z))
    y_down = flat_pairs(mesh, lambda x, y, z: (x, y - 1, z))
    last_x = mesh.shape["gx"] - 1
    z_up = flat_pairs(mesh, lambda x, y, z: (x if z < end else last_x - x, y, z + 1))
    z_down = flat_pairs(mesh, lambda x, y, z: (x if z > 0 else last_x - x, y, z - 1))

    def send(value, pairs):
        return lax.ppermute(value, AXES, pairs)

    def local(c, v):
        x, z = lax.axis_index("gx"), lax.axis_index("gz")
        place = jnp.stack([x % 2, (z > 0).astype(x.dtype), (z == 0).astype(x.dtype), (z == end).astype(x.dtype)])
        place = place.astype(jnp.int32)
        far = (x % 4 == 0) | (x % 4 == 3)
        layers = (6, 4, 16, 128)
        edge = (4, 16, 128)
        ac, av, b, _ = call(pack_x, [(14, 16, 128), (12, 16, 128), layers, edge], (), 2)(place, c, v)
        own_end = ac[12:]
        passed = send(av, aside)
        ac = send(ac, across)
        passed = send(jnp.concatenate([passed, own_end]), relay)
        near_av = send(av, beside)
        b = send(b, other)
        held = jnp.where(far, ac, passed)
        forwarded = send(held, other)
        end_a = jnp.where(far, own_end, send(passed[12:], beside))
        av = jnp.where(far, forwarded[:12], near_av)
        left, right = call(pack_z, [edge, edge], (), 8)(
            place, c, v, ac, av, b, held[12:], end_a, forwarded[12:]
        )
        zl = send(right, z_up)
        zr = send(left, z_down)
        down, up = call(pack_y, [(52, 8, 128)] * 2, (), 7)(place, c, v, ac, av, b, zl, zr)
        above = send(down, y_down)
        below = send(up, y_up)
        block = (16, 24, 128)
        scratch = [
            (6, *block), block, block, (3, *block), (3, *block), block, (3, 3, *block), (3, *block),
        ]
        (out,) = call(compute, [(3, 8, 16, 128)], scratch, 9)(place, c, v, ac, av, b, zl, zr, above, below)
        return out

    placed = P(None, *AXES)
    return jax.shard_map(local, mesh=mesh, in_specs=(placed, placed), out_specs=placed, check_vma=False)
```

```python
import jax
import jax.numpy as jnp
from jax import lax
from jax.experimental import pallas as pl
from jax.experimental.pallas import tpu as pltpu
from jax.sharding import PartitionSpec as P


AXES = ("gx", "gy", "gz")
HALF = 0.5
DIRECT = 4
STRIPS = 4 * DIRECT
RELAYED = 24 - STRIPS


def flat_pairs(mesh, move):
    nx, ny, nz = (mesh.shape[a] for a in AXES)
    pairs = []
    for x in range(nx):
        for y in range(ny):
            for z in range(nz):
                to = move(x, y, z)
                if to is not None:
                    tx, ty, tz = to[0] % nx, to[1] % ny, to[2] % nz
                    pairs.append(((x * ny + y) * nz + z, (tx * ny + ty) * nz + tz))
    return pairs


def lanes_of(shape):
    return lax.broadcasted_iota(jnp.int32, shape, len(shape) - 1)


def rows_of(shape):
    return lax.broadcasted_iota(jnp.int32, shape, len(shape) - 2)


def roll(x, shift, axis):
    shift = shift % x.shape[axis]
    return x if shift == 0 else pltpu.roll(x, shift, axis)


def between(index, first, last):
    return (index >= first) & (index < last)


def loop(first, last, body, unroll=1):
    def step(i, carry):
        body(i)
        return carry

    lax.fori_loop(first, last, step, 0, unroll=unroll)


def field_of(c_ref, v_ref, field):
    return (c_ref, field) if field < 3 else (v_ref, field - 3)


def across_field(ac_ref, av_ref, field):
    return (ac_ref, field) if field < DIRECT else (av_ref, field - DIRECT)


def pack_x(place_ref, c_ref, v_ref, ac_ref, av_ref, b_ref, edge_ref):
    high = 4 * place_ref[0]
    low = 4 - high
    shift = 4 * place_ref[1]

    def copy(q):
        for field in range(6):
            ref, i = field_of(c_ref, v_ref, field)
            to, j = across_field(ac_ref, av_ref, field)
            to[4 * j + q] = ref[i, high + q]
            b_ref[field, q] = ref[i, low + q]
        lane = lanes_of((16, 128))
        edge = jnp.zeros((16, 128), jnp.float32)
        for g in (1, 2):
            for field in range(6):
                ref, i = field_of(c_ref, v_ref, field)
                at = 32 * g + 4 * field
                x = pltpu.roll(ref[i, 4 * (g - 1) + q], shift + at, 1)
                edge = jnp.where(between(lane, at, at + 4), x, edge)
        edge_ref[q] = edge

    loop(0, 4, copy)
    for q in range(2):
        ac_ref[STRIPS + q] = edge_ref[q] + roll(edge_ref[q + 2], 64, 1)


def lower_upper(odd, ac_ref, av_ref, b_ref, field, q):
    ref, i = across_field(ac_ref, av_ref, field)
    a, b = ref[4 * i + q], b_ref[field, q]
    return jnp.where(odd, b, a), jnp.where(odd, a, b)


def pack_z(
    place_ref, c_ref, v_ref, ac_ref, av_ref, b_ref, end_ref, end_a_ref, end_b_ref, left_ref, right_ref
):
    odd = place_ref[0] == 1
    first_end = place_ref[2] == 1
    last_end = place_ref[3] == 1

    def pack(q):
        lane = lanes_of((16, 128))
        left = jnp.zeros((16, 128), jnp.float32)
        right = left
        for field in range(6):
            ref, i = field_of(c_ref, v_ref, field)
            lo, hi = lower_upper(odd, ac_ref, av_ref, b_ref, field, q)
            for g, x in enumerate((lo, ref[i, q], ref[i, 4 + q], hi)):
                at = 32 * g + 4 * field
                here = between(lane, at, at + 4)
                left = jnp.where(here, roll(x, at, 1), left)
                right = jnp.where(here, roll(x, at + 4, 1), right)
        turn = 64 * lax.shift_right_logical(q, 1)
        base, a, b = (
            pltpu.roll(ref[lax.bitwise_and(q, 1)], turn, 1) for ref in (end_ref, end_a_ref, end_b_ref)
        )
        a, b = roll(a, 64, 1), roll(b, 64, 1)
        lo, hi = jnp.where(odd, a, b), jnp.where(odd, b, a)
        end = jnp.where(lane < 32, lo, jnp.where(lane < 96, base, hi))
        left_ref[q] = jnp.where(first_end, end, left)
        right_ref[q] = jnp.where(last_end, end, right)

    loop(0, 4, pack)


def pack_y(
    place_ref, c_ref, v_ref, ac_ref, av_ref, b_ref, zl_ref, zr_ref, down_ref, up_ref
):
    odd = place_ref[0] == 1
    upper = rows_of((8, 128)) < 4

    def join(entry, first, second):
        down_ref[entry] = jnp.where(upper, first[0:8], roll(second[0:8], 4, 0))
        up_ref[entry] = jnp.where(upper, roll(first[8:16], 4, 0), second[8:16])

    def pack(q):
        for field in range(6):
            ref, i = field_of(c_ref, v_ref, field)
            lo, hi = lower_upper(odd, ac_ref, av_ref, b_ref, field, q)
            near, far = ref[i, q], ref[i, 4 + q]
            join(8 * field + q, lo, far)
            join(8 * field + 4 + q, near, hi)
        join(48 + q, zl_ref[q], zr_ref[q])

    loop(0, 4, pack)


def weights(v):
    t = HALF * jnp.abs(v)
    ahead = v > 0.0
    u = 1.0 - t
    tt = t * t
    centre = 1.0 + tt * (1.5 * t - 2.5)
    near = t * (0.5 + t * (2.0 - 1.5 * t))
    tu = -0.5 * t * u
    behind = tu * u
    far = tu * t
    return (
        jnp.where(ahead, 0.0, far),
        jnp.where(ahead, behind, near),
        centre,
        jnp.where(ahead, near, behind),
        jnp.where(ahead, far, 0.0),
    )


def spread(c, w, axis):
    near = roll(w[3] * c, 1, axis) + roll(w[1] * c, -1, axis)
    far = roll(w[4] * c, 2, axis) + roll(w[0] * c, -2, axis)
    return w[2] * c + near + far


def slope_of(two_back, back, forth, two_forth):
    return (8.0 * (forth - back) - (two_forth - two_back)) * (1.0 / 12.0)


def slope_roll(v, axis):
    return slope_of(roll(v, 2, axis), roll(v, 1, axis), roll(v, -1, axis), roll(v, -2, axis))


def replicate(e):
    lane = lanes_of(e.shape)
    up1, up2 = roll(e, 32, 1), roll(e, 64, 1)
    dn1, dn2 = roll(e, -32, 1), roll(e, -64, 1)
    first, second = lane < 32, lane < 64
    return (
        jnp.where(first, e, jnp.where(second, up1, up2)),
        jnp.where(first, dn1, jnp.where(second, e, up1)),
        jnp.where(first, dn2, jnp.where(second, dn1, e)),
    )


def compute(
    place_ref, c_ref, v_ref, ac_ref, av_ref, b_ref, zl_ref, zr_ref, above_ref, below_ref, out_ref,
    m_ref, ec_ref, ev_ref, ed_ref, x_ref, ex_ref, s_ref, es_ref,
):
    odd = place_ref[0] == 1
    upper = rows_of((8, 128)) < 4

    def halo(entry):
        above, below = above_ref[entry], below_ref[entry]
        first = jnp.where(upper, above, roll(below, 4, 0))
        return first, jnp.where(upper, roll(above, 4, 0), below)

    def widen(q):
        for field in range(6):
            ref, i = field_of(c_ref, v_ref, field)
            lo, hi = lower_upper(odd, ac_ref, av_ref, b_ref, field, q)
            m_ref[field, q, 0:16] = lo
            m_ref[field, 4 + q, 0:16] = ref[i, q]
            m_ref[field, 8 + q, 0:16] = ref[i, 4 + q]
            m_ref[field, 12 + q, 0:16] = hi
            m_ref[field, q, 16:24], m_ref[field, 8 + q, 16:24] = halo(8 * field + q)
            m_ref[field, 4 + q, 16:24], m_ref[field, 12 + q, 16:24] = halo(8 * field + 4 + q)

    loop(0, 4, widen)

    def edges(s):
        lane = lanes_of((24, 128))
        g, q = lax.shift_right_logical(s, 2), lax.bitwise_and(s, 3)
        zl_halo, zr_halo = halo(48 + q)
        zl = jnp.concatenate([zl_ref[q], zl_halo], axis=0)
        zr = jnp.concatenate([zr_ref[q], zr_halo], axis=0)
        back = 128 - 32 * g
        zl, zr = pltpu.roll(zl, back, 1), pltpu.roll(zr, back, 1)
        for kind, e_ref in ((0, ec_ref), (1, ev_ref)):
            e = jnp.zeros((24, 128), jnp.float32)
            for i in range(3):
                field = 3 * kind + i
                at = 32 * i
                x = m_ref[field, s]
                e = jnp.where(between(lane, at, at + 4), roll(zl, at - 4 * field, 1), e)
                e = jnp.where(between(lane, at + 4, at + 16), roll(x, at + 4, 1), e)
                e = jnp.where(between(lane, at + 16, at + 28), roll(x, at + 28, 1), e)
                e = jnp.where(between(lane, at + 28, at + 32), roll(zr, at + 28 - 4 * field, 1), e)
            e_ref[s] = e
        for k, d in enumerate(replicate(e)):
            ed_ref[k, s] = d

    loop(0, 16, edges, 2)

    def slopes(s):
        for i in range(3):
            v = m_ref[3 + i, s]
            s_ref[0, i, s] = slope_of(*[m_ref[3 + i, s + k] for k in (-2, -1, 1, 2)])
            s_ref[1, i, s] = slope_roll(v, 0)
            s_ref[2, i, s] = slope_roll(v, 1)
        v = ev_ref[s]
        es_ref[0, s] = slope_of(*[ev_ref[s + k] for k in (-2, -1, 1, 2)])
        es_ref[1, s] = slope_roll(v, 0)
        es_ref[2, s] = slope_roll(v, 1)

    loop(2, 14, slopes, 2)

    def along_x(sources, v_of, stores, rows):
        open_sums = {}
        for p in range(16):
            w = weights(v_of(p, rows))
            cs = [source(p, rows) for source in sources]
            for a in range(-2, 3):
                to = p + a
                if 2 <= to < 14:
                    terms = [w[a + 2] * c for c in cs]
                    had = open_sums.get(to)
                    open_sums[to] = terms if had is None else [h + t for h, t in zip(had, terms)]
            done = open_sums.pop(p - 2, None)
            if done is not None:
                for store, value in zip(stores, done):
                    store(p - 2, rows, value)

    def put(ref, *lead):
        def store(p, rows, value):
            ref[(*lead, p, rows)] = value

        return store

    def get(ref, *lead):
        return lambda p, rows: ref[(*lead, p, rows)]

    def tile_along_x(tile):
        rows = pl.ds(pl.multiple_of(8 * tile, 8), 8)
        along_x(
            [get(m_ref, i) for i in range(3)], get(m_ref, 3), [put(x_ref, i) for i in range(3)], rows
        )
        along_x([get(ec_ref)], get(ed_ref, 0), [put(ex_ref)], rows)

    def along_yz(s):
        w = weights(m_ref[4, s])
        cs = [spread(x_ref[i, s], w, 0) for i in range(3)]
        w = weights(m_ref[5, s])
        cs = [spread(c, w, 1) for c in cs]
        e = spread(ex_ref[s], weights(ed_ref[1, s]), 0)
        e = spread(e, weights(ed_ref[2, s]), 1)
        for i in range(3):
            stretch = sum(cs[j] * s_ref[j, i, s] for j in range(3))
            m_ref[i, s] = cs[i] + HALF * stretch
        parts = replicate(e)
        ec_ref[s] = e + HALF * sum(parts[j] * es_ref[j, s] for j in range(3))

    def substep(n):
        loop(0, 3, tile_along_x)
        loop(2, 14, along_yz, 2)

    loop(0, 2, substep)

    def finish(s):
        lane = lanes_of((16, 128))
        e = ec_ref[s + 4, 0:16]
        for i in range(3):
            value = jnp.where(lane < 4, roll(e, -(32 * i + 4), 1), m_ref[i, s + 4, 0:16])
            out_ref[i, s] = jnp.where(lane >= 124, roll(e, 100 - 32 * i, 1), value)

    loop(0, 8, finish, 2)


def call(kernel, outs, scratch=(), operands=0):
    smem = pl.BlockSpec(memory_space=pltpu.SMEM)
    vmem = pl.BlockSpec(memory_space=pltpu.VMEM)
    shapes = [jax.ShapeDtypeStruct(o, jnp.float32) for o in outs]
    return pl.pallas_call(
        kernel,
        out_shape=shapes,
        in_specs=[smem] + [vmem] * operands,
        out_specs=[vmem] * len(outs),
        scratch_shapes=[pltpu.VMEM(s, jnp.float32) for s in scratch],
        compiler_params=pltpu.CompilerParams(vmem_limit_bytes=16 * 1024 * 1024),
    )


def is_far(x):
    return x % 4 in (0, 3)


def solution(mesh):
    end = mesh.shape["gz"] - 1

    def across_of(x):
        return x + 1 if x % 2 else x - 1

    def other_of(x):
        return x - 1 if x % 2 else x + 1

    across = flat_pairs(mesh, lambda x, y, z: (across_of(x), y, z))
    other = flat_pairs(mesh, lambda x, y, z: (other_of(x), y, z))
    aside = flat_pairs(mesh, lambda x, y, z: (other_of(x), y, z) if is_far(x) else None)
    relay = flat_pairs(
        mesh, lambda x, y, z: None if is_far(x) else (other_of(across_of(other_of(x))), y, z)
    )
    beside = flat_pairs(mesh, lambda x, y, z: None if is_far(x) else (across_of(x), y, z))
    y_up = flat_pairs(mesh, lambda x, y, z: (x, y + 1, z))
    y_down = flat_pairs(mesh, lambda x, y, z: (x, y - 1, z))
    last_x = mesh.shape["gx"] - 1
    z_up = flat_pairs(mesh, lambda x, y, z: (x if z < end else last_x - x, y, z + 1))
    z_down = flat_pairs(mesh, lambda x, y, z: (x if z > 0 else last_x - x, y, z - 1))

    def send(value, pairs):
        return lax.ppermute(value, AXES, pairs)

    def local(c, v):
        x, z = lax.axis_index("gx"), lax.axis_index("gz")
        place = jnp.stack([x % 2, (z > 0).astype(x.dtype), (z == 0).astype(x.dtype), (z == end).astype(x.dtype)])
        place = place.astype(jnp.int32)
        far = (x % 4 == 0) | (x % 4 == 3)
        layers = (6, 4, 16, 128)
        edge = (4, 16, 128)
        shapes = [(STRIPS + 2, 16, 128), (RELAYED, 16, 128), layers, edge]
        ac, av, b, _ = call(pack_x, shapes, (), 2)(place, c, v)
        own_end = ac[STRIPS:]
        passed = send(av, aside)
        ac = send(ac, across)
        passed = send(jnp.concatenate([passed, own_end]), relay)
        near_av = send(av, beside)
        b = send(b, other)
        held = jnp.where(far, ac[STRIPS - RELAYED :], passed)
        forwarded = send(held, other)
        end_a = jnp.where(far, own_end, send(passed[RELAYED:], beside))
        av = jnp.where(far, forwarded[:RELAYED], near_av)
        left, right = call(pack_z, [edge, edge], (), 8)(
            place, c, v, ac, av, b, held[RELAYED:], end_a, forwarded[RELAYED:]
        )
        zl = send(right, z_up)
        zr = send(left, z_down)
        down, up = call(pack_y, [(52, 8, 128)] * 2, (), 7)(place, c, v, ac, av, b, zl, zr)
        above = send(down, y_down)
        below = send(up, y_up)
        block = (16, 24, 128)
        scratch = [
            (6, *block), block, block, (3, *block), (3, *block), block, (3, 3, *block), (3, *block),
        ]
        (out,) = call(compute, [(3, 8, 16, 128)], scratch, 9)(place, c, v, ac, av, b, zl, zr, above, below)
        return out

    placed = P(None, *AXES)
    return jax.shard_map(local, mesh=mesh, in_specs=(placed, placed), out_specs=placed, check_vma=False)
```

```python
import jax
import jax.numpy as jnp
from jax import lax
from jax.experimental import pallas as pl
from jax.experimental.pallas import tpu as pltpu
from jax.sharding import PartitionSpec as P


AXES = ("gx", "gy", "gz")
HALF = 0.5


def flat_pairs(mesh, move):
    nx, ny, nz = (mesh.shape[a] for a in AXES)
    pairs = []
    for x in range(nx):
        for y in range(ny):
            for z in range(nz):
                to = move(x, y, z)
                if to is not None:
                    tx, ty, tz = to[0] % nx, to[1] % ny, to[2] % nz
                    pairs.append(((x * ny + y) * nz + z, (tx * ny + ty) * nz + tz))
    return pairs


def lanes_of(shape):
    return lax.broadcasted_iota(jnp.int32, shape, len(shape) - 1)


def rows_of(shape):
    return lax.broadcasted_iota(jnp.int32, shape, len(shape) - 2)


def roll(x, shift, axis):
    shift = shift % x.shape[axis]
    return x if shift == 0 else pltpu.roll(x, shift, axis)


def between(index, first, last):
    return (index >= first) & (index < last)


def loop(first, last, body, unroll=1):
    def step(i, carry):
        body(i)
        return carry

    lax.fori_loop(first, last, step, 0, unroll=unroll)


def field_of(c_ref, v_ref, field):
    return (c_ref, field) if field < 3 else (v_ref, field - 3)


def pack_x(place_ref, c_ref, v_ref, ac_ref, av_ref, b_ref, edge_ref):
    high = 4 * place_ref[0]
    low = 4 - high
    shift = 4 * place_ref[1]

    def copy(q):
        for field in range(6):
            ref, i = field_of(c_ref, v_ref, field)
            to, j = field_of(ac_ref, av_ref, field)
            to[4 * j + q] = ref[i, high + q]
            b_ref[field, q] = ref[i, low + q]
        lane = lanes_of((16, 128))
        edge = jnp.zeros((16, 128), jnp.float32)
        for g in (1, 2):
            for field in range(6):
                ref, i = field_of(c_ref, v_ref, field)
                at = 32 * g + 4 * field
                x = pltpu.roll(ref[i, 4 * (g - 1) + q], shift + at, 1)
                edge = jnp.where(between(lane, at, at + 4), x, edge)
        edge_ref[q] = edge

    loop(0, 4, copy)
    for q in range(2):
        ac_ref[12 + q] = edge_ref[q] + roll(edge_ref[q + 2], 64, 1)


def lower_upper(odd, ac_ref, av_ref, b_ref, field, q):
    ref, i = field_of(ac_ref, av_ref, field)
    a, b = ref[4 * i + q], b_ref[field, q]
    return jnp.where(odd, b, a), jnp.where(odd, a, b)


def pack_z(
    place_ref, c_ref, v_ref, ac_ref, av_ref, b_ref, end_ref, end_a_ref, end_b_ref, left_ref, right_ref
):
    odd = place_ref[0] == 1
    first_end = place_ref[2] == 1
    last_end = place_ref[3] == 1

    def pack(q):
        lane = lanes_of((16, 128))
        left = jnp.zeros((16, 128), jnp.float32)
        right = left
        for field in range(6):
            ref, i = field_of(c_ref, v_ref, field)
            lo, hi = lower_upper(odd, ac_ref, av_ref, b_ref, field, q)
            for g, x in enumerate((lo, ref[i, q], ref[i, 4 + q], hi)):
                at = 32 * g + 4 * field
                here = between(lane, at, at + 4)
                left = jnp.where(here, roll(x, at, 1), left)
                right = jnp.where(here, roll(x, at + 4, 1), right)
        turn = 64 * lax.shift_right_logical(q, 1)
        base, a, b = (
            pltpu.roll(ref[lax.bitwise_and(q, 1)], turn, 1) for ref in (end_ref, end_a_ref, end_b_ref)
        )
        a, b = roll(a, 64, 1), roll(b, 64, 1)
        lo, hi = jnp.where(odd, a, b), jnp.where(odd, b, a)
        end = jnp.where(lane < 32, lo, jnp.where(lane < 96, base, hi))
        left_ref[q] = jnp.where(first_end, end, left)
        right_ref[q] = jnp.where(last_end, end, right)

    loop(0, 4, pack)


def join(down_ref, up_ref, entry, first, second):
    upper = rows_of((8, 128)) < 4
    down_ref[entry] = jnp.where(upper, first[0:8], roll(second[0:8], 4, 0))
    up_ref[entry] = jnp.where(upper, roll(first[8:16], 4, 0), second[8:16])


def halo(above_ref, below_ref, entry):
    upper = rows_of((8, 128)) < 4
    above, below = above_ref[entry], below_ref[entry]
    first = jnp.where(upper, above, roll(below, 4, 0))
    return first, jnp.where(upper, roll(above, 4, 0), below)


def pack_y_early(place_ref, c_ref, v_ref, b_ref, down_ref, up_ref):
    for field in range(6):
        ref, i = field_of(c_ref, v_ref, field)

        def own(q):
            join(down_ref, up_ref, 6 * field + q, ref[i, q], ref[i, 4 + q])

        def side(q):
            join(down_ref, up_ref, 6 * field + 4 + q, b_ref[field, q], b_ref[field, 2 + q])

        loop(0, 4, own)
        loop(0, 2, side)


def pack_y_late(place_ref, ac_ref, av_ref, zl_ref, zr_ref, down_ref, up_ref):
    def side(q):
        for field in range(6):
            ref, i = field_of(ac_ref, av_ref, field)
            join(down_ref, up_ref, 2 * field + q, ref[4 * i + q], ref[4 * i + 2 + q])

    def strip(q):
        join(down_ref, up_ref, 12 + q, zl_ref[q], zr_ref[q])

    loop(0, 2, side)
    loop(0, 4, strip)


def weights(v):
    t = HALF * jnp.abs(v)
    ahead = v > 0.0
    u = 1.0 - t
    tt = t * t
    centre = 1.0 + tt * (1.5 * t - 2.5)
    near = t * (0.5 + t * (2.0 - 1.5 * t))
    tu = -0.5 * t * u
    behind = tu * u
    far = tu * t
    return (
        jnp.where(ahead, 0.0, far),
        jnp.where(ahead, behind, near),
        centre,
        jnp.where(ahead, near, behind),
        jnp.where(ahead, far, 0.0),
    )


def spread(c, w, axis):
    near = roll(w[3] * c, 1, axis) + roll(w[1] * c, -1, axis)
    far = roll(w[4] * c, 2, axis) + roll(w[0] * c, -2, axis)
    return w[2] * c + near + far


def slope_of(two_back, back, forth, two_forth):
    return (8.0 * (forth - back) - (two_forth - two_back)) * (1.0 / 12.0)


def slope_roll(v, axis):
    return slope_of(roll(v, 2, axis), roll(v, 1, axis), roll(v, -1, axis), roll(v, -2, axis))


def replicate(e):
    lane = lanes_of(e.shape)
    up1, up2 = roll(e, 32, 1), roll(e, 64, 1)
    dn1, dn2 = roll(e, -32, 1), roll(e, -64, 1)
    first, second = lane < 32, lane < 64
    return (
        jnp.where(first, e, jnp.where(second, up1, up2)),
        jnp.where(first, dn1, jnp.where(second, e, up1)),
        jnp.where(first, dn2, jnp.where(second, dn1, e)),
    )


def along_x(sources, v_of, stores, rows, base, count):
    open_sums = {}
    for p in range(-2, count + 2):
        w = weights(v_of(base + p, rows))
        cs = [source(base + p, rows) for source in sources]
        for a in range(-2, 3):
            to = p + a
            if 0 <= to < count:
                terms = [w[a + 2] * c for c in cs]
                had = open_sums.get(to)
                open_sums[to] = terms if had is None else [h + t for h, t in zip(had, terms)]
        done = open_sums.pop(p - 2, None)
        if done is not None:
            for store, value in zip(stores, done):
                store(base + p - 2, rows, value)


def put(ref, *lead):
    def store(p, rows, value):
        ref[(*lead, p, rows)] = value

    return store


def get(ref, *lead):
    return lambda p, rows: ref[(*lead, p, rows)]


def over_tiles(body):
    loop(0, 3, lambda tile: body(pl.ds(pl.multiple_of(8 * tile, 8), 8)))


def main_along_x(from_ref, m_ref, x_ref, base, count):
    sources = [get(from_ref, i) for i in range(3)]
    stores = [put(x_ref, i) for i in range(3)]
    over_tiles(lambda rows: along_x(sources, get(m_ref, 3), stores, rows, base, count))


def main_along_yz(m_ref, x_ref, s_ref, slot, rows):
    w = weights(m_ref[4, slot])
    cs = [spread(x_ref[i, slot], w, 0)[0:rows] for i in range(3)]
    w = weights(m_ref[5, slot, 0:rows])
    cs = [spread(c, w, 1) for c in cs]
    return [c + HALF * sum(cs[j] * s_ref[j, i, slot, 0:rows] for j in range(3)) for i, c in enumerate(cs)]


def main_slopes(m_ref, s_ref, slot):
    for i in range(3):
        v = m_ref[3 + i, slot]
        s_ref[0, i, slot] = slope_of(*[m_ref[3 + i, slot + k] for k in (-2, -1, 1, 2)])
        s_ref[1, i, slot] = slope_roll(v, 0)
        s_ref[2, i, slot] = slope_roll(v, 1)


def compute_early(
    place_ref, c_ref, v_ref, b_ref, above_ref, below_ref, m_ref, n_ref, s_ref, o_ref, x_ref
):
    odd = place_ref[0]
    side = 12 - 12 * odd
    first = 4 - 4 * odd

    def own(q):
        for field in range(6):
            ref, i = field_of(c_ref, v_ref, field)
            m_ref[field, 4 + q, 0:16] = ref[i, q]
            m_ref[field, 8 + q, 0:16] = ref[i, 4 + q]
            m_ref[field, 4 + q, 16:24], m_ref[field, 8 + q, 16:24] = halo(
                above_ref, below_ref, 6 * field + q
            )

    def beyond(q):
        for field in range(6):
            m_ref[field, side + q, 0:16] = b_ref[field, q]
            m_ref[field, side + 2 + q, 0:16] = b_ref[field, 2 + q]
            m_ref[field, side + q, 16:24], m_ref[field, side + 2 + q, 16:24] = halo(
                above_ref, below_ref, 6 * field + 4 + q
            )

    loop(0, 4, own)
    loop(0, 2, beyond)
    loop(0, 8, lambda k: main_slopes(m_ref, s_ref, first + 2 + k), 2)
    main_along_x(m_ref, m_ref, x_ref, first + 2, 8)

    def substep_one(k):
        slot = first + 2 + k
        for i, value in enumerate(main_along_yz(m_ref, x_ref, s_ref, slot, 24)):
            n_ref[i, slot] = value

    def substep_two(k):
        slot = first + 4 + k
        for i, value in enumerate(main_along_yz(m_ref, x_ref, s_ref, slot, 16)):
            o_ref[i, slot - 4] = value

    loop(0, 8, substep_one, 2)
    main_along_x(n_ref, m_ref, x_ref, first + 4, 4)
    loop(0, 4, substep_two, 2)


def compute_late(
    place_ref, ac_ref, av_ref, zl_ref, zr_ref, above_ref, below_ref, m_in, n_in, s_in, o_in,
    m_ref, n_ref, s_ref, o_ref, out_ref, x_ref, ec_ref, ev_ref, ed_ref, ex_ref, es_ref,
):
    odd = place_ref[0]
    side = 12 * odd
    first = 2 + 8 * odd
    second = 4 + 4 * odd

    def beyond(q):
        for field in range(6):
            ref, i = field_of(ac_ref, av_ref, field)
            m_ref[field, side + q, 0:16] = ref[4 * i + q]
            m_ref[field, side + 2 + q, 0:16] = ref[4 * i + 2 + q]
            m_ref[field, side + q, 16:24], m_ref[field, side + 2 + q, 16:24] = halo(
                above_ref, below_ref, 2 * field + q
            )

    loop(0, 2, beyond)

    def edges(s):
        lane = lanes_of((24, 128))
        g, q = lax.shift_right_logical(s, 2), lax.bitwise_and(s, 3)
        zl_halo, zr_halo = halo(above_ref, below_ref, 12 + q)
        zl = jnp.concatenate([zl_ref[q], zl_halo], axis=0)
        zr = jnp.concatenate([zr_ref[q], zr_halo], axis=0)
        back = 128 - 32 * g
        zl, zr = pltpu.roll(zl, back, 1), pltpu.roll(zr, back, 1)
        for kind, e_ref in ((0, ec_ref), (1, ev_ref)):
            e = jnp.zeros((24, 128), jnp.float32)
            for i in range(3):
                field = 3 * kind + i
                at = 32 * i
                x = m_ref[field, s]
                e = jnp.where(between(lane, at, at + 4), roll(zl, at - 4 * field, 1), e)
                e = jnp.where(between(lane, at + 4, at + 16), roll(x, at + 4, 1), e)
                e = jnp.where(between(lane, at + 16, at + 28), roll(x, at + 28, 1), e)
                e = jnp.where(between(lane, at + 28, at + 32), roll(zr, at + 28 - 4 * field, 1), e)
            e_ref[s] = e
        for k, d in enumerate(replicate(e)):
            ed_ref[k, s] = d

    loop(0, 16, edges, 2)
    loop(0, 4, lambda k: main_slopes(m_ref, s_ref, first + k), 2)

    def edge_slopes(s):
        v = ev_ref[s]
        es_ref[0, s] = slope_of(*[ev_ref[s + k] for k in (-2, -1, 1, 2)])
        es_ref[1, s] = slope_roll(v, 0)
        es_ref[2, s] = slope_roll(v, 1)

    loop(2, 14, edge_slopes, 4)

    def edge_along_yz(s):
        e = spread(ex_ref[s], weights(ed_ref[1, s]), 0)
        e = spread(e, weights(ed_ref[2, s]), 1)
        parts = replicate(e)
        ec_ref[s] = e + HALF * sum(parts[j] * es_ref[j, s] for j in range(3))

    def edge_substep(n):
        over_tiles(lambda rows: along_x([get(ec_ref)], get(ed_ref, 0), [put(ex_ref)], rows, 2, 12))
        loop(2, 14, edge_along_yz, 4)

    loop(0, 2, edge_substep)

    main_along_x(m_ref, m_ref, x_ref, first, 4)

    def substep_one(k):
        slot = first + k
        for i, value in enumerate(main_along_yz(m_ref, x_ref, s_ref, slot, 24)):
            n_ref[i, slot] = value

    def substep_two(k):
        slot = second + k
        for i, value in enumerate(main_along_yz(m_ref, x_ref, s_ref, slot, 16)):
            o_ref[i, slot - 4] = value

    loop(0, 4, substep_one, 2)
    main_along_x(n_ref, m_ref, x_ref, second, 4)
    loop(0, 4, substep_two, 2)

    def finish(s):
        lane = lanes_of((16, 128))
        e = ec_ref[s + 4, 0:16]
        for i in range(3):
            value = jnp.where(lane < 4, roll(e, -(32 * i + 4), 1), o_ref[i, s])
            out_ref[i, s] = jnp.where(lane >= 124, roll(e, 100 - 32 * i, 1), value)

    loop(0, 8, finish, 2)


def call(kernel, outs, scratch=(), operands=0, aliases=()):
    smem = pl.BlockSpec(memory_space=pltpu.SMEM)
    vmem = pl.BlockSpec(memory_space=pltpu.VMEM)
    shapes = [jax.ShapeDtypeStruct(o, jnp.float32) for o in outs]
    return pl.pallas_call(
        kernel,
        out_shape=shapes,
        in_specs=[smem] + [vmem] * operands,
        out_specs=[vmem] * len(outs),
        scratch_shapes=[pltpu.VMEM(s, jnp.float32) for s in scratch],
        input_output_aliases=dict(aliases),
        compiler_params=pltpu.CompilerParams(vmem_limit_bytes=16 * 1024 * 1024),
    )


def is_far(x):
    return x % 4 in (0, 3)


def solution(mesh):
    end = mesh.shape["gz"] - 1

    def across_of(x):
        return x + 1 if x % 2 else x - 1

    def other_of(x):
        return x - 1 if x % 2 else x + 1

    across = flat_pairs(mesh, lambda x, y, z: (across_of(x), y, z))
    other = flat_pairs(mesh, lambda x, y, z: (other_of(x), y, z))
    aside = flat_pairs(mesh, lambda x, y, z: (other_of(x), y, z) if is_far(x) else None)
    relay = flat_pairs(
        mesh, lambda x, y, z: None if is_far(x) else (other_of(across_of(other_of(x))), y, z)
    )
    beside = flat_pairs(mesh, lambda x, y, z: None if is_far(x) else (across_of(x), y, z))
    y_up = flat_pairs(mesh, lambda x, y, z: (x, y + 1, z))
    y_down = flat_pairs(mesh, lambda x, y, z: (x, y - 1, z))
    last_x = mesh.shape["gx"] - 1
    z_up = flat_pairs(mesh, lambda x, y, z: (x if z < end else last_x - x, y, z + 1))
    z_down = flat_pairs(mesh, lambda x, y, z: (x if z > 0 else last_x - x, y, z - 1))

    def send(value, pairs):
        return lax.ppermute(value, AXES, pairs)

    def local(c, v):
        x, z = lax.axis_index("gx"), lax.axis_index("gz")
        place = jnp.stack([x % 2, (z > 0).astype(x.dtype), (z == 0).astype(x.dtype), (z == end).astype(x.dtype)])
        place = place.astype(jnp.int32)
        far = (x % 4 == 0) | (x % 4 == 3)
        layers = (6, 4, 16, 128)
        edge = (4, 16, 128)
        ac, av, b, _ = call(pack_x, [(14, 16, 128), (12, 16, 128), layers, edge], (), 2)(place, c, v)
        own_end = ac[12:]
        passed = send(av, aside)
        ac = send(ac, across)
        passed = send(jnp.concatenate([passed, own_end]), relay)
        near_av = send(av, beside)
        b = send(b, other)
        down, up = call(pack_y_early, [(36, 8, 128)] * 2, (), 3)(place, c, v, b)
        early_above = send(down, y_down)
        early_below = send(up, y_up)
        held = jnp.where(far, ac, passed)
        forwarded = send(held, other)
        end_a = jnp.where(far, own_end, send(passed[12:], beside))
        av = jnp.where(far, forwarded[:12], near_av)
        left, right = call(pack_z, [edge, edge], (), 8)(
            place, c, v, ac, av, b, held[12:], end_a, forwarded[12:]
        )
        zl = send(right, z_up)
        zr = send(left, z_down)
        down, up = call(pack_y_late, [(16, 8, 128)] * 2, (), 4)(place, ac, av, zl, zr)
        above = send(down, y_down)
        below = send(up, y_up)
        block = (16, 24, 128)
        state = [(6, *block), (3, *block), (3, 3, *block), (3, 8, 16, 128)]
        m, n, s, o = call(compute_early, state, [(3, *block)], 5)(
            place, c, v, b, early_above, early_below
        )
        scratch = [(3, *block), block, block, (3, *block), block, (3, *block)]
        *_, out = call(
            compute_late, state + [(3, 8, 16, 128)], scratch, 10, {7 + k: k for k in range(4)}
        )(place, ac, av, zl, zr, above, below, m, n, s, o)
        return out

    placed = P(None, *AXES)
    return jax.shard_map(local, mesh=mesh, in_specs=(placed, placed), out_specs=placed, check_vma=False)
```

```python
import jax
import jax.numpy as jnp
from jax import lax
from jax.experimental import pallas as pl
from jax.experimental.pallas import tpu as pltpu
from jax.sharding import PartitionSpec as P


AXES = ("gx", "gy", "gz")
HALF = 0.5


def flat_pairs(mesh, move):
    nx, ny, nz = (mesh.shape[a] for a in AXES)
    pairs = []
    for x in range(nx):
        for y in range(ny):
            for z in range(nz):
                to = move(x, y, z)
                if to is not None:
                    tx, ty, tz = to[0] % nx, to[1] % ny, to[2] % nz
                    pairs.append(((x * ny + y) * nz + z, (tx * ny + ty) * nz + tz))
    return pairs


def lanes_of(shape):
    return lax.broadcasted_iota(jnp.int32, shape, len(shape) - 1)


def rows_of(shape):
    return lax.broadcasted_iota(jnp.int32, shape, len(shape) - 2)


def roll(x, shift, axis):
    shift = shift % x.shape[axis]
    return x if shift == 0 else pltpu.roll(x, shift, axis)


def between(index, first, last):
    return (index >= first) & (index < last)


def loop(first, last, body, unroll=1):
    def step(i, carry):
        body(i)
        return carry

    lax.fori_loop(first, last, step, 0, unroll=unroll)


def field_of(c_ref, v_ref, field):
    return (c_ref, field) if field < 3 else (v_ref, field - 3)


def pack_x(place_ref, c_ref, v_ref, ac_ref, av_ref, b_ref, edge_ref, c_out, v_out):
    high = 4 * place_ref[0]
    low = 4 - high
    shift = 4 * place_ref[1]

    def copy(q):
        for field in range(6):
            ref, i = field_of(c_ref, v_ref, field)
            to, j = field_of(ac_ref, av_ref, field)
            to[4 * j + q] = ref[i, high + q]
            b_ref[field, q] = ref[i, low + q]
            kept = c_out if field < 3 else v_out
            kept[i, q], kept[i, 4 + q] = ref[i, q], ref[i, 4 + q]
        lane = lanes_of((16, 128))
        edge = jnp.zeros((16, 128), jnp.float32)
        for g in (1, 2):
            for field in range(6):
                ref, i = field_of(c_ref, v_ref, field)
                at = 32 * g + 4 * field
                x = pltpu.roll(ref[i, 4 * (g - 1) + q], shift + at, 1)
                edge = jnp.where(between(lane, at, at + 4), x, edge)
        edge_ref[q] = edge

    loop(0, 4, copy)
    for q in range(2):
        ac_ref[12 + q] = edge_ref[q] + roll(edge_ref[q + 2], 64, 1)


def lower_upper(odd, ac_ref, av_ref, b_ref, field, q):
    ref, i = field_of(ac_ref, av_ref, field)
    a, b = ref[4 * i + q], b_ref[field, q]
    return jnp.where(odd, b, a), jnp.where(odd, a, b)


def pack_z(
    place_ref, c_ref, v_ref, ac_ref, av_ref, b_ref, end_ref, end_a_ref, end_b_ref, left_ref, right_ref
):
    odd = place_ref[0] == 1
    first_end = place_ref[2] == 1
    last_end = place_ref[3] == 1

    def pack(q):
        lane = lanes_of((16, 128))
        left = jnp.zeros((16, 128), jnp.float32)
        right = left
        for field in range(6):
            ref, i = field_of(c_ref, v_ref, field)
            lo, hi = lower_upper(odd, ac_ref, av_ref, b_ref, field, q)
            for g, x in enumerate((lo, ref[i, q], ref[i, 4 + q], hi)):
                at = 32 * g + 4 * field
                here = between(lane, at, at + 4)
                left = jnp.where(here, roll(x, at, 1), left)
                right = jnp.where(here, roll(x, at + 4, 1), right)
        turn = 64 * lax.shift_right_logical(q, 1)
        base, a, b = (
            pltpu.roll(ref[lax.bitwise_and(q, 1)], turn, 1) for ref in (end_ref, end_a_ref, end_b_ref)
        )
        a, b = roll(a, 64, 1), roll(b, 64, 1)
        lo, hi = jnp.where(odd, a, b), jnp.where(odd, b, a)
        end = jnp.where(lane < 32, lo, jnp.where(lane < 96, base, hi))
        left_ref[q] = jnp.where(first_end, end, left)
        right_ref[q] = jnp.where(last_end, end, right)

    loop(0, 4, pack)


def join(down_ref, up_ref, entry, first, second):
    upper = rows_of((8, 128)) < 4
    down_ref[entry] = jnp.where(upper, first[0:8], roll(second[0:8], 4, 0))
    up_ref[entry] = jnp.where(upper, roll(first[8:16], 4, 0), second[8:16])


def halo(above_ref, below_ref, entry):
    upper = rows_of((8, 128)) < 4
    above, below = above_ref[entry], below_ref[entry]
    first = jnp.where(upper, above, roll(below, 4, 0))
    return first, jnp.where(upper, roll(above, 4, 0), below)


def pack_y_early(place_ref, c_ref, v_ref, b_ref, down_ref, up_ref):
    for field in range(6):
        ref, i = field_of(c_ref, v_ref, field)

        def own(q):
            join(down_ref, up_ref, 6 * field + q, ref[i, q], ref[i, 4 + q])

        def side(q):
            join(down_ref, up_ref, 6 * field + 4 + q, b_ref[field, q], b_ref[field, 2 + q])

        loop(0, 4, own)
        loop(0, 2, side)


def pack_y_late(place_ref, ac_ref, av_ref, zl_ref, zr_ref, down_ref, up_ref):
    def side(q):
        for field in range(6):
            ref, i = field_of(ac_ref, av_ref, field)
            join(down_ref, up_ref, 2 * field + q, ref[4 * i + q], ref[4 * i + 2 + q])

    def strip(q):
        join(down_ref, up_ref, 12 + q, zl_ref[q], zr_ref[q])

    loop(0, 2, side)
    loop(0, 4, strip)


def weights(v):
    t = HALF * jnp.abs(v)
    ahead = v > 0.0
    u = 1.0 - t
    tt = t * t
    centre = 1.0 + tt * (1.5 * t - 2.5)
    near = t * (0.5 + t * (2.0 - 1.5 * t))
    tu = -0.5 * t * u
    behind = tu * u
    far = tu * t
    return (
        jnp.where(ahead, 0.0, far),
        jnp.where(ahead, behind, near),
        centre,
        jnp.where(ahead, near, behind),
        jnp.where(ahead, far, 0.0),
    )


def spread(c, w, axis):
    near = roll(w[3] * c, 1, axis) + roll(w[1] * c, -1, axis)
    far = roll(w[4] * c, 2, axis) + roll(w[0] * c, -2, axis)
    return w[2] * c + near + far


def slope_of(two_back, back, forth, two_forth):
    return (8.0 * (forth - back) - (two_forth - two_back)) * (1.0 / 12.0)


def slope_roll(v, axis):
    return slope_of(roll(v, 2, axis), roll(v, 1, axis), roll(v, -1, axis), roll(v, -2, axis))


def replicate(e):
    lane = lanes_of(e.shape)
    up1, up2 = roll(e, 32, 1), roll(e, 64, 1)
    dn1, dn2 = roll(e, -32, 1), roll(e, -64, 1)
    first, second = lane < 32, lane < 64
    return (
        jnp.where(first, e, jnp.where(second, up1, up2)),
        jnp.where(first, dn1, jnp.where(second, e, up1)),
        jnp.where(first, dn2, jnp.where(second, dn1, e)),
    )


def along_x(sources, v_of, stores, rows, base, count):
    open_sums = {}
    for p in range(-2, count + 2):
        w = weights(v_of(base + p, rows))
        cs = [source(base + p, rows) for source in sources]
        for a in range(-2, 3):
            to = p + a
            if 0 <= to < count:
                terms = [w[a + 2] * c for c in cs]
                had = open_sums.get(to)
                open_sums[to] = terms if had is None else [h + t for h, t in zip(had, terms)]
        done = open_sums.pop(p - 2, None)
        if done is not None:
            for store, value in zip(stores, done):
                store(base + p - 2, rows, value)


def put(ref, *lead):
    def store(p, rows, value):
        ref[(*lead, p, rows)] = value

    return store


def get(ref, *lead):
    return lambda p, rows: ref[(*lead, p, rows)]


def over_tiles(body):
    loop(0, 3, lambda tile: body(pl.ds(pl.multiple_of(8 * tile, 8), 8)))


def main_along_x(t_ref, v_ref, x_ref, stage, base, count):
    sources = [get(t_ref, stage, i) for i in range(3)]
    stores = [put(x_ref, i) for i in range(3)]
    over_tiles(lambda rows: along_x(sources, get(v_ref, 0), stores, rows, base, count))


def main_along_yz(t_ref, v_ref, x_ref, s_ref, stage, slot):
    w = weights(v_ref[1, slot])
    cs = [spread(x_ref[i, slot], w, 0) for i in range(3)]
    w = weights(v_ref[2, slot])
    cs = [spread(c, w, 1) for c in cs]
    for i, c in enumerate(cs):
        t_ref[stage + 1, i, slot] = c + HALF * sum(cs[j] * s_ref[j, i, slot] for j in range(3))


def main_slopes(v_ref, s_ref, slot):
    for i in range(3):
        v = v_ref[i, slot]
        s_ref[0, i, slot] = slope_of(*[v_ref[i, slot + k] for k in (-2, -1, 1, 2)])
        s_ref[1, i, slot] = slope_roll(v, 0)
        s_ref[2, i, slot] = slope_roll(v, 1)


def widened(t_ref, w_ref, field):
    return (t_ref, (0, field)) if field < 3 else (w_ref, (field - 3,))


def compute_early(
    place_ref, c_ref, v_ref, b_ref, above_ref, below_ref, t_ref, w_ref, s_ref, x_ref
):
    odd = place_ref[0]
    side = 12 - 12 * odd
    first = 4 - 4 * odd

    def own(q):
        for field in range(6):
            ref, i = field_of(c_ref, v_ref, field)
            to, at = widened(t_ref, w_ref, field)
            to[(*at, 4 + q, slice(0, 16))] = ref[i, q]
            to[(*at, 8 + q, slice(0, 16))] = ref[i, 4 + q]
            near, far = halo(above_ref, below_ref, 6 * field + q)
            to[(*at, 4 + q, slice(16, 24))] = near
            to[(*at, 8 + q, slice(16, 24))] = far

    def beyond(q):
        for field in range(6):
            to, at = widened(t_ref, w_ref, field)
            to[(*at, side + q, slice(0, 16))] = b_ref[field, q]
            to[(*at, side + 2 + q, slice(0, 16))] = b_ref[field, 2 + q]
            near, far = halo(above_ref, below_ref, 6 * field + 4 + q)
            to[(*at, side + q, slice(16, 24))] = near
            to[(*at, side + 2 + q, slice(16, 24))] = far

    loop(0, 4, own)
    loop(0, 2, beyond)
    loop(0, 8, lambda k: main_slopes(w_ref, s_ref, first + 2 + k))

    def substep(n):
        main_along_x(t_ref, w_ref, x_ref, n, first + 2, 8)

        def pair(k):
            for j in range(2):
                main_along_yz(t_ref, w_ref, x_ref, s_ref, n, first + 2 + 2 * n + 2 * k + j)

        loop(0, 4 - 2 * n, pair)

    loop(0, 2, substep)


def compute_late(
    place_ref, ac_ref, av_ref, zl_ref, zr_ref, above_ref, below_ref, t_in, w_in, s_in,
    t_ref, w_ref, s_ref, out_ref, x_ref, ec_ref, ev_ref, ed_ref, ex_ref, es_ref,
):
    odd = place_ref[0]
    side = 12 * odd
    first = 2 + 8 * odd
    step = 2 - 4 * odd

    def beyond(q):
        for field in range(6):
            ref, i = field_of(ac_ref, av_ref, field)
            to, at = widened(t_ref, w_ref, field)
            to[(*at, side + q, slice(0, 16))] = ref[4 * i + q]
            to[(*at, side + 2 + q, slice(0, 16))] = ref[4 * i + 2 + q]
            near, far = halo(above_ref, below_ref, 2 * field + q)
            to[(*at, side + q, slice(16, 24))] = near
            to[(*at, side + 2 + q, slice(16, 24))] = far

    loop(0, 2, beyond)

    def edges(s):
        lane = lanes_of((24, 128))
        g, q = lax.shift_right_logical(s, 2), lax.bitwise_and(s, 3)
        zl_halo, zr_halo = halo(above_ref, below_ref, 12 + q)
        zl = jnp.concatenate([zl_ref[q], zl_halo], axis=0)
        zr = jnp.concatenate([zr_ref[q], zr_halo], axis=0)
        back = 128 - 32 * g
        zl, zr = pltpu.roll(zl, back, 1), pltpu.roll(zr, back, 1)
        for kind, e_ref in ((0, ec_ref), (1, ev_ref)):
            e = jnp.zeros((24, 128), jnp.float32)
            for i in range(3):
                field = 3 * kind + i
                at = 32 * i
                source, where = widened(t_ref, w_ref, field)
                x = source[(*where, s)]
                e = jnp.where(between(lane, at, at + 4), roll(zl, at - 4 * field, 1), e)
                e = jnp.where(between(lane, at + 4, at + 16), roll(x, at + 4, 1), e)
                e = jnp.where(between(lane, at + 16, at + 28), roll(x, at + 28, 1), e)
                e = jnp.where(between(lane, at + 28, at + 32), roll(zr, at + 28 - 4 * field, 1), e)
            e_ref[s] = e
        for k, d in enumerate(replicate(e)):
            ed_ref[k, s] = d

    loop(0, 16, edges, 2)
    loop(0, 4, lambda k: main_slopes(w_ref, s_ref, first + k))

    def edge_slopes(s):
        v = ev_ref[s]
        es_ref[0, s] = slope_of(*[ev_ref[s + k] for k in (-2, -1, 1, 2)])
        es_ref[1, s] = slope_roll(v, 0)
        es_ref[2, s] = slope_roll(v, 1)

    loop(2, 14, edge_slopes, 4)

    def edge_along_yz(s):
        e = spread(ex_ref[s], weights(ed_ref[1, s]), 0)
        e = spread(e, weights(ed_ref[2, s]), 1)
        parts = replicate(e)
        ec_ref[s] = e + HALF * sum(parts[j] * es_ref[j, s] for j in range(3))

    def edge_substep(n):
        over_tiles(lambda rows: along_x([get(ec_ref)], get(ed_ref, 0), [put(ex_ref)], rows, 2, 12))

        def four(k):
            for j in range(4):
                edge_along_yz(2 + 2 * n + 4 * k + j)

        loop(0, 3 - n, four)

    loop(0, 2, edge_substep)

    def substep(n):
        base = first + step * n
        main_along_x(t_ref, w_ref, x_ref, n, base, 4)

        def pair(k):
            for j in range(2):
                main_along_yz(t_ref, w_ref, x_ref, s_ref, n, base + 2 * k + j)

        loop(0, 2, pair)

    loop(0, 2, substep)

    def finish(s):
        lane = lanes_of((16, 128))
        e = ec_ref[s + 4, 0:16]
        for i in range(3):
            value = jnp.where(lane < 4, roll(e, -(32 * i + 4), 1), t_ref[2, i, s + 4, 0:16])
            out_ref[i, s] = jnp.where(lane >= 124, roll(e, 100 - 32 * i, 1), value)

    loop(0, 8, finish)


def call(kernel, outs, scratch=(), operands=0, aliases=()):
    smem = pl.BlockSpec(memory_space=pltpu.SMEM)
    vmem = pl.BlockSpec(memory_space=pltpu.VMEM)
    shapes = [jax.ShapeDtypeStruct(o, jnp.float32) for o in outs]
    return pl.pallas_call(
        kernel,
        out_shape=shapes,
        in_specs=[smem] + [vmem] * operands,
        out_specs=[vmem] * len(outs),
        scratch_shapes=[pltpu.VMEM(s, jnp.float32) for s in scratch],
        input_output_aliases=dict(aliases),
        compiler_params=pltpu.CompilerParams(vmem_limit_bytes=16 * 1024 * 1024),
    )


def is_far(x):
    return x % 4 in (0, 3)


def solution(mesh):
    end = mesh.shape["gz"] - 1

    def across_of(x):
        return x + 1 if x % 2 else x - 1

    def other_of(x):
        return x - 1 if x % 2 else x + 1

    across = flat_pairs(mesh, lambda x, y, z: (across_of(x), y, z))
    other = flat_pairs(mesh, lambda x, y, z: (other_of(x), y, z))
    aside = flat_pairs(mesh, lambda x, y, z: (other_of(x), y, z) if is_far(x) else None)
    relay = flat_pairs(
        mesh, lambda x, y, z: None if is_far(x) else (other_of(across_of(other_of(x))), y, z)
    )
    beside = flat_pairs(mesh, lambda x, y, z: None if is_far(x) else (across_of(x), y, z))
    y_up = flat_pairs(mesh, lambda x, y, z: (x, y + 1, z))
    y_down = flat_pairs(mesh, lambda x, y, z: (x, y - 1, z))
    last_x = mesh.shape["gx"] - 1
    z_up = flat_pairs(mesh, lambda x, y, z: (x if z < end else last_x - x, y, z + 1))
    z_down = flat_pairs(mesh, lambda x, y, z: (x if z > 0 else last_x - x, y, z - 1))

    def send(value, pairs):
        return lax.ppermute(value, AXES, pairs)

    def local(c, v):
        x, z = lax.axis_index("gx"), lax.axis_index("gz")
        place = jnp.stack([x % 2, (z > 0).astype(x.dtype), (z == 0).astype(x.dtype), (z == end).astype(x.dtype)])
        place = place.astype(jnp.int32)
        far = (x % 4 == 0) | (x % 4 == 3)
        layers = (6, 4, 16, 128)
        edge = (4, 16, 128)
        block = (3, 8, 16, 128)
        shapes = [(14, 16, 128), (12, 16, 128), layers, edge, block, block]
        ac, av, b, _, c, v = call(pack_x, shapes, (), 2)(place, c, v)
        own_end = ac[12:]
        passed = send(av, aside)
        ac = send(ac, across)
        passed = send(jnp.concatenate([passed, own_end]), relay)
        near_av = send(av, beside)
        b = send(b, other)
        down, up = call(pack_y_early, [(36, 8, 128)] * 2, (), 3)(place, c, v, b)
        early_above = send(down, y_down)
        early_below = send(up, y_up)
        held = jnp.where(far, ac, passed)
        forwarded = send(held, other)
        end_a = jnp.where(far, own_end, send(passed[12:], beside))
        av = jnp.where(far, forwarded[:12], near_av)
        left, right = call(pack_z, [edge, edge], (), 8)(
            place, c, v, ac, av, b, held[12:], end_a, forwarded[12:]
        )
        zl = send(right, z_up)
        zr = send(left, z_down)
        down, up = call(pack_y_late, [(16, 8, 128)] * 2, (), 4)(place, ac, av, zl, zr)
        above = send(down, y_down)
        below = send(up, y_up)
        block = (16, 24, 128)
        state = [(3, 3, *block), (3, *block), (3, 3, *block)]
        state = call(compute_early, state, [(3, *block)], 5)(
            place, c, v, b, early_above, early_below
        )
        scratch = [(3, *block), block, block, (3, *block), block, (3, *block)]
        shapes = [a.shape for a in state] + [(3, 8, 16, 128)]
        *_, out = call(compute_late, shapes, scratch, 9, {7 + k: k for k in range(3)})(
            place, ac, av, zl, zr, above, below, *state
        )
        return out

    placed = P(None, *AXES)
    return jax.shard_map(local, mesh=mesh, in_specs=(placed, placed), out_specs=placed, check_vma=False)
```

```python
import jax
import jax.numpy as jnp
from jax import lax
from jax.experimental import pallas as pl
from jax.experimental.pallas import tpu as pltpu
from jax.sharding import PartitionSpec as P


AXES = ("gx", "gy", "gz")
HALF = 0.5


def flat_pairs(mesh, move):
    nx, ny, nz = (mesh.shape[a] for a in AXES)
    pairs = []
    for x in range(nx):
        for y in range(ny):
            for z in range(nz):
                to = move(x, y, z)
                if to is not None:
                    tx, ty, tz = to[0] % nx, to[1] % ny, to[2] % nz
                    pairs.append(((x * ny + y) * nz + z, (tx * ny + ty) * nz + tz))
    return pairs


def lanes_of(shape):
    return lax.broadcasted_iota(jnp.int32, shape, len(shape) - 1)


def rows_of(shape):
    return lax.broadcasted_iota(jnp.int32, shape, len(shape) - 2)


def roll(x, shift, axis):
    shift = shift % x.shape[axis]
    return x if shift == 0 else pltpu.roll(x, shift, axis)


def between(index, first, last):
    return (index >= first) & (index < last)


def loop(first, last, body, unroll=1):
    def step(i, carry):
        body(i)
        return carry

    lax.fori_loop(first, last, step, 0, unroll=unroll)


def field_of(c_ref, v_ref, field):
    return (c_ref, field) if field < 3 else (v_ref, field - 3)


def pack_aside(place_ref, v_ref, av_ref, v_out):
    high = 4 * place_ref[0]
    for i in range(3):
        for q in range(4):
            av_ref[4 * i + q] = v_ref[i, high + q]
    v_out[...] = v_ref[...]


def pack_x(place_ref, c_ref, v_ref, ac_ref, b_ref, edge_ref, c_out):
    high = 4 * place_ref[0]
    low = 4 - high
    shift = 4 * place_ref[1]

    def copy(q):
        for field in range(6):
            ref, i = field_of(c_ref, v_ref, field)
            if field < 3:
                ac_ref[4 * field + q] = ref[i, high + q]
                c_out[i, q], c_out[i, 4 + q] = ref[i, q], ref[i, 4 + q]
            b_ref[field, q] = ref[i, low + q]
        lane = lanes_of((16, 128))
        edge = jnp.zeros((16, 128), jnp.float32)
        for g in (1, 2):
            for field in range(6):
                ref, i = field_of(c_ref, v_ref, field)
                at = 32 * g + 4 * field
                x = pltpu.roll(ref[i, 4 * (g - 1) + q], shift + at, 1)
                edge = jnp.where(between(lane, at, at + 4), x, edge)
        edge_ref[q] = edge

    loop(0, 4, copy)
    for q in range(2):
        ac_ref[12 + q] = edge_ref[q] + roll(edge_ref[q + 2], 64, 1)


def lower_upper(odd, ac_ref, av_ref, b_ref, field, q):
    ref, i = field_of(ac_ref, av_ref, field)
    a, b = ref[4 * i + q], b_ref[field, q]
    return jnp.where(odd, b, a), jnp.where(odd, a, b)


def pack_z(
    place_ref, c_ref, v_ref, ac_ref, av_ref, b_ref, end_ref, end_a_ref, end_b_ref, left_ref, right_ref
):
    odd = place_ref[0] == 1
    first_end = place_ref[2] == 1
    last_end = place_ref[3] == 1

    def pack(q):
        lane = lanes_of((16, 128))
        left = jnp.zeros((16, 128), jnp.float32)
        right = left
        for field in range(6):
            ref, i = field_of(c_ref, v_ref, field)
            lo, hi = lower_upper(odd, ac_ref, av_ref, b_ref, field, q)
            for g, x in enumerate((lo, ref[i, q], ref[i, 4 + q], hi)):
                at = 32 * g + 4 * field
                here = between(lane, at, at + 4)
                left = jnp.where(here, roll(x, at, 1), left)
                right = jnp.where(here, roll(x, at + 4, 1), right)
        turn = 64 * lax.shift_right_logical(q, 1)
        base, a, b = (
            pltpu.roll(ref[lax.bitwise_and(q, 1)], turn, 1) for ref in (end_ref, end_a_ref, end_b_ref)
        )
        a, b = roll(a, 64, 1), roll(b, 64, 1)
        lo, hi = jnp.where(odd, a, b), jnp.where(odd, b, a)
        end = jnp.where(lane < 32, lo, jnp.where(lane < 96, base, hi))
        left_ref[q] = jnp.where(first_end, end, left)
        right_ref[q] = jnp.where(last_end, end, right)

    loop(0, 4, pack)


def join(down_ref, up_ref, entry, first, second):
    upper = rows_of((8, 128)) < 4
    down_ref[entry] = jnp.where(upper, first[0:8], roll(second[0:8], 4, 0))
    up_ref[entry] = jnp.where(upper, roll(first[8:16], 4, 0), second[8:16])


def halo(above_ref, below_ref, entry):
    upper = rows_of((8, 128)) < 4
    above, below = above_ref[entry], below_ref[entry]
    first = jnp.where(upper, above, roll(below, 4, 0))
    return first, jnp.where(upper, roll(above, 4, 0), below)


def pack_y_early(place_ref, c_ref, v_ref, b_ref, down_ref, up_ref):
    for field in range(6):
        ref, i = field_of(c_ref, v_ref, field)

        def own(q):
            join(down_ref, up_ref, 6 * field + q, ref[i, q], ref[i, 4 + q])

        def side(q):
            join(down_ref, up_ref, 6 * field + 4 + q, b_ref[field, q], b_ref[field, 2 + q])

        loop(0, 4, own)
        loop(0, 2, side)


def pack_y_late(place_ref, ac_ref, av_ref, zl_ref, zr_ref, down_ref, up_ref):
    def side(q):
        for field in range(6):
            ref, i = field_of(ac_ref, av_ref, field)
            join(down_ref, up_ref, 2 * field + q, ref[4 * i + q], ref[4 * i + 2 + q])

    def strip(q):
        join(down_ref, up_ref, 12 + q, zl_ref[q], zr_ref[q])

    loop(0, 2, side)
    loop(0, 4, strip)


def weights(v):
    t = HALF * jnp.abs(v)
    ahead = v > 0.0
    u = 1.0 - t
    tt = t * t
    centre = 1.0 + tt * (1.5 * t - 2.5)
    near = t * (0.5 + t * (2.0 - 1.5 * t))
    tu = -0.5 * t * u
    behind = tu * u
    far = tu * t
    return (
        jnp.where(ahead, 0.0, far),
        jnp.where(ahead, behind, near),
        centre,
        jnp.where(ahead, near, behind),
        jnp.where(ahead, far, 0.0),
    )


def spread(c, w, axis):
    near = roll(w[3] * c, 1, axis) + roll(w[1] * c, -1, axis)
    far = roll(w[4] * c, 2, axis) + roll(w[0] * c, -2, axis)
    return w[2] * c + near + far


def slope_of(two_back, back, forth, two_forth):
    return (8.0 * (forth - back) - (two_forth - two_back)) * (1.0 / 12.0)


def slope_roll(v, axis):
    return slope_of(roll(v, 2, axis), roll(v, 1, axis), roll(v, -1, axis), roll(v, -2, axis))


def replicate(e):
    lane = lanes_of(e.shape)
    up1, up2 = roll(e, 32, 1), roll(e, 64, 1)
    dn1, dn2 = roll(e, -32, 1), roll(e, -64, 1)
    first, second = lane < 32, lane < 64
    return (
        jnp.where(first, e, jnp.where(second, up1, up2)),
        jnp.where(first, dn1, jnp.where(second, e, up1)),
        jnp.where(first, dn2, jnp.where(second, dn1, e)),
    )


def along_x(sources, v_of, stores, rows, base, count):
    open_sums = {}
    for p in range(-2, count + 2):
        w = weights(v_of(base + p, rows))
        cs = [source(base + p, rows) for source in sources]
        for a in range(-2, 3):
            to = p + a
            if 0 <= to < count:
                terms = [w[a + 2] * c for c in cs]
                had = open_sums.get(to)
                open_sums[to] = terms if had is None else [h + t for h, t in zip(had, terms)]
        done = open_sums.pop(p - 2, None)
        if done is not None:
            for store, value in zip(stores, done):
                store(base + p - 2, rows, value)


def put(ref, *lead):
    def store(p, rows, value):
        ref[(*lead, p, rows)] = value

    return store


def get(ref, *lead):
    return lambda p, rows: ref[(*lead, p, rows)]


def over_tiles(body):
    loop(0, 3, lambda tile: body(pl.ds(pl.multiple_of(8 * tile, 8), 8)))


def main_along_x(t_ref, v_ref, x_ref, stage, base, count):
    sources = [get(t_ref, stage, i) for i in range(3)]
    stores = [put(x_ref, i) for i in range(3)]
    over_tiles(lambda rows: along_x(sources, get(v_ref, 0), stores, rows, base, count))


def main_along_yz(t_ref, v_ref, x_ref, s_ref, stage, slot):
    w = weights(v_ref[1, slot])
    cs = [spread(x_ref[i, slot], w, 0) for i in range(3)]
    w = weights(v_ref[2, slot])
    cs = [spread(c, w, 1) for c in cs]
    for i, c in enumerate(cs):
        t_ref[stage + 1, i, slot] = c + HALF * sum(cs[j] * s_ref[j, i, slot] for j in range(3))


def main_slopes(v_ref, s_ref, slot):
    for i in range(3):
        v = v_ref[i, slot]
        s_ref[0, i, slot] = slope_of(*[v_ref[i, slot + k] for k in (-2, -1, 1, 2)])
        s_ref[1, i, slot] = slope_roll(v, 0)
        s_ref[2, i, slot] = slope_roll(v, 1)


def widened(t_ref, w_ref, field):
    return (t_ref, (0, field)) if field < 3 else (w_ref, (field - 3,))


def compute_early(
    place_ref, c_ref, v_ref, b_ref, above_ref, below_ref, t_ref, w_ref, s_ref, x_ref
):
    odd = place_ref[0]
    side = 12 - 12 * odd
    first = 4 - 4 * odd

    def own(q):
        for field in range(6):
            ref, i = field_of(c_ref, v_ref, field)
            to, at = widened(t_ref, w_ref, field)
            to[(*at, 4 + q, slice(0, 16))] = ref[i, q]
            to[(*at, 8 + q, slice(0, 16))] = ref[i, 4 + q]
            near, far = halo(above_ref, below_ref, 6 * field + q)
            to[(*at, 4 + q, slice(16, 24))] = near
            to[(*at, 8 + q, slice(16, 24))] = far

    def beyond(q):
        for field in range(6):
            to, at = widened(t_ref, w_ref, field)
            to[(*at, side + q, slice(0, 16))] = b_ref[field, q]
            to[(*at, side + 2 + q, slice(0, 16))] = b_ref[field, 2 + q]
            near, far = halo(above_ref, below_ref, 6 * field + 4 + q)
            to[(*at, side + q, slice(16, 24))] = near
            to[(*at, side + 2 + q, slice(16, 24))] = far

    loop(0, 4, own)
    loop(0, 2, beyond)
    loop(0, 8, lambda k: main_slopes(w_ref, s_ref, first + 2 + k))

    def substep(n):
        main_along_x(t_ref, w_ref, x_ref, n, first + 2, 8)

        def pair(k):
            for j in range(2):
                main_along_yz(t_ref, w_ref, x_ref, s_ref, n, first + 2 + 2 * n + 2 * k + j)

        loop(0, 4 - 2 * n, pair)

    loop(0, 2, substep)


def compute_late(
    place_ref, ac_ref, av_ref, zl_ref, zr_ref, above_ref, below_ref, t_in, w_in, s_in,
    t_ref, w_ref, s_ref, out_ref, x_ref, ec_ref, ev_ref, ed_ref, ex_ref, es_ref,
):
    odd = place_ref[0]
    side = 12 * odd
    first = 2 + 8 * odd
    step = 2 - 4 * odd

    def beyond(q):
        for field in range(6):
            ref, i = field_of(ac_ref, av_ref, field)
            to, at = widened(t_ref, w_ref, field)
            to[(*at, side + q, slice(0, 16))] = ref[4 * i + q]
            to[(*at, side + 2 + q, slice(0, 16))] = ref[4 * i + 2 + q]
            near, far = halo(above_ref, below_ref, 2 * field + q)
            to[(*at, side + q, slice(16, 24))] = near
            to[(*at, side + 2 + q, slice(16, 24))] = far

    loop(0, 2, beyond)

    def edges(s):
        lane = lanes_of((24, 128))
        g, q = lax.shift_right_logical(s, 2), lax.bitwise_and(s, 3)
        zl_halo, zr_halo = halo(above_ref, below_ref, 12 + q)
        zl = jnp.concatenate([zl_ref[q], zl_halo], axis=0)
        zr = jnp.concatenate([zr_ref[q], zr_halo], axis=0)
        back = 128 - 32 * g
        zl, zr = pltpu.roll(zl, back, 1), pltpu.roll(zr, back, 1)
        for kind, e_ref in ((0, ec_ref), (1, ev_ref)):
            e = jnp.zeros((24, 128), jnp.float32)
            for i in range(3):
                field = 3 * kind + i
                at = 32 * i
                source, where = widened(t_ref, w_ref, field)
                x = source[(*where, s)]
                e = jnp.where(between(lane, at, at + 4), roll(zl, at - 4 * field, 1), e)
                e = jnp.where(between(lane, at + 4, at + 16), roll(x, at + 4, 1), e)
                e = jnp.where(between(lane, at + 16, at + 28), roll(x, at + 28, 1), e)
                e = jnp.where(between(lane, at + 28, at + 32), roll(zr, at + 28 - 4 * field, 1), e)
            e_ref[s] = e
        for k, d in enumerate(replicate(e)):
            ed_ref[k, s] = d

    loop(0, 16, edges, 2)
    loop(0, 4, lambda k: main_slopes(w_ref, s_ref, first + k))

    def edge_slopes(s):
        v = ev_ref[s]
        es_ref[0, s] = slope_of(*[ev_ref[s + k] for k in (-2, -1, 1, 2)])
        es_ref[1, s] = slope_roll(v, 0)
        es_ref[2, s] = slope_roll(v, 1)

    loop(2, 14, edge_slopes, 4)

    def edge_along_yz(s):
        e = spread(ex_ref[s], weights(ed_ref[1, s]), 0)
        e = spread(e, weights(ed_ref[2, s]), 1)
        parts = replicate(e)
        ec_ref[s] = e + HALF * sum(parts[j] * es_ref[j, s] for j in range(3))

    def edge_substep(n):
        over_tiles(lambda rows: along_x([get(ec_ref)], get(ed_ref, 0), [put(ex_ref)], rows, 2, 12))

        def four(k):
            for j in range(4):
                edge_along_yz(2 + 2 * n + 4 * k + j)

        loop(0, 3 - n, four)

    loop(0, 2, edge_substep)

    def substep(n):
        base = first + step * n
        main_along_x(t_ref, w_ref, x_ref, n, base, 4)

        def pair(k):
            for j in range(2):
                main_along_yz(t_ref, w_ref, x_ref, s_ref, n, base + 2 * k + j)

        loop(0, 2, pair)

    loop(0, 2, substep)

    def finish(s):
        lane = lanes_of((16, 128))
        e = ec_ref[s + 4, 0:16]
        for i in range(3):
            value = jnp.where(lane < 4, roll(e, -(32 * i + 4), 1), t_ref[2, i, s + 4, 0:16])
            out_ref[i, s] = jnp.where(lane >= 124, roll(e, 100 - 32 * i, 1), value)

    loop(0, 8, finish)


def call(kernel, outs, scratch=(), operands=0, aliases=()):
    smem = pl.BlockSpec(memory_space=pltpu.SMEM)
    vmem = pl.BlockSpec(memory_space=pltpu.VMEM)
    shapes = [jax.ShapeDtypeStruct(o, jnp.float32) for o in outs]
    return pl.pallas_call(
        kernel,
        out_shape=shapes,
        in_specs=[smem] + [vmem] * operands,
        out_specs=[vmem] * len(outs),
        scratch_shapes=[pltpu.VMEM(s, jnp.float32) for s in scratch],
        input_output_aliases=dict(aliases),
        compiler_params=pltpu.CompilerParams(vmem_limit_bytes=16 * 1024 * 1024),
    )


def is_far(x):
    return x % 4 in (0, 3)


def solution(mesh):
    end = mesh.shape["gz"] - 1

    def across_of(x):
        return x + 1 if x % 2 else x - 1

    def other_of(x):
        return x - 1 if x % 2 else x + 1

    across = flat_pairs(mesh, lambda x, y, z: (across_of(x), y, z))
    other = flat_pairs(mesh, lambda x, y, z: (other_of(x), y, z))
    aside = flat_pairs(mesh, lambda x, y, z: (other_of(x), y, z) if is_far(x) else None)
    relay = flat_pairs(
        mesh, lambda x, y, z: None if is_far(x) else (other_of(across_of(other_of(x))), y, z)
    )
    beside = flat_pairs(mesh, lambda x, y, z: None if is_far(x) else (across_of(x), y, z))
    turn = flat_pairs(
        mesh,
        lambda x, y, z: None if is_far(x) or z not in (0, end) else (across_of(x), y, z),
    )
    y_up = flat_pairs(mesh, lambda x, y, z: (x, y + 1, z))
    y_down = flat_pairs(mesh, lambda x, y, z: (x, y - 1, z))
    last_x = mesh.shape["gx"] - 1
    z_up = flat_pairs(mesh, lambda x, y, z: (x if z < end else last_x - x, y, z + 1))
    z_down = flat_pairs(mesh, lambda x, y, z: (x if z > 0 else last_x - x, y, z - 1))

    def send(value, pairs):
        return lax.ppermute(value, AXES, pairs)

    def local(c, v):
        x, z = lax.axis_index("gx"), lax.axis_index("gz")
        place = jnp.stack([x % 2, (z > 0).astype(x.dtype), (z == 0).astype(x.dtype), (z == end).astype(x.dtype)])
        place = place.astype(jnp.int32)
        far = (x % 4 == 0) | (x % 4 == 3)
        layers = (6, 4, 16, 128)
        edge = (4, 16, 128)
        block = (3, 8, 16, 128)
        av, v = call(pack_aside, [(12, 16, 128), block], (), 1)(place, v)
        passed = send(av, aside)
        shapes = [(14, 16, 128), layers, edge, block]
        ac, b, _, c = call(pack_x, shapes, (), 2)(place, c, v)
        own_end = ac[12:]
        ac = send(ac, across)
        passed = send(jnp.concatenate([passed, own_end]), relay)
        near_av = send(av, beside)
        b = send(b, other)
        down, up = call(pack_y_early, [(36, 8, 128)] * 2, (), 3)(place, c, v, b)
        early_above = send(down, y_down)
        early_below = send(up, y_up)
        held = jnp.where(far, ac, passed)
        forwarded = send(held, other)
        end_a = jnp.where(far, own_end, send(passed[12:], turn))
        av = jnp.where(far, forwarded[:12], near_av)
        left, right = call(pack_z, [edge, edge], (), 8)(
            place, c, v, ac, av, b, held[12:], end_a, forwarded[12:]
        )
        zl = send(right, z_up)
        zr = send(left, z_down)
        down, up = call(pack_y_late, [(16, 8, 128)] * 2, (), 4)(place, ac, av, zl, zr)
        above = send(down, y_down)
        below = send(up, y_up)
        block = (16, 24, 128)
        state = [(3, 3, *block), (3, *block), (3, 3, *block)]
        state = call(compute_early, state, [(3, *block)], 5)(
            place, c, v, b, early_above, early_below
        )
        scratch = [(3, *block), block, block, (3, *block), block, (3, *block)]
        shapes = [a.shape for a in state] + [(3, 8, 16, 128)]
        *_, out = call(compute_late, shapes, scratch, 9, {7 + k: k for k in range(3)})(
            place, ac, av, zl, zr, above, below, *state
        )
        return out

    placed = P(None, *AXES)
    return jax.shard_map(local, mesh=mesh, in_specs=(placed, placed), out_specs=placed, check_vma=False)
```

```python
import jax
import jax.numpy as jnp
from jax import lax
from jax.experimental import pallas as pl
from jax.experimental.pallas import tpu as pltpu
from jax.sharding import PartitionSpec as P


AXES = ("gx", "gy", "gz")
HALF = 0.5


def flat_pairs(mesh, move):
    nx, ny, nz = (mesh.shape[a] for a in AXES)
    pairs = []
    for x in range(nx):
        for y in range(ny):
            for z in range(nz):
                to = move(x, y, z)
                if to is not None:
                    tx, ty, tz = to[0] % nx, to[1] % ny, to[2] % nz
                    pairs.append(((x * ny + y) * nz + z, (tx * ny + ty) * nz + tz))
    return pairs


def lanes_of(shape):
    return lax.broadcasted_iota(jnp.int32, shape, len(shape) - 1)


def rows_of(shape):
    return lax.broadcasted_iota(jnp.int32, shape, len(shape) - 2)


def roll(x, shift, axis):
    shift = shift % x.shape[axis]
    return x if shift == 0 else pltpu.roll(x, shift, axis)


def between(index, first, last):
    return (index >= first) & (index < last)


def loop(first, last, body, unroll=1):
    def step(i, carry):
        body(i)
        return carry

    lax.fori_loop(first, last, step, 0, unroll=unroll)


def field_of(c_ref, v_ref, field):
    return (c_ref, field) if field < 3 else (v_ref, field - 3)


def pack_aside(place_ref, v_ref, av_ref, v_out):
    high = 4 * place_ref[0]
    for i in range(3):
        for q in range(4):
            av_ref[4 * i + q] = v_ref[i, high + q]
    v_out[...] = v_ref[...]


def pack_x(place_ref, c_ref, v_ref, ac_ref, b_ref, edge_ref, c_out):
    high = 4 * place_ref[0]
    low = 4 - high
    shift = 4 * place_ref[1]

    def copy(q):
        for field in range(6):
            ref, i = field_of(c_ref, v_ref, field)
            if field < 3:
                ac_ref[4 * field + q] = ref[i, high + q]
                c_out[i, q], c_out[i, 4 + q] = ref[i, q], ref[i, 4 + q]
            b_ref[field, q] = ref[i, low + q]
        lane = lanes_of((16, 128))
        edge = jnp.zeros((16, 128), jnp.float32)
        for g in (1, 2):
            for field in range(6):
                ref, i = field_of(c_ref, v_ref, field)
                at = 32 * g + 4 * field
                x = pltpu.roll(ref[i, 4 * (g - 1) + q], shift + at, 1)
                edge = jnp.where(between(lane, at, at + 4), x, edge)
        edge_ref[q] = edge

    loop(0, 4, copy)
    for q in range(2):
        ac_ref[12 + q] = edge_ref[q] + roll(edge_ref[q + 2], 64, 1)


def lower_upper(odd, ac_ref, av_ref, b_ref, field, q):
    ref, i = field_of(ac_ref, av_ref, field)
    a, b = ref[4 * i + q], b_ref[field, q]
    return jnp.where(odd, b, a), jnp.where(odd, a, b)


def pack_z(
    place_ref, c_ref, v_ref, ac_ref, av_ref, b_ref, end_ref, end_a_ref, end_b_ref, left_ref, right_ref
):
    odd = place_ref[0] == 1
    first_end = place_ref[2] == 1
    last_end = place_ref[3] == 1

    def pack(q):
        lane = lanes_of((16, 128))
        left = jnp.zeros((16, 128), jnp.float32)
        right = left
        for field in range(6):
            ref, i = field_of(c_ref, v_ref, field)
            lo, hi = lower_upper(odd, ac_ref, av_ref, b_ref, field, q)
            for g, x in enumerate((lo, ref[i, q], ref[i, 4 + q], hi)):
                at = 32 * g + 4 * field
                here = between(lane, at, at + 4)
                left = jnp.where(here, roll(x, at, 1), left)
                right = jnp.where(here, roll(x, at + 4, 1), right)
        turn = 64 * lax.shift_right_logical(q, 1)
        base, a, b = (
            pltpu.roll(ref[lax.bitwise_and(q, 1)], turn, 1) for ref in (end_ref, end_a_ref, end_b_ref)
        )
        a, b = roll(a, 64, 1), roll(b, 64, 1)
        lo, hi = jnp.where(odd, a, b), jnp.where(odd, b, a)
        end = jnp.where(lane < 32, lo, jnp.where(lane < 96, base, hi))
        left_ref[q] = jnp.where(first_end, end, left)
        right_ref[q] = jnp.where(last_end, end, right)

    loop(0, 4, pack)


def join(down_ref, up_ref, entry, first, second):
    upper = rows_of((8, 128)) < 4
    down_ref[entry] = jnp.where(upper, first[0:8], roll(second[0:8], 4, 0))
    up_ref[entry] = jnp.where(upper, roll(first[8:16], 4, 0), second[8:16])


def halo(above_ref, below_ref, entry):
    upper = rows_of((8, 128)) < 4
    above, below = above_ref[entry], below_ref[entry]
    first = jnp.where(upper, above, roll(below, 4, 0))
    return first, jnp.where(upper, roll(above, 4, 0), below)


def pack_y_early(place_ref, c_ref, v_ref, b_ref, down_ref, up_ref):
    for field in range(6):
        ref, i = field_of(c_ref, v_ref, field)

        def own(q):
            join(down_ref, up_ref, 6 * field + q, ref[i, q], ref[i, 4 + q])

        def side(q):
            join(down_ref, up_ref, 6 * field + 4 + q, b_ref[field, q], b_ref[field, 2 + q])

        loop(0, 4, own)
        loop(0, 2, side)


def pack_y_late(place_ref, ac_ref, av_ref, zl_ref, zr_ref, down_ref, up_ref):
    def side(q):
        for field in range(6):
            ref, i = field_of(ac_ref, av_ref, field)
            join(down_ref, up_ref, 2 * field + q, ref[4 * i + q], ref[4 * i + 2 + q])

    def strip(q):
        join(down_ref, up_ref, 12 + q, zl_ref[q], zr_ref[q])

    loop(0, 2, side)
    loop(0, 4, strip)


def weights(v):
    t = HALF * jnp.abs(v)
    ahead = v > 0.0
    u = 1.0 - t
    tt = t * t
    centre = 1.0 + tt * (1.5 * t - 2.5)
    near = t * (0.5 + t * (2.0 - 1.5 * t))
    tu = -0.5 * t * u
    behind = tu * u
    far = tu * t
    return (
        jnp.where(ahead, 0.0, far),
        jnp.where(ahead, behind, near),
        centre,
        jnp.where(ahead, near, behind),
        jnp.where(ahead, far, 0.0),
    )


def spread(c, w, axis):
    near = roll(w[3] * c, 1, axis) + roll(w[1] * c, -1, axis)
    far = roll(w[4] * c, 2, axis) + roll(w[0] * c, -2, axis)
    return w[2] * c + near + far


def slope_of(two_back, back, forth, two_forth):
    return (8.0 * (forth - back) - (two_forth - two_back)) * (1.0 / 12.0)


def slope_roll(v, axis):
    return slope_of(roll(v, 2, axis), roll(v, 1, axis), roll(v, -1, axis), roll(v, -2, axis))


def replicate(e):
    lane = lanes_of(e.shape)
    up1, up2 = roll(e, 32, 1), roll(e, 64, 1)
    dn1, dn2 = roll(e, -32, 1), roll(e, -64, 1)
    first, second = lane < 32, lane < 64
    return (
        jnp.where(first, e, jnp.where(second, up1, up2)),
        jnp.where(first, dn1, jnp.where(second, e, up1)),
        jnp.where(first, dn2, jnp.where(second, dn1, e)),
    )


def along_x(sources, v_of, stores, rows, base, count):
    open_sums = {}
    for p in range(-2, count + 2):
        w = weights(v_of(base + p, rows))
        cs = [source(base + p, rows) for source in sources]
        for a in range(-2, 3):
            to = p + a
            if 0 <= to < count:
                terms = [w[a + 2] * c for c in cs]
                had = open_sums.get(to)
                open_sums[to] = terms if had is None else [h + t for h, t in zip(had, terms)]
        done = open_sums.pop(p - 2, None)
        if done is not None:
            for store, value in zip(stores, done):
                store(base + p - 2, rows, value)


def put(ref, *lead):
    def store(p, rows, value):
        ref[(*lead, p, rows)] = value

    return store


def get(ref, *lead):
    return lambda p, rows: ref[(*lead, p, rows)]


def over_tiles(body):
    loop(0, 3, lambda tile: body(pl.ds(pl.multiple_of(8 * tile, 8), 8)))


def main_along_x(t_ref, v_ref, x_ref, stage, base, count):
    sources = [get(t_ref, stage, i) for i in range(3)]
    stores = [put(x_ref, i) for i in range(3)]
    over_tiles(lambda rows: along_x(sources, get(v_ref, 0), stores, rows, base, count))


def main_along_yz(t_ref, v_ref, x_ref, s_ref, stage, slot):
    w = weights(v_ref[1, slot])
    cs = [spread(x_ref[i, slot], w, 0) for i in range(3)]
    w = weights(v_ref[2, slot])
    cs = [spread(c, w, 1) for c in cs]
    for i, c in enumerate(cs):
        t_ref[stage + 1, i, slot] = c + HALF * sum(cs[j] * s_ref[j, i, slot] for j in range(3))


def main_slopes(v_ref, s_ref, slot):
    for i in range(3):
        v = v_ref[i, slot]
        s_ref[0, i, slot] = slope_of(*[v_ref[i, slot + k] for k in (-2, -1, 1, 2)])
        s_ref[1, i, slot] = slope_roll(v, 0)
        s_ref[2, i, slot] = slope_roll(v, 1)


def widened(t_ref, w_ref, field):
    return (t_ref, (0, field)) if field < 3 else (w_ref, (field - 3,))


def edge_rows(t_ref, w_ref, ec_ref, ev_ref, ed_ref, zl, zr, s, rows):
    lane = lanes_of(zl.shape)
    back = 128 - 32 * lax.shift_right_logical(s, 2)
    zl, zr = pltpu.roll(zl, back, 1), pltpu.roll(zr, back, 1)
    for kind, e_ref in ((0, ec_ref), (1, ev_ref)):
        e = jnp.zeros(zl.shape, jnp.float32)
        for i in range(3):
            field = 3 * kind + i
            at = 32 * i
            source, where = widened(t_ref, w_ref, field)
            x = source[(*where, s, rows)]
            e = jnp.where(between(lane, at, at + 4), roll(zl, at - 4 * field, 1), e)
            e = jnp.where(between(lane, at + 4, at + 16), roll(x, at + 4, 1), e)
            e = jnp.where(between(lane, at + 16, at + 28), roll(x, at + 28, 1), e)
            e = jnp.where(between(lane, at + 28, at + 32), roll(zr, at + 28 - 4 * field, 1), e)
        e_ref[s, rows] = e
    for k, d in enumerate(replicate(e)):
        ed_ref[k, s, rows] = d


def compute_early(
    place_ref, c_ref, v_ref, b_ref, above_ref, below_ref, ac_ref, av_ref, zl_ref, zr_ref,
    t_ref, w_ref, s_ref, ec_ref, ev_ref, ed_ref, x_ref,
):
    odd = place_ref[0]
    side = 12 - 12 * odd
    first = 4 - 4 * odd

    def own(q):
        for field in range(6):
            ref, i = field_of(c_ref, v_ref, field)
            to, at = widened(t_ref, w_ref, field)
            to[(*at, 4 + q, slice(0, 16))] = ref[i, q]
            to[(*at, 8 + q, slice(0, 16))] = ref[i, 4 + q]
            near, far = halo(above_ref, below_ref, 6 * field + q)
            to[(*at, 4 + q, slice(16, 24))] = near
            to[(*at, 8 + q, slice(16, 24))] = far

    def beyond(q):
        for field in range(6):
            to, at = widened(t_ref, w_ref, field)
            to[(*at, side + q, slice(0, 16))] = b_ref[field, q]
            to[(*at, side + 2 + q, slice(0, 16))] = b_ref[field, 2 + q]
            near, far = halo(above_ref, below_ref, 6 * field + 4 + q)
            to[(*at, side + q, slice(16, 24))] = near
            to[(*at, side + 2 + q, slice(16, 24))] = far

    def across(q):
        for field in range(6):
            ref, i = field_of(ac_ref, av_ref, field)
            to, at = widened(t_ref, w_ref, field)
            to[(*at, 12 - side + q, slice(0, 16))] = ref[4 * i + q]

    def edges(s):
        q = lax.bitwise_and(s, 3)
        edge_rows(t_ref, w_ref, ec_ref, ev_ref, ed_ref, zl_ref[q], zr_ref[q], s, slice(0, 16))

    loop(0, 4, own)
    loop(0, 2, beyond)
    loop(0, 4, across)
    loop(0, 16, edges, 2)
    loop(0, 8, lambda k: main_slopes(w_ref, s_ref, first + 2 + k))

    def substep(n):
        main_along_x(t_ref, w_ref, x_ref, n, first + 2, 8)

        def pair(k):
            for j in range(2):
                main_along_yz(t_ref, w_ref, x_ref, s_ref, n, first + 2 + 2 * n + 2 * k + j)

        loop(0, 4 - 2 * n, pair)

    loop(0, 2, substep)


def compute_late(
    place_ref, above_ref, below_ref, t_in, w_in, s_in, ec_in, ev_in, ed_in,
    t_ref, w_ref, s_ref, ec_ref, ev_ref, ed_ref, out_ref, x_ref, ex_ref, es_ref,
):
    odd = place_ref[0]
    side = 12 * odd
    first = 2 + 8 * odd
    step = 2 - 4 * odd

    def beyond(q):
        for field in range(6):
            to, at = widened(t_ref, w_ref, field)
            near, far = halo(above_ref, below_ref, 2 * field + q)
            to[(*at, side + q, slice(16, 24))] = near
            to[(*at, side + 2 + q, slice(16, 24))] = far

    loop(0, 2, beyond)

    def edges(s):
        zl, zr = halo(above_ref, below_ref, 12 + lax.bitwise_and(s, 3))
        edge_rows(t_ref, w_ref, ec_ref, ev_ref, ed_ref, zl, zr, s, slice(16, 24))

    loop(0, 16, edges, 2)
    loop(0, 4, lambda k: main_slopes(w_ref, s_ref, first + k))

    def edge_slopes(s):
        v = ev_ref[s]
        es_ref[0, s] = slope_of(*[ev_ref[s + k] for k in (-2, -1, 1, 2)])
        es_ref[1, s] = slope_roll(v, 0)
        es_ref[2, s] = slope_roll(v, 1)

    loop(2, 14, edge_slopes, 4)

    def edge_along_yz(s):
        e = spread(ex_ref[s], weights(ed_ref[1, s]), 0)
        e = spread(e, weights(ed_ref[2, s]), 1)
        parts = replicate(e)
        ec_ref[s] = e + HALF * sum(parts[j] * es_ref[j, s] for j in range(3))

    def edge_substep(n):
        over_tiles(lambda rows: along_x([get(ec_ref)], get(ed_ref, 0), [put(ex_ref)], rows, 2, 12))

        def four(k):
            for j in range(4):
                edge_along_yz(2 + 2 * n + 4 * k + j)

        loop(0, 3 - n, four)

    loop(0, 2, edge_substep)

    def substep(n):
        base = first + step * n
        main_along_x(t_ref, w_ref, x_ref, n, base, 4)

        def pair(k):
            for j in range(2):
                main_along_yz(t_ref, w_ref, x_ref, s_ref, n, base + 2 * k + j)

        loop(0, 2, pair)

    loop(0, 2, substep)

    def finish(s):
        lane = lanes_of((16, 128))
        e = ec_ref[s + 4, 0:16]
        for i in range(3):
            value = jnp.where(lane < 4, roll(e, -(32 * i + 4), 1), t_ref[2, i, s + 4, 0:16])
            out_ref[i, s] = jnp.where(lane >= 124, roll(e, 100 - 32 * i, 1), value)

    loop(0, 8, finish)


def call(kernel, outs, scratch=(), operands=0, aliases=()):
    smem = pl.BlockSpec(memory_space=pltpu.SMEM)
    vmem = pl.BlockSpec(memory_space=pltpu.VMEM)
    shapes = [jax.ShapeDtypeStruct(o, jnp.float32) for o in outs]
    return pl.pallas_call(
        kernel,
        out_shape=shapes,
        in_specs=[smem] + [vmem] * operands,
        out_specs=[vmem] * len(outs),
        scratch_shapes=[pltpu.VMEM(s, jnp.float32) for s in scratch],
        input_output_aliases=dict(aliases),
        compiler_params=pltpu.CompilerParams(vmem_limit_bytes=16 * 1024 * 1024),
    )


def is_far(x):
    return x % 4 in (0, 3)


def solution(mesh):
    end = mesh.shape["gz"] - 1

    def across_of(x):
        return x + 1 if x % 2 else x - 1

    def other_of(x):
        return x - 1 if x % 2 else x + 1

    across = flat_pairs(mesh, lambda x, y, z: (across_of(x), y, z))
    other = flat_pairs(mesh, lambda x, y, z: (other_of(x), y, z))
    aside = flat_pairs(mesh, lambda x, y, z: (other_of(x), y, z) if is_far(x) else None)
    relay = flat_pairs(
        mesh, lambda x, y, z: None if is_far(x) else (other_of(across_of(other_of(x))), y, z)
    )
    beside = flat_pairs(mesh, lambda x, y, z: None if is_far(x) else (across_of(x), y, z))
    turn = flat_pairs(
        mesh,
        lambda x, y, z: None if is_far(x) or z not in (0, end) else (across_of(x), y, z),
    )
    y_up = flat_pairs(mesh, lambda x, y, z: (x, y + 1, z))
    y_down = flat_pairs(mesh, lambda x, y, z: (x, y - 1, z))
    last_x = mesh.shape["gx"] - 1
    z_up = flat_pairs(mesh, lambda x, y, z: (x if z < end else last_x - x, y, z + 1))
    z_down = flat_pairs(mesh, lambda x, y, z: (x if z > 0 else last_x - x, y, z - 1))

    def send(value, pairs):
        return lax.ppermute(value, AXES, pairs)

    def local(c, v):
        x, z = lax.axis_index("gx"), lax.axis_index("gz")
        place = jnp.stack([x % 2, (z > 0).astype(x.dtype), (z == 0).astype(x.dtype), (z == end).astype(x.dtype)])
        place = place.astype(jnp.int32)
        far = (x % 4 == 0) | (x % 4 == 3)
        layers = (6, 4, 16, 128)
        edge = (4, 16, 128)
        block = (3, 8, 16, 128)
        av, v = call(pack_aside, [(12, 16, 128), block], (), 1)(place, v)
        passed = send(av, aside)
        shapes = [(14, 16, 128), layers, edge, block]
        ac, b, _, c = call(pack_x, shapes, (), 2)(place, c, v)
        own_end = ac[12:]
        ac = send(ac, across)
        passed = send(jnp.concatenate([passed, own_end]), relay)
        near_av = send(av, beside)
        b = send(b, other)
        down, up = call(pack_y_early, [(36, 8, 128)] * 2, (), 3)(place, c, v, b)
        early_above = send(down, y_down)
        early_below = send(up, y_up)
        held = jnp.where(far, ac, passed)
        forwarded = send(held, other)
        end_a = jnp.where(far, own_end, send(passed[12:], turn))
        av = jnp.where(far, forwarded[:12], near_av)
        left, right = call(pack_z, [edge, edge], (), 8)(
            place, c, v, ac, av, b, held[12:], end_a, forwarded[12:]
        )
        zl = send(right, z_up)
        zr = send(left, z_down)
        down, up = call(pack_y_late, [(16, 8, 128)] * 2, (), 4)(place, ac, av, zl, zr)
        above = send(down, y_down)
        below = send(up, y_up)
        block = (16, 24, 128)
        state = [(3, 3, *block), (3, *block), (3, 3, *block), block, block, (3, *block)]
        state = call(compute_early, state, [(3, *block)], 9)(
            place, c, v, b, early_above, early_below, ac, av, zl, zr
        )
        scratch = [(3, *block), block, (3, *block)]
        shapes = [a.shape for a in state] + [(3, 8, 16, 128)]
        *_, out = call(compute_late, shapes, scratch, 8, {3 + k: k for k in range(6)})(
            place, above, below, *state
        )
        return out

    placed = P(None, *AXES)
    return jax.shard_map(local, mesh=mesh, in_specs=(placed, placed), out_specs=placed, check_vma=False)
```

```python
import jax
import jax.numpy as jnp
from jax import lax
from jax.experimental import pallas as pl
from jax.experimental.pallas import tpu as pltpu
from jax.sharding import PartitionSpec as P


AXES = ("gx", "gy", "gz")
HALF = 0.5


def flat_pairs(mesh, move):
    nx, ny, nz = (mesh.shape[a] for a in AXES)
    pairs = []
    for x in range(nx):
        for y in range(ny):
            for z in range(nz):
                to = move(x, y, z)
                if to is not None:
                    tx, ty, tz = to[0] % nx, to[1] % ny, to[2] % nz
                    pairs.append(((x * ny + y) * nz + z, (tx * ny + ty) * nz + tz))
    return pairs


def lanes_of(shape):
    return lax.broadcasted_iota(jnp.int32, shape, len(shape) - 1)


def rows_of(shape):
    return lax.broadcasted_iota(jnp.int32, shape, len(shape) - 2)


def roll(x, shift, axis):
    shift = shift % x.shape[axis]
    return x if shift == 0 else pltpu.roll(x, shift, axis)


def between(index, first, last):
    return (index >= first) & (index < last)


def loop(first, last, body, unroll=1):
    def step(i, carry):
        body(i)
        return carry

    lax.fori_loop(first, last, step, 0, unroll=unroll)


def field_of(c_ref, v_ref, field):
    return (c_ref, field) if field < 3 else (v_ref, field - 3)


def pack_aside(place_ref, v_ref, av_ref, v_out):
    high = 4 * place_ref[0]
    for i in range(3):
        for q in range(4):
            av_ref[4 * i + q] = v_ref[i, high + q]
    v_out[...] = v_ref[...]


def pack_x(place_ref, c_ref, v_ref, ac_ref, b_ref, edge_ref, c_out):
    high = 4 * place_ref[0]
    low = 4 - high
    shift = 4 * place_ref[1]

    def copy(q):
        for field in range(6):
            ref, i = field_of(c_ref, v_ref, field)
            if field < 3:
                ac_ref[4 * field + q] = ref[i, high + q]
                c_out[i, q], c_out[i, 4 + q] = ref[i, q], ref[i, 4 + q]
            b_ref[field, q] = ref[i, low + q]
        lane = lanes_of((16, 128))
        edge = jnp.zeros((16, 128), jnp.float32)
        for g in (1, 2):
            for field in range(6):
                ref, i = field_of(c_ref, v_ref, field)
                at = 32 * g + 4 * field
                x = pltpu.roll(ref[i, 4 * (g - 1) + q], shift + at, 1)
                edge = jnp.where(between(lane, at, at + 4), x, edge)
        edge_ref[q] = edge

    loop(0, 4, copy)
    for q in range(2):
        ac_ref[12 + q] = edge_ref[q] + roll(edge_ref[q + 2], 64, 1)


def lower_upper(odd, ac_ref, av_ref, b_ref, field, q):
    ref, i = field_of(ac_ref, av_ref, field)
    a, b = ref[4 * i + q], b_ref[field, q]
    return jnp.where(odd, b, a), jnp.where(odd, a, b)


def pack_z(
    place_ref, c_ref, v_ref, ac_ref, av_ref, b_ref, end_ref, end_a_ref, end_b_ref, left_ref, right_ref
):
    odd = place_ref[0] == 1
    first_end = place_ref[2] == 1
    last_end = place_ref[3] == 1

    def pack(q):
        lane = lanes_of((16, 128))
        left = jnp.zeros((16, 128), jnp.float32)
        right = left
        for field in range(6):
            ref, i = field_of(c_ref, v_ref, field)
            lo, hi = lower_upper(odd, ac_ref, av_ref, b_ref, field, q)
            for g, x in enumerate((lo, ref[i, q], ref[i, 4 + q], hi)):
                at = 32 * g + 4 * field
                here = between(lane, at, at + 4)
                left = jnp.where(here, roll(x, at, 1), left)
                right = jnp.where(here, roll(x, at + 4, 1), right)
        turn = 64 * lax.shift_right_logical(q, 1)
        base, a, b = (
            pltpu.roll(ref[lax.bitwise_and(q, 1)], turn, 1) for ref in (end_ref, end_a_ref, end_b_ref)
        )
        a, b = roll(a, 64, 1), roll(b, 64, 1)
        lo, hi = jnp.where(odd, a, b), jnp.where(odd, b, a)
        end = jnp.where(lane < 32, lo, jnp.where(lane < 96, base, hi))
        left_ref[q] = jnp.where(first_end, end, left)
        right_ref[q] = jnp.where(last_end, end, right)

    loop(0, 4, pack)


def join(down_ref, up_ref, entry, first, second):
    upper = rows_of((8, 128)) < 4
    down_ref[entry] = jnp.where(upper, first[0:8], roll(second[0:8], 4, 0))
    up_ref[entry] = jnp.where(upper, roll(first[8:16], 4, 0), second[8:16])


def halo(above_ref, below_ref, entry):
    upper = rows_of((8, 128)) < 4
    above, below = above_ref[entry], below_ref[entry]
    first = jnp.where(upper, above, roll(below, 4, 0))
    return first, jnp.where(upper, roll(above, 4, 0), below)


def pack_y_early(place_ref, c_ref, v_ref, b_ref, down_ref, up_ref):
    for field in range(6):
        ref, i = field_of(c_ref, v_ref, field)

        def own(q):
            join(down_ref, up_ref, 6 * field + q, ref[i, q], ref[i, 4 + q])

        def side(q):
            join(down_ref, up_ref, 6 * field + 4 + q, b_ref[field, q], b_ref[field, 2 + q])

        loop(0, 4, own)
        loop(0, 2, side)


def pack_y_late(place_ref, ac_ref, av_ref, zl_ref, zr_ref, down_ref, up_ref):
    def side(q):
        for field in range(6):
            ref, i = field_of(ac_ref, av_ref, field)
            join(down_ref, up_ref, 2 * field + q, ref[4 * i + q], ref[4 * i + 2 + q])

    def strip(q):
        join(down_ref, up_ref, 12 + q, zl_ref[q], zr_ref[q])

    loop(0, 2, side)
    loop(0, 4, strip)


def weights(v):
    t = HALF * jnp.abs(v)
    ahead = v > 0.0
    u = 1.0 - t
    tt = t * t
    centre = 1.0 + tt * (1.5 * t - 2.5)
    near = t * (0.5 + t * (2.0 - 1.5 * t))
    tu = -0.5 * t * u
    behind = tu * u
    far = tu * t
    return (
        jnp.where(ahead, 0.0, far),
        jnp.where(ahead, behind, near),
        centre,
        jnp.where(ahead, near, behind),
        jnp.where(ahead, far, 0.0),
    )


def spread(c, w, axis):
    near = roll(w[3] * c, 1, axis) + roll(w[1] * c, -1, axis)
    far = roll(w[4] * c, 2, axis) + roll(w[0] * c, -2, axis)
    return w[2] * c + near + far


def slope_of(two_back, back, forth, two_forth):
    return (8.0 * (forth - back) - (two_forth - two_back)) * (1.0 / 12.0)


def slope_roll(v, axis):
    return slope_of(roll(v, 2, axis), roll(v, 1, axis), roll(v, -1, axis), roll(v, -2, axis))


def replicate(e):
    lane = lanes_of(e.shape)
    up1, up2 = roll(e, 32, 1), roll(e, 64, 1)
    dn1, dn2 = roll(e, -32, 1), roll(e, -64, 1)
    first, second = lane < 32, lane < 64
    return (
        jnp.where(first, e, jnp.where(second, up1, up2)),
        jnp.where(first, dn1, jnp.where(second, e, up1)),
        jnp.where(first, dn2, jnp.where(second, dn1, e)),
    )


def along_x(sources, v_of, stores, rows, base, count):
    open_sums = {}
    for p in range(-2, count + 2):
        w = weights(v_of(base + p, rows))
        cs = [source(base + p, rows) for source in sources]
        for a in range(-2, 3):
            to = p + a
            if 0 <= to < count:
                terms = [w[a + 2] * c for c in cs]
                had = open_sums.get(to)
                open_sums[to] = terms if had is None else [h + t for h, t in zip(had, terms)]
        done = open_sums.pop(p - 2, None)
        if done is not None:
            for store, value in zip(stores, done):
                store(base + p - 2, rows, value)


def put(ref, *lead):
    def store(p, rows, value):
        ref[(*lead, p, rows)] = value

    return store


def get(ref, *lead):
    return lambda p, rows: ref[(*lead, p, rows)]


def over_tiles(body):
    loop(0, 3, lambda tile: body(pl.ds(pl.multiple_of(8 * tile, 8), 8)))


def main_along_x(t_ref, v_ref, x_ref, stage, base, count):
    sources = [get(t_ref, stage, i) for i in range(3)]
    stores = [put(x_ref, i) for i in range(3)]
    over_tiles(lambda rows: along_x(sources, get(v_ref, 0), stores, rows, base, count))


def main_along_yz(t_ref, v_ref, x_ref, s_ref, stage, slot):
    w = weights(v_ref[1, slot])
    cs = [spread(x_ref[i, slot], w, 0) for i in range(3)]
    w = weights(v_ref[2, slot])
    cs = [spread(c, w, 1) for c in cs]
    for i, c in enumerate(cs):
        t_ref[stage + 1, i, slot] = c + HALF * sum(cs[j] * s_ref[j, i, slot] for j in range(3))


def main_slopes(v_ref, s_ref, slot):
    for i in range(3):
        v = v_ref[i, slot]
        s_ref[0, i, slot] = slope_of(*[v_ref[i, slot + k] for k in (-2, -1, 1, 2)])
        s_ref[1, i, slot] = slope_roll(v, 0)
        s_ref[2, i, slot] = slope_roll(v, 1)


def widened(t_ref, w_ref, field):
    return (t_ref, (0, field)) if field < 3 else (w_ref, (field - 3,))


def edge_rows(t_ref, w_ref, ec_ref, ev_ref, ed_ref, zl, zr, s, rows):
    lane = lanes_of(zl.shape)
    back = 128 - 32 * lax.shift_right_logical(s, 2)
    zl, zr = pltpu.roll(zl, back, 1), pltpu.roll(zr, back, 1)
    for kind, e_ref in ((0, ec_ref), (1, ev_ref)):
        e = jnp.zeros(zl.shape, jnp.float32)
        for i in range(3):
            field = 3 * kind + i
            at = 32 * i
            source, where = widened(t_ref, w_ref, field)
            x = source[(*where, s, rows)]
            e = jnp.where(between(lane, at, at + 4), roll(zl, at - 4 * field, 1), e)
            e = jnp.where(between(lane, at + 4, at + 16), roll(x, at + 4, 1), e)
            e = jnp.where(between(lane, at + 16, at + 28), roll(x, at + 28, 1), e)
            e = jnp.where(between(lane, at + 28, at + 32), roll(zr, at + 28 - 4 * field, 1), e)
        e_ref[s, rows] = e
    for k, d in enumerate(replicate(e)):
        ed_ref[k, s, rows] = d


def compute_early(
    place_ref, c_ref, v_ref, b_ref, above_ref, below_ref, t_ref, w_ref, s_ref, x_ref
):
    odd = place_ref[0]
    side = 12 - 12 * odd
    first = 4 - 4 * odd

    def own(q):
        for field in range(6):
            ref, i = field_of(c_ref, v_ref, field)
            to, at = widened(t_ref, w_ref, field)
            to[(*at, 4 + q, slice(0, 16))] = ref[i, q]
            to[(*at, 8 + q, slice(0, 16))] = ref[i, 4 + q]
            near, far = halo(above_ref, below_ref, 6 * field + q)
            to[(*at, 4 + q, slice(16, 24))] = near
            to[(*at, 8 + q, slice(16, 24))] = far

    def beyond(q):
        for field in range(6):
            to, at = widened(t_ref, w_ref, field)
            to[(*at, side + q, slice(0, 16))] = b_ref[field, q]
            to[(*at, side + 2 + q, slice(0, 16))] = b_ref[field, 2 + q]
            near, far = halo(above_ref, below_ref, 6 * field + 4 + q)
            to[(*at, side + q, slice(16, 24))] = near
            to[(*at, side + 2 + q, slice(16, 24))] = far

    loop(0, 4, own)
    loop(0, 2, beyond)
    loop(0, 8, lambda k: main_slopes(w_ref, s_ref, first + 2 + k))

    def substep(n):
        main_along_x(t_ref, w_ref, x_ref, n, first + 2, 8)

        def pair(k):
            for j in range(2):
                main_along_yz(t_ref, w_ref, x_ref, s_ref, n, first + 2 + 2 * n + 2 * k + j)

        loop(0, 4 - 2 * n, pair)

    loop(0, 2, substep)


def own_edges(
    place_ref, ac_ref, av_ref, zl_ref, zr_ref, t_in, w_in, t_ref, w_ref, ec_ref, ev_ref, ed_ref
):
    side = 12 * place_ref[0]

    def across(q):
        for field in range(6):
            ref, i = field_of(ac_ref, av_ref, field)
            to, at = widened(t_ref, w_ref, field)
            to[(*at, side + q, slice(0, 16))] = ref[4 * i + q]

    def edges(s):
        q = lax.bitwise_and(s, 3)
        edge_rows(t_ref, w_ref, ec_ref, ev_ref, ed_ref, zl_ref[q], zr_ref[q], s, slice(0, 16))

    loop(0, 4, across)
    loop(0, 16, edges, 2)


def compute_late(
    place_ref, above_ref, below_ref, t_in, w_in, s_in, ec_in, ev_in, ed_in,
    t_ref, w_ref, s_ref, ec_ref, ev_ref, ed_ref, out_ref, x_ref, ex_ref, es_ref,
):
    odd = place_ref[0]
    side = 12 * odd
    first = 2 + 8 * odd
    step = 2 - 4 * odd

    def beyond(q):
        for field in range(6):
            to, at = widened(t_ref, w_ref, field)
            near, far = halo(above_ref, below_ref, 2 * field + q)
            to[(*at, side + q, slice(16, 24))] = near
            to[(*at, side + 2 + q, slice(16, 24))] = far

    loop(0, 2, beyond)

    def edges(s):
        zl, zr = halo(above_ref, below_ref, 12 + lax.bitwise_and(s, 3))
        edge_rows(t_ref, w_ref, ec_ref, ev_ref, ed_ref, zl, zr, s, slice(16, 24))

    loop(0, 16, edges, 2)
    loop(0, 4, lambda k: main_slopes(w_ref, s_ref, first + k))

    def edge_slopes(s):
        v = ev_ref[s]
        es_ref[0, s] = slope_of(*[ev_ref[s + k] for k in (-2, -1, 1, 2)])
        es_ref[1, s] = slope_roll(v, 0)
        es_ref[2, s] = slope_roll(v, 1)

    loop(2, 14, edge_slopes, 4)

    def edge_along_yz(s):
        e = spread(ex_ref[s], weights(ed_ref[1, s]), 0)
        e = spread(e, weights(ed_ref[2, s]), 1)
        parts = replicate(e)
        ec_ref[s] = e + HALF * sum(parts[j] * es_ref[j, s] for j in range(3))

    def edge_substep(n):
        over_tiles(lambda rows: along_x([get(ec_ref)], get(ed_ref, 0), [put(ex_ref)], rows, 2, 12))

        def four(k):
            for j in range(4):
                edge_along_yz(2 + 2 * n + 4 * k + j)

        loop(0, 3 - n, four)

    loop(0, 2, edge_substep)

    def substep(n):
        base = first + step * n
        main_along_x(t_ref, w_ref, x_ref, n, base, 4)

        def pair(k):
            for j in range(2):
                main_along_yz(t_ref, w_ref, x_ref, s_ref, n, base + 2 * k + j)

        loop(0, 2, pair)

    loop(0, 2, substep)

    def finish(s):
        lane = lanes_of((16, 128))
        e = ec_ref[s + 4, 0:16]
        for i in range(3):
            value = jnp.where(lane < 4, roll(e, -(32 * i + 4), 1), t_ref[2, i, s + 4, 0:16])
            out_ref[i, s] = jnp.where(lane >= 124, roll(e, 100 - 32 * i, 1), value)

    loop(0, 8, finish)


def call(kernel, outs, scratch=(), operands=0, aliases=()):
    smem = pl.BlockSpec(memory_space=pltpu.SMEM)
    vmem = pl.BlockSpec(memory_space=pltpu.VMEM)
    shapes = [jax.ShapeDtypeStruct(o, jnp.float32) for o in outs]
    return pl.pallas_call(
        kernel,
        out_shape=shapes,
        in_specs=[smem] + [vmem] * operands,
        out_specs=[vmem] * len(outs),
        scratch_shapes=[pltpu.VMEM(s, jnp.float32) for s in scratch],
        input_output_aliases=dict(aliases),
        compiler_params=pltpu.CompilerParams(vmem_limit_bytes=16 * 1024 * 1024),
    )


def is_far(x):
    return x % 4 in (0, 3)


def solution(mesh):
    end = mesh.shape["gz"] - 1

    def across_of(x):
        return x + 1 if x % 2 else x - 1

    def other_of(x):
        return x - 1 if x % 2 else x + 1

    across = flat_pairs(mesh, lambda x, y, z: (across_of(x), y, z))
    other = flat_pairs(mesh, lambda x, y, z: (other_of(x), y, z))
    aside = flat_pairs(mesh, lambda x, y, z: (other_of(x), y, z) if is_far(x) else None)
    relay = flat_pairs(
        mesh, lambda x, y, z: None if is_far(x) else (other_of(across_of(other_of(x))), y, z)
    )
    beside = flat_pairs(mesh, lambda x, y, z: None if is_far(x) else (across_of(x), y, z))
    turn = flat_pairs(
        mesh,
        lambda x, y, z: None if is_far(x) or z not in (0, end) else (across_of(x), y, z),
    )
    y_up = flat_pairs(mesh, lambda x, y, z: (x, y + 1, z))
    y_down = flat_pairs(mesh, lambda x, y, z: (x, y - 1, z))
    last_x = mesh.shape["gx"] - 1
    z_up = flat_pairs(mesh, lambda x, y, z: (x if z < end else last_x - x, y, z + 1))
    z_down = flat_pairs(mesh, lambda x, y, z: (x if z > 0 else last_x - x, y, z - 1))

    def send(value, pairs):
        return lax.ppermute(value, AXES, pairs)

    def local(c, v):
        x, z = lax.axis_index("gx"), lax.axis_index("gz")
        place = jnp.stack([x % 2, (z > 0).astype(x.dtype), (z == 0).astype(x.dtype), (z == end).astype(x.dtype)])
        place = place.astype(jnp.int32)
        far = (x % 4 == 0) | (x % 4 == 3)
        layers = (6, 4, 16, 128)
        edge = (4, 16, 128)
        block = (3, 8, 16, 128)
        av, v = call(pack_aside, [(12, 16, 128), block], (), 1)(place, v)
        passed = send(av, aside)
        shapes = [(14, 16, 128), layers, edge, block]
        ac, b, _, c = call(pack_x, shapes, (), 2)(place, c, v)
        own_end = ac[12:]
        ac = send(ac, across)
        passed = send(jnp.concatenate([passed, own_end]), relay)
        near_av = send(av, beside)
        b = send(b, other)
        down, up = call(pack_y_early, [(36, 8, 128)] * 2, (), 3)(place, c, v, b)
        early_above = send(down, y_down)
        early_below = send(up, y_up)
        held = jnp.where(far, ac, passed)
        forwarded = send(held, other)
        end_a = jnp.where(far, own_end, send(passed[12:], turn))
        av = jnp.where(far, forwarded[:12], near_av)
        left, right = call(pack_z, [edge, edge], (), 8)(
            place, c, v, ac, av, b, held[12:], end_a, forwarded[12:]
        )
        zl = send(right, z_up)
        zr = send(left, z_down)
        down, up = call(pack_y_late, [(16, 8, 128)] * 2, (), 4)(place, ac, av, zl, zr)
        above = send(down, y_down)
        below = send(up, y_up)
        block = (16, 24, 128)
        state = [(3, 3, *block), (3, *block), (3, 3, *block)]
        t, w, slopes = call(compute_early, state, [(3, *block)], 5)(
            place, c, v, b, early_above, early_below
        )
        state = [(3, 3, *block), (3, *block), block, block, (3, *block)]
        t, w, *edges = call(own_edges, state, (), 6, {5: 0, 6: 1})(
            place, ac, av, zl, zr, t, w
        )
        state = [t, w, slopes, *edges]
        scratch = [(3, *block), block, (3, *block)]
        shapes = [a.shape for a in state] + [(3, 8, 16, 128)]
        *_, out = call(compute_late, shapes, scratch, 8, {3 + k: k for k in range(6)})(
            place, above, below, *state
        )
        return out

    placed = P(None, *AXES)
    return jax.shard_map(local, mesh=mesh, in_specs=(placed, placed), out_specs=placed, check_vma=False)
```

```python
import jax
import jax.numpy as jnp
from jax import lax
from jax.experimental import pallas as pl
from jax.experimental.pallas import tpu as pltpu
from jax.sharding import PartitionSpec as P


AXES = ("gx", "gy", "gz")
HALF = 0.5


def flat_pairs(mesh, move):
    nx, ny, nz = (mesh.shape[a] for a in AXES)
    pairs = []
    for x in range(nx):
        for y in range(ny):
            for z in range(nz):
                to = move(x, y, z)
                if to is not None:
                    tx, ty, tz = to[0] % nx, to[1] % ny, to[2] % nz
                    pairs.append(((x * ny + y) * nz + z, (tx * ny + ty) * nz + tz))
    return pairs


def lanes_of(shape):
    return lax.broadcasted_iota(jnp.int32, shape, len(shape) - 1)


def rows_of(shape):
    return lax.broadcasted_iota(jnp.int32, shape, len(shape) - 2)


def roll(x, shift, axis):
    shift = shift % x.shape[axis]
    return x if shift == 0 else pltpu.roll(x, shift, axis)


def between(index, first, last):
    return (index >= first) & (index < last)


def loop(first, last, body, unroll=1):
    def step(i, carry):
        body(i)
        return carry

    lax.fori_loop(first, last, step, 0, unroll=unroll)


def field_of(c_ref, v_ref, field):
    return (c_ref, field) if field < 3 else (v_ref, field - 3)


def pack_aside(place_ref, v_ref, av_ref, v_out):
    high = 4 * place_ref[0]
    for i in range(3):
        for q in range(4):
            av_ref[4 * i + q] = v_ref[i, high + q]
    v_out[...] = v_ref[...]


def pack_x(place_ref, c_ref, v_ref, ac_ref, b_ref, edge_ref, c_out):
    high = 4 * place_ref[0]
    low = 4 - high
    shift = 4 * place_ref[1]

    def copy(q):
        for field in range(6):
            ref, i = field_of(c_ref, v_ref, field)
            if field < 3:
                ac_ref[4 * field + q] = ref[i, high + q]
                c_out[i, q], c_out[i, 4 + q] = ref[i, q], ref[i, 4 + q]
            b_ref[field, q] = ref[i, low + q]
        lane = lanes_of((16, 128))
        edge = jnp.zeros((16, 128), jnp.float32)
        for g in (1, 2):
            for field in range(6):
                ref, i = field_of(c_ref, v_ref, field)
                at = 32 * g + 4 * field
                x = pltpu.roll(ref[i, 4 * (g - 1) + q], shift + at, 1)
                edge = jnp.where(between(lane, at, at + 4), x, edge)
        edge_ref[q] = edge

    loop(0, 4, copy)
    for q in range(2):
        ac_ref[12 + q] = edge_ref[q] + roll(edge_ref[q + 2], 64, 1)


def lower_upper(odd, ac_ref, av_ref, b_ref, field, q):
    ref, i = field_of(ac_ref, av_ref, field)
    a, b = ref[4 * i + q], b_ref[field, q]
    return jnp.where(odd, b, a), jnp.where(odd, a, b)


def pack_z(
    place_ref, c_ref, v_ref, ac_ref, av_ref, b_ref, end_ref, end_a_ref, end_b_ref, left_ref, right_ref
):
    odd = place_ref[0] == 1
    first_end = place_ref[2] == 1
    last_end = place_ref[3] == 1

    def pack(q):
        lane = lanes_of((16, 128))
        left = jnp.zeros((16, 128), jnp.float32)
        right = left
        for field in range(6):
            ref, i = field_of(c_ref, v_ref, field)
            lo, hi = lower_upper(odd, ac_ref, av_ref, b_ref, field, q)
            for g, x in enumerate((lo, ref[i, q], ref[i, 4 + q], hi)):
                at = 32 * g + 4 * field
                here = between(lane, at, at + 4)
                left = jnp.where(here, roll(x, at, 1), left)
                right = jnp.where(here, roll(x, at + 4, 1), right)
        turn = 64 * lax.shift_right_logical(q, 1)
        base, a, b = (
            pltpu.roll(ref[lax.bitwise_and(q, 1)], turn, 1) for ref in (end_ref, end_a_ref, end_b_ref)
        )
        a, b = roll(a, 64, 1), roll(b, 64, 1)
        lo, hi = jnp.where(odd, a, b), jnp.where(odd, b, a)
        end = jnp.where(lane < 32, lo, jnp.where(lane < 96, base, hi))
        left_ref[q] = jnp.where(first_end, end, left)
        right_ref[q] = jnp.where(last_end, end, right)

    loop(0, 4, pack)


def join(down_ref, up_ref, entry, first, second):
    upper = rows_of((8, 128)) < 4
    down_ref[entry] = jnp.where(upper, first[0:8], roll(second[0:8], 4, 0))
    up_ref[entry] = jnp.where(upper, roll(first[8:16], 4, 0), second[8:16])


def halo(above_ref, below_ref, entry):
    upper = rows_of((8, 128)) < 4
    above, below = above_ref[entry], below_ref[entry]
    first = jnp.where(upper, above, roll(below, 4, 0))
    return first, jnp.where(upper, roll(above, 4, 0), below)


def pack_y_early(place_ref, c_ref, v_ref, b_ref, down_ref, up_ref):
    for field in range(6):
        ref, i = field_of(c_ref, v_ref, field)

        def own(q):
            join(down_ref, up_ref, 6 * field + q, ref[i, q], ref[i, 4 + q])

        def side(q):
            join(down_ref, up_ref, 6 * field + 4 + q, b_ref[field, q], b_ref[field, 2 + q])

        loop(0, 4, own)
        loop(0, 2, side)


def pack_y_late(place_ref, ac_ref, av_ref, zl_ref, zr_ref, down_ref, up_ref):
    def side(q):
        for field in range(6):
            ref, i = field_of(ac_ref, av_ref, field)
            join(down_ref, up_ref, 2 * field + q, ref[4 * i + q], ref[4 * i + 2 + q])

    def strip(q):
        join(down_ref, up_ref, 12 + q, zl_ref[q], zr_ref[q])

    loop(0, 2, side)
    loop(0, 4, strip)


def weights(v):
    t = HALF * jnp.abs(v)
    ahead = v > 0.0
    u = 1.0 - t
    tt = t * t
    centre = 1.0 + tt * (1.5 * t - 2.5)
    near = t * (0.5 + t * (2.0 - 1.5 * t))
    tu = -0.5 * t * u
    behind = tu * u
    far = tu * t
    return (
        jnp.where(ahead, 0.0, far),
        jnp.where(ahead, behind, near),
        centre,
        jnp.where(ahead, near, behind),
        jnp.where(ahead, far, 0.0),
    )


def spread(c, w, axis):
    near = roll(w[3] * c, 1, axis) + roll(w[1] * c, -1, axis)
    far = roll(w[4] * c, 2, axis) + roll(w[0] * c, -2, axis)
    return w[2] * c + near + far


def slope_of(two_back, back, forth, two_forth):
    return (8.0 * (forth - back) - (two_forth - two_back)) * (1.0 / 12.0)


def slope_roll(v, axis):
    return slope_of(roll(v, 2, axis), roll(v, 1, axis), roll(v, -1, axis), roll(v, -2, axis))


def replicate(e):
    lane = lanes_of(e.shape)
    up1, up2 = roll(e, 32, 1), roll(e, 64, 1)
    dn1, dn2 = roll(e, -32, 1), roll(e, -64, 1)
    first, second = lane < 32, lane < 64
    return (
        jnp.where(first, e, jnp.where(second, up1, up2)),
        jnp.where(first, dn1, jnp.where(second, e, up1)),
        jnp.where(first, dn2, jnp.where(second, dn1, e)),
    )


def along_x(sources, v_of, stores, rows, base, count):
    open_sums = {}
    for p in range(-2, count + 2):
        w = weights(v_of(base + p, rows))
        cs = [source(base + p, rows) for source in sources]
        for a in range(-2, 3):
            to = p + a
            if 0 <= to < count:
                terms = [w[a + 2] * c for c in cs]
                had = open_sums.get(to)
                open_sums[to] = terms if had is None else [h + t for h, t in zip(had, terms)]
        done = open_sums.pop(p - 2, None)
        if done is not None:
            for store, value in zip(stores, done):
                store(base + p - 2, rows, value)


def put(ref, *lead):
    def store(p, rows, value):
        ref[(*lead, p, rows)] = value

    return store


def get(ref, *lead):
    return lambda p, rows: ref[(*lead, p, rows)]


def over_tiles(body):
    loop(0, 3, lambda tile: body(pl.ds(pl.multiple_of(8 * tile, 8), 8)))


def main_along_x(t_ref, v_ref, x_ref, stage, base, count):
    sources = [get(t_ref, stage, i) for i in range(3)]
    stores = [put(x_ref, i) for i in range(3)]
    over_tiles(lambda rows: along_x(sources, get(v_ref, 0), stores, rows, base, count))


def main_along_yz(t_ref, v_ref, x_ref, s_ref, stage, slot):
    w = weights(v_ref[1, slot])
    cs = [spread(x_ref[i, slot], w, 0) for i in range(3)]
    w = weights(v_ref[2, slot])
    cs = [spread(c, w, 1) for c in cs]
    for i, c in enumerate(cs):
        t_ref[stage + 1, i, slot] = c + HALF * sum(cs[j] * s_ref[j, i, slot] for j in range(3))


def main_slopes(v_ref, s_ref, slot):
    for i in range(3):
        v = v_ref[i, slot]
        s_ref[0, i, slot] = slope_of(*[v_ref[i, slot + k] for k in (-2, -1, 1, 2)])
        s_ref[1, i, slot] = slope_roll(v, 0)
        s_ref[2, i, slot] = slope_roll(v, 1)


def widened(t_ref, w_ref, field):
    return (t_ref, (0, field)) if field < 3 else (w_ref, (field - 3,))


def edge_rows(t_ref, w_ref, ec_ref, ev_ref, ed_ref, zl, zr, s, rows):
    lane = lanes_of(zl.shape)
    back = 128 - 32 * lax.shift_right_logical(s, 2)

    def turned(x, shift):
        return pltpu.roll(x, lax.bitwise_and(back + shift + 128, 127), 1)

    for kind, e_ref in ((0, ec_ref), (1, ev_ref)):
        e = jnp.zeros(zl.shape, jnp.float32)
        for i in range(3):
            field = 3 * kind + i
            at = 32 * i
            source, where = widened(t_ref, w_ref, field)
            x = source[(*where, s, rows)]
            e = jnp.where(between(lane, at, at + 4), turned(zl, at - 4 * field), e)
            e = jnp.where(between(lane, at + 4, at + 16), roll(x, at + 4, 1), e)
            e = jnp.where(between(lane, at + 16, at + 28), roll(x, at + 28, 1), e)
            e = jnp.where(between(lane, at + 28, at + 32), turned(zr, at + 28 - 4 * field), e)
        e_ref[s, rows] = e
    for k, d in enumerate(replicate(e)):
        ed_ref[k, s, rows] = d


def compute_early(
    place_ref, c_ref, v_ref, b_ref, above_ref, below_ref, t_ref, w_ref, s_ref, x_ref
):
    odd = place_ref[0]
    side = 12 - 12 * odd
    first = 4 - 4 * odd

    def own(q):
        for field in range(6):
            ref, i = field_of(c_ref, v_ref, field)
            to, at = widened(t_ref, w_ref, field)
            to[(*at, 4 + q, slice(0, 16))] = ref[i, q]
            to[(*at, 8 + q, slice(0, 16))] = ref[i, 4 + q]
            near, far = halo(above_ref, below_ref, 6 * field + q)
            to[(*at, 4 + q, slice(16, 24))] = near
            to[(*at, 8 + q, slice(16, 24))] = far

    def beyond(q):
        for field in range(6):
            to, at = widened(t_ref, w_ref, field)
            to[(*at, side + q, slice(0, 16))] = b_ref[field, q]
            to[(*at, side + 2 + q, slice(0, 16))] = b_ref[field, 2 + q]
            near, far = halo(above_ref, below_ref, 6 * field + 4 + q)
            to[(*at, side + q, slice(16, 24))] = near
            to[(*at, side + 2 + q, slice(16, 24))] = far

    loop(0, 4, own)
    loop(0, 2, beyond)
    loop(0, 8, lambda k: main_slopes(w_ref, s_ref, first + 2 + k))

    def substep(n):
        main_along_x(t_ref, w_ref, x_ref, n, first + 2, 8)

        def pair(k):
            for j in range(2):
                main_along_yz(t_ref, w_ref, x_ref, s_ref, n, first + 2 + 2 * n + 2 * k + j)

        loop(0, 4 - 2 * n, pair)

    loop(0, 2, substep)


def own_edges(
    place_ref, ac_ref, av_ref, zl_ref, zr_ref, t_in, w_in, t_ref, w_ref, ec_ref, ev_ref, ed_ref
):
    side = 12 * place_ref[0]

    def across(q):
        for field in range(6):
            ref, i = field_of(ac_ref, av_ref, field)
            to, at = widened(t_ref, w_ref, field)
            to[(*at, side + q, slice(0, 16))] = ref[4 * i + q]

    def edges(s):
        q = lax.bitwise_and(s, 3)
        edge_rows(t_ref, w_ref, ec_ref, ev_ref, ed_ref, zl_ref[q], zr_ref[q], s, slice(0, 16))

    loop(0, 4, across)
    loop(0, 16, edges, 2)


def compute_late(
    place_ref, above_ref, below_ref, t_in, w_in, s_in, ec_in, ev_in, ed_in,
    t_ref, w_ref, s_ref, ec_ref, ev_ref, ed_ref, out_ref, x_ref, ex_ref, es_ref,
):
    odd = place_ref[0]
    side = 12 * odd
    first = 2 + 8 * odd
    step = 2 - 4 * odd

    def beyond(q):
        for field in range(6):
            to, at = widened(t_ref, w_ref, field)
            near, far = halo(above_ref, below_ref, 2 * field + q)
            to[(*at, side + q, slice(16, 24))] = near
            to[(*at, side + 2 + q, slice(16, 24))] = far

    loop(0, 2, beyond)

    def edges(s):
        zl, zr = halo(above_ref, below_ref, 12 + lax.bitwise_and(s, 3))
        edge_rows(t_ref, w_ref, ec_ref, ev_ref, ed_ref, zl, zr, s, slice(16, 24))

    loop(0, 16, edges, 2)
    loop(0, 4, lambda k: main_slopes(w_ref, s_ref, first + k))

    def edge_slopes(s):
        v = ev_ref[s]
        es_ref[0, s] = slope_of(*[ev_ref[s + k] for k in (-2, -1, 1, 2)])
        es_ref[1, s] = slope_roll(v, 0)
        es_ref[2, s] = slope_roll(v, 1)

    loop(2, 14, edge_slopes, 4)

    def edge_along_yz(s):
        e = spread(ex_ref[s], weights(ed_ref[1, s]), 0)
        e = spread(e, weights(ed_ref[2, s]), 1)
        parts = replicate(e)
        ec_ref[s] = e + HALF * sum(parts[j] * es_ref[j, s] for j in range(3))

    def edge_substep(n):
        over_tiles(lambda rows: along_x([get(ec_ref)], get(ed_ref, 0), [put(ex_ref)], rows, 2, 12))

        def four(k):
            for j in range(4):
                edge_along_yz(2 + 2 * n + 4 * k + j)

        loop(0, 3 - n, four)

    loop(0, 2, edge_substep)

    def substep(n):
        base = first + step * n
        main_along_x(t_ref, w_ref, x_ref, n, base, 4)

        def pair(k):
            for j in range(2):
                main_along_yz(t_ref, w_ref, x_ref, s_ref, n, base + 2 * k + j)

        loop(0, 2, pair)

    loop(0, 2, substep)

    def finish(s):
        lane = lanes_of((16, 128))
        e = ec_ref[s + 4, 0:16]
        for i in range(3):
            value = jnp.where(lane < 4, roll(e, -(32 * i + 4), 1), t_ref[2, i, s + 4, 0:16])
            out_ref[i, s] = jnp.where(lane >= 124, roll(e, 100 - 32 * i, 1), value)

    loop(0, 8, finish)


def call(kernel, outs, scratch=(), operands=0, aliases=()):
    smem = pl.BlockSpec(memory_space=pltpu.SMEM)
    vmem = pl.BlockSpec(memory_space=pltpu.VMEM)
    shapes = [jax.ShapeDtypeStruct(o, jnp.float32) for o in outs]
    return pl.pallas_call(
        kernel,
        out_shape=shapes,
        in_specs=[smem] + [vmem] * operands,
        out_specs=[vmem] * len(outs),
        scratch_shapes=[pltpu.VMEM(s, jnp.float32) for s in scratch],
        input_output_aliases=dict(aliases),
        compiler_params=pltpu.CompilerParams(vmem_limit_bytes=16 * 1024 * 1024),
    )


def is_far(x):
    return x % 4 in (0, 3)


def solution(mesh):
    end = mesh.shape["gz"] - 1

    def across_of(x):
        return x + 1 if x % 2 else x - 1

    def other_of(x):
        return x - 1 if x % 2 else x + 1

    across = flat_pairs(mesh, lambda x, y, z: (across_of(x), y, z))
    other = flat_pairs(mesh, lambda x, y, z: (other_of(x), y, z))
    aside = flat_pairs(mesh, lambda x, y, z: (other_of(x), y, z) if is_far(x) else None)
    relay = flat_pairs(
        mesh, lambda x, y, z: None if is_far(x) else (other_of(across_of(other_of(x))), y, z)
    )
    beside = flat_pairs(mesh, lambda x, y, z: None if is_far(x) else (across_of(x), y, z))
    turn = flat_pairs(
        mesh,
        lambda x, y, z: None if is_far(x) or z not in (0, end) else (across_of(x), y, z),
    )
    y_up = flat_pairs(mesh, lambda x, y, z: (x, y + 1, z))
    y_down = flat_pairs(mesh, lambda x, y, z: (x, y - 1, z))
    last_x = mesh.shape["gx"] - 1
    z_up = flat_pairs(mesh, lambda x, y, z: (x if z < end else last_x - x, y, z + 1))
    z_down = flat_pairs(mesh, lambda x, y, z: (x if z > 0 else last_x - x, y, z - 1))

    def send(value, pairs):
        return lax.ppermute(value, AXES, pairs)

    def local(c, v):
        x, z = lax.axis_index("gx"), lax.axis_index("gz")
        place = jnp.stack([x % 2, (z > 0).astype(x.dtype), (z == 0).astype(x.dtype), (z == end).astype(x.dtype)])
        place = place.astype(jnp.int32)
        far = (x % 4 == 0) | (x % 4 == 3)
        layers = (6, 4, 16, 128)
        edge = (4, 16, 128)
        block = (3, 8, 16, 128)
        av, v = call(pack_aside, [(12, 16, 128), block], (), 1)(place, v)
        passed = send(av, aside)
        shapes = [(14, 16, 128), layers, edge, block]
        ac, b, _, c = call(pack_x, shapes, (), 2)(place, c, v)
        own_end = ac[12:]
        ac = send(ac, across)
        passed = send(jnp.concatenate([passed, own_end]), relay)
        near_av = send(av, beside)
        b = send(b, other)
        down, up = call(pack_y_early, [(36, 8, 128)] * 2, (), 3)(place, c, v, b)
        early_above = send(down, y_down)
        early_below = send(up, y_up)
        held = jnp.where(far, ac, passed)
        forwarded = send(held, other)
        end_a = jnp.where(far, own_end, send(passed[12:], turn))
        av = jnp.where(far, forwarded[:12], near_av)
        left, right = call(pack_z, [edge, edge], (), 8)(
            place, c, v, ac, av, b, held[12:], end_a, forwarded[12:]
        )
        zl = send(right, z_up)
        zr = send(left, z_down)
        down, up = call(pack_y_late, [(16, 8, 128)] * 2, (), 4)(place, ac, av, zl, zr)
        above = send(down, y_down)
        below = send(up, y_up)
        block = (16, 24, 128)
        state = [(3, 3, *block), (3, *block), (3, 3, *block)]
        t, w, slopes = call(compute_early, state, [(3, *block)], 5)(
            place, c, v, b, early_above, early_below
        )
        state = [(3, 3, *block), (3, *block), block, block, (3, *block)]
        t, w, *edges = call(own_edges, state, (), 6, {5: 0, 6: 1})(
            place, ac, av, zl, zr, t, w
        )
        state = [t, w, slopes, *edges]
        scratch = [(3, *block), block, (3, *block)]
        shapes = [a.shape for a in state] + [(3, 8, 16, 128)]
        *_, out = call(compute_late, shapes, scratch, 8, {3 + k: k for k in range(6)})(
            place, above, below, *state
        )
        return out

    placed = P(None, *AXES)
    return jax.shard_map(local, mesh=mesh, in_specs=(placed, placed), out_specs=placed, check_vma=False)
```
